32 devices in a mesh: ctx: 8 (over y, x, core), fsdp: 4 (over z).
Axes of the slice: x: 2, y: 2, z: 4, core: 2. Of those that a mesh axis runs over, the one named last changes fastest.
Arguments:
- tokens: bfloat16 [4096, 1600], P(('fsdp', 'ctx')), may hold values from -6 to 6
- block_table: int32 [8, 2], replicated, may hold values from 0 to 15, as said below
- ln1_gain: bfloat16 [1600], P('fsdp'), may hold values from 0.099609375 to 1.8984375
- ln1_bias: bfloat16 [1600], P('fsdp'), may hold values from -1.75 to 1.75
- qkv_weight: bfloat16 [1600, 4800], P('fsdp'), may hold values from -0.15625 to 0.15625
- query_bias: bfloat16 [1600], P('fsdp'), may hold values from -3 to 3
- value_bias: bfloat16 [1600], P('fsdp'), may hold values from -0.875 to 0.875
- proj_weight: bfloat16 [1600, 1600], P('fsdp'), may hold values from -1.25 to 1.25
- proj_bias: bfloat16 [1600], P('fsdp'), may hold values from -1.75 to 1.75
- ln2_gain: bfloat16 [1600], P('fsdp'), may hold values from 0.099609375 to 1.8984375
- ln2_bias: bfloat16 [1600], P('fsdp'), may hold values from -1.75 to 1.75
- fc_weight: bfloat16 [1600, 6400], P('fsdp'), may hold values from -0.15625 to 0.15625
- fc_bias: bfloat16 [6400], P('fsdp'), may hold values from -3 to 3
- out_weight: bfloat16 [6400, 1600], P('fsdp'), may hold values from -0.078125 to 0.078125
- out_bias: bfloat16 [1600], P('fsdp'), may hold values from -1.75 to 1.75
- cotangent: bfloat16 [4096, 1600], P(('fsdp', 'ctx')), may hold values from -6 to 6
Outputs:
- layer_out: bfloat16 [4096, 1600], P(('fsdp', 'ctx'))
- grad_tokens: bfloat16 [4096, 1600], P(('fsdp', 'ctx'))
- grad_ln1_gain: float32 [1600], P('fsdp')
- grad_ln1_bias: float32 [1600], P('fsdp')
- grad_qkv_weight: float32 [1600, 4800], P('fsdp')
- grad_query_bias: float32 [1600], P('fsdp')
- grad_value_bias: float32 [1600], P('fsdp')
- grad_proj_weight: float32 [1600, 1600], P('fsdp')
- grad_proj_bias: float32 [1600], P('fsdp')
- grad_ln2_gain: float32 [1600], P('fsdp')
- grad_ln2_bias: float32 [1600], P('fsdp')
- grad_fc_weight: float32 [1600, 6400], P('fsdp')
- grad_fc_bias: float32 [6400], P('fsdp')
- grad_out_weight: float32 [6400, 1600], P('fsdp')
- grad_out_bias: float32 [1600], P('fsdp')
The draws below stay inside these ranges and needn't reach their ends.
Inputs may be any that keep to these rules, and one draw needn't show every extreme that they name: `block_table`: row i is (p_i, 15 - p_i) with p_i below 8; every block number appears exactly once.
All inputs are finite; a program needn't handle non-finite values.
Results may differ from the reference program's by a relative error of at most 0.02.
Values may be sent and summed in bfloat16 or wider, within the bound.
A program may use at most 256 MiB of HBM per device.

```python
import math
import jax
import jax.numpy as jnp
from jax import lax

D = 1600
HEADS = 25
HD = 64
FF = 6400
BLK = 64
BLOCKS = 16
L = 1024
SEQS = 4
TOKENS = 4096


def draw_block_table(key, part):
    order_ids = jax.random.permutation(jax.random.fold_in(key, 5), BLOCKS // 2).astype(jnp.int32)
    return jnp.stack([order_ids, BLOCKS - 1 - order_ids], axis=1).astype(jnp.int32)


def block_levels(rng, extent, split, low, high):
    gain = 1.0
    for axis_at, shards_of in split:
        draws = jax.random.uniform(jax.random.fold_in(jax.random.fold_in(rng, 6), axis_at), (shards_of,), jnp.float32, low / len(split), high / len(split))
        gain = gain * jnp.repeat(jnp.exp(draws), extent[axis_at] // shards_of).reshape((-1,) + (1,) * (len(extent) - 1 - axis_at))
    return gain


def noise(stream_key, shape, width, limit, cuts=(), kind=jnp.bfloat16):
    factor_of = block_levels(stream_key, shape, cuts, -0.22, 0.18) if cuts else 1.0
    values = jax.random.normal(stream_key, shape, jnp.float32) * width * factor_of
    return jnp.minimum(jnp.maximum(values, -limit), limit).astype(kind)


def setup_inputs(seed: int = 0) -> dict:
    key_of = jax.random.split(jax.random.key(seed), 17)
    tokens = noise(key_of[0], (TOKENS, D), 1.0, 6.0, ((0, 32),))
    block_table = draw_block_table(jax.random.fold_in(key_of[16], 71), 0)
    ln1_gain = jnp.clip(1.0 + 0.18 * jax.random.normal(key_of[2], (D,), jnp.float32), 0.099609375, 1.8984375).astype(jnp.bfloat16)
    ln1_bias = noise(key_of[3], (D,), 0.3, 1.75, ((0, 4),))
    qkv_weight = noise(key_of[4], (D, 3 * D), D ** -0.5, 0.15625, ((0, 4),))
    query_bias = noise(key_of[5], (D,), 0.5, 3.0, ((0, 4),))
    value_bias = noise(key_of[6], (D,), 0.15, 0.875, ((0, 4),))
    proj_weight = noise(key_of[7], (D, D), ((L / (16.0 * D)) ** 0.5), 1.25, ((0, 4),))
    proj_bias = noise(key_of[8], (D,), 0.3, 1.75, ((0, 4),))
    ln2_gain = jnp.clip(1.0 + 0.18 * jax.random.normal(key_of[9], (D,), jnp.float32), 0.099609375, 1.8984375).astype(jnp.bfloat16)
    ln2_bias = noise(key_of[10], (D,), 0.3, 1.75, ((0, 4),))
    fc_weight = noise(key_of[11], (D, FF), D ** -0.5, 0.15625, ((0, 4),))
    fc_bias = noise(key_of[12], (FF,), 0.5, 3.0, ((0, 4),))
    out_weight = noise(key_of[13], (FF, D), FF ** -0.5, 0.078125, ((0, 4),))
    out_bias = noise(key_of[14], (D,), 0.3, 1.75, ((0, 4),))
    cotangent = noise(key_of[15], (TOKENS, D), 1.0, 6.0, ((0, 32),))
    return dict(tokens=tokens, block_table=block_table, ln1_gain=ln1_gain, ln1_bias=ln1_bias, qkv_weight=qkv_weight, query_bias=query_bias, value_bias=value_bias, proj_weight=proj_weight, proj_bias=proj_bias, ln2_gain=ln2_gain, ln2_bias=ln2_bias, fc_weight=fc_weight, fc_bias=fc_bias, out_weight=out_weight, out_bias=out_bias, cotangent=cotangent)


@jax.custom_vjp
def low(v):
    return lax.optimization_barrier(v.astype(jnp.bfloat16)).astype(jnp.float32)

@jax.custom_vjp
def low_back(v):
    return v

def low_keep(v):
    return (low(v), None)

def low_pass(kept, grad):
    return (grad,)

def back_keep(v):
    return (v, None)

def back_low(kept, grad):
    return (low(grad),)
low.defvjp(low_keep, low_pass)
low_back.defvjp(back_keep, back_low)
highest = lax.Precision.HIGHEST

def layer_norm(values, gain_vec, shift_vec):
    centre = values - lax.optimization_barrier(jnp.mean(values, axis=-1, keepdims=True))
    spread = lax.optimization_barrier(jnp.mean(centre * centre, axis=-1, keepdims=True))
    return centre * lax.rsqrt(spread + 1e-05) * gain_vec + shift_vec

def attend(query_rows, key_rows, value_rows, query_pos, key_pos):
    raw_scores = low_back(jnp.einsum('qhd,khd->hqk', query_rows, key_rows, precision=highest))
    allowed = key_pos[None, None, :] <= query_pos[None, :, None]
    masked = jnp.where(allowed, raw_scores * HD ** (-0.5), -1e+30)
    soft_w = low(jax.nn.softmax(masked, axis=-1))
    return jnp.einsum('hqk,khd->qhd', soft_w, value_rows, precision=highest)

def reference(tokens, block_table, ln1_gain, ln1_bias, qkv_weight, query_bias, value_bias, proj_weight, proj_bias, ln2_gain, ln2_bias, fc_weight, fc_bias, out_weight, out_bias, cotangent):
    slot_ids = block_table.reshape(-1).astype(jnp.int32)
    positions = (slot_ids[:, None] * BLK + jnp.arange(BLK, dtype=jnp.int32)[None, :]).reshape(-1)
    q_block = math.gcd(L, 512)
    block_count = L // q_block

    def forward(inputs, gain_one, shift_one, qkv_w, q_bias, v_bias, proj_w, proj_b, gain_two, shift_two, fc_w, fc_b, out_w, out_b):

        def per_sequence(seq_rows):
            normed = low(layer_norm(seq_rows, gain_one, shift_one))
            bias_row = jnp.concatenate([q_bias, jnp.zeros_like(q_bias), v_bias])
            joined = low_back(jnp.dot(normed, qkv_w, precision=highest) + bias_row)
            query_rows = low(joined[:, :D]).reshape(L, HEADS, HD)
            key_rows = low(joined[:, D:2 * D]).reshape(L, HEADS, HD)
            value_rows = low(joined[:, 2 * D:]).reshape(L, HEADS, HD)

            def query_block(inputs_pair):
                return attend(inputs_pair[0], key_rows, value_rows, inputs_pair[1], positions)
            mixed_raw = lax.map(jax.checkpoint(query_block), (query_rows.reshape(block_count, q_block, HEADS, HD), positions.reshape(block_count, q_block))).reshape(L, D)
            heads_out = low(low_back(mixed_raw))
            branch = low_back(jnp.dot(heads_out, proj_w, precision=highest) + proj_b)
            middle = seq_rows + branch
            normed_two = low(layer_norm(middle, gain_two, shift_two))
            hidden_pre = low_back(jnp.dot(normed_two, fc_w, precision=highest) + fc_b)
            hidden = low(jax.nn.gelu(hidden_pre, approximate=True))
            return middle + low_back(jnp.dot(hidden, out_w, precision=highest) + out_b)
        return lax.map(jax.checkpoint(per_sequence), inputs)
    result, puller = jax.vjp(forward, tokens.astype(jnp.float32).reshape(SEQS, L, D), ln1_gain.astype(jnp.float32), ln1_bias.astype(jnp.float32), qkv_weight.astype(jnp.float32), query_bias.astype(jnp.float32), value_bias.astype(jnp.float32), proj_weight.astype(jnp.float32), proj_bias.astype(jnp.float32), ln2_gain.astype(jnp.float32), ln2_bias.astype(jnp.float32), fc_weight.astype(jnp.float32), fc_bias.astype(jnp.float32), out_weight.astype(jnp.float32), out_bias.astype(jnp.float32))
    gradients = puller(cotangent.astype(jnp.float32).reshape(SEQS, L, D))
    return (result.reshape(TOKENS, D).astype(jnp.bfloat16), gradients[0].reshape(TOKENS, D).astype(jnp.bfloat16), gradients[1], gradients[2], gradients[3], gradients[4], gradients[5], gradients[6], gradients[7], gradients[8], gradients[9], gradients[10], gradients[11], gradients[12], gradients[13])
```

```python
import functools

import jax
import jax.numpy as jnp
from jax import lax
from jax.experimental import pallas as pl
from jax.experimental.pallas import tpu as pltpu
from jax.sharding import PartitionSpec as P

HEADS = 25
BF = jnp.bfloat16
F32 = jnp.float32
MESH = pl.DeviceIdType.MESH
ANY = pl.BlockSpec(memory_space=pl.ANY)
VMEM = pl.BlockSpec(memory_space=pltpu.VMEM)
NT = (((1,), (1,)), ((), ()))


def dot(a, b, dims=(((1,), (0,)), ((), ()))):
    return lax.dot_general(a, b, dims, preferred_element_type=F32)


def places(n):
    me = lax.axis_index("ctx")
    core = lax.rem(me, 2)
    chip = me // 2
    sib = me + 1 - 2 * core
    if n == 8:
        across = chip + 1 - 2 * lax.rem(chip, 2)
        along = lax.rem(chip + 2, 4)
        first = across * (1 - core) + along * core
        second = along * (1 - core) + across * core
        others = [first, second, 3 - chip]
    else:
        half = n // 2
        others = [lax.rem(chip + d, half) for d in range(1, half)]
    return me, core, chip, sib, others


def twin(square, k):
    return 1 - k if square and k < 2 else k


def greet(devices):
    barrier = pltpu.get_barrier_semaphore()
    for device in devices:
        pl.semaphore_signal(barrier, inc=1, device_id={"ctx": device}, device_id_type=MESH)
    pl.semaphore_wait(barrier, len(devices))


def send(src, dst, ssem, rsem, device):
    return pltpu.make_async_remote_copy(
        src_ref=src,
        dst_ref=dst,
        send_sem=ssem,
        recv_sem=rsem,
        device_id={"ctx": device},
        device_id_type=MESH,
    )


def gather_kernel(n, count, parts, *refs):
    ins, outs = refs[:count], refs[count : 2 * count]
    own_sem, sib_s, sib_r, far_s, far_r = refs[2 * count :]
    me, core, chip, sib, others = places(n)
    square = n == 8
    peers = others[:2] if square else others
    half = n // 2
    if square:
        froms = others
    else:
        froms = [lax.rem(chip + half - d, half) for d in range(1, half)]
    greet([sib] + [2 * p + core for p in peers])
    rows = ins[0].shape[0] // parts
    started = []
    locals_ = []
    for j in range(count):
        own = pltpu.make_async_copy(ins[j], outs[j].at[me], own_sem.at[j])
        own.start()
        locals_.append(own)
    for j in range(count):
        for c in range(parts):
            win = pl.ds(c * rows, rows)
            for d, p in enumerate(peers):
                cp = send(
                    ins[j].at[win],
                    outs[j].at[me, win],
                    far_s.at[j, d, c],
                    far_r.at[j, d, c],
                    2 * p + core,
                )
                cp.start()
                started.append(cp)
            cp = send(
                ins[j].at[win],
                outs[j].at[me, win],
                sib_s.at[j, 0, c],
                sib_r.at[j, 0, c],
                sib,
            )
            cp.start()
            started.append(cp)

    def arrived(j, d, c):
        src = 2 * froms[d] + core
        win = pl.ds(c * rows, rows)
        piece = outs[j].at[src, win]
        send(piece, piece, far_s.at[j, d, c], far_r.at[j, d, c], sib).wait_recv()
        if square and d == 0:
            cp = send(
                piece, piece, far_s.at[j, 2, c], far_r.at[j, 2, c], 2 * others[1] + core
            )
            cp.start()
            started.append(cp)
        e = twin(square, d) + 1
        cp = send(piece, piece, sib_s.at[j, e, c], sib_r.at[j, e, c], sib)
        cp.start()
        started.append(cp)

    for j in range(count):
        for c in range(parts):
            for d in range(2 if square else len(others)):
                arrived(j, d, c)
        if square:
            for c in range(parts):
                arrived(j, 2, c)
    for own in locals_:
        own.wait()
    for j in range(count):
        for d in range(len(others) + 1):
            src = (me if d == 0 else 2 * froms[d - 1] + core) + sib - me
            for c in range(parts):
                piece = outs[j].at[src, pl.ds(c * rows, rows)]
                send(piece, piece, sib_s.at[j, d, c], sib_r.at[j, d, c], sib).wait_recv()
    for cp in started:
        cp.wait_send()


def plane_gather(n, cid, *arrays):
    count = len(arrays)
    rows, width = arrays[0].shape
    parts = 4 if n == 8 else 1
    far = n // 2 - 1
    outs = pl.pallas_call(
        functools.partial(gather_kernel, n, count, parts),
        out_shape=[jax.ShapeDtypeStruct((n,) + a.shape, a.dtype) for a in arrays],
        in_specs=[VMEM] * count,
        out_specs=[ANY] * count,
        scratch_shapes=[
            pltpu.SemaphoreType.DMA((count,)),
            pltpu.SemaphoreType.DMA((count, far + 1, parts)),
            pltpu.SemaphoreType.DMA((count, far + 1, parts)),
            pltpu.SemaphoreType.DMA((count, far, parts)),
            pltpu.SemaphoreType.DMA((count, far, parts)),
        ],
        compiler_params=pltpu.CompilerParams(collective_id=cid, has_side_effects=True),
        name=f"plane_gather_{cid}",
    )(*arrays)
    return [o.reshape(n * rows, width) for o in outs]


def scatter_kernel(n, parts, part_ref, out_ref, mine, theirs, sums, inbox, own_s, sib_s, sib_r, far_s, far_r):
    me, core, chip, sib, others = places(n)
    square = n == 8
    half = n // 2
    peers = others[:2] if square else others
    greet([sib] + [2 * p + core for p in peers])
    rows = part_ref.shape[1] // parts
    order = ([2, 0, 1, 3] if square else list(range(half)))
    chips = others + [chip]
    started = []
    loads = {}
    for c in range(parts):
        win = pl.ds(c * rows, rows)
        for k in order:
            e = twin(square, k)
            cp = send(
                part_ref.at[2 * chips[k] + 1 - core, win],
                theirs.at[e, win],
                sib_s.at[e, c],
                sib_r.at[e, c],
                sib,
            )
            cp.start()
            started.append(cp)
            ld = pltpu.make_async_copy(
                part_ref.at[2 * chips[k] + core, win], mine.at[k, win], own_s.at[k, c]
            )
            ld.start()
            loads[k, c] = ld

    def chip_sum(k, c):
        win = pl.ds(c * rows, rows)
        loads[k, c].wait()
        send(
            theirs.at[k, win], theirs.at[k, win], sib_s.at[k, c], sib_r.at[k, c], sib
        ).wait_recv()
        return mine[k, win, :].astype(F32) + theirs[k, win, :].astype(F32)

    def pass_on(k, c, slot, peer):
        win = pl.ds(c * rows, rows)
        cp = send(
            sums.at[k, win], inbox.at[slot, win], far_s.at[slot, c], far_r.at[slot, c], peer
        )
        cp.start()
        started.append(cp)

    def wait_in(slot, c):
        win = pl.ds(c * rows, rows)
        send(
            inbox.at[slot, win], inbox.at[slot, win], far_s.at[slot, c], far_r.at[slot, c], sib
        ).wait_recv()
        return inbox[slot, win, :].astype(F32)

    if square:
        a, b = 2 * others[0] + core, 2 * others[1] + core
        for c in range(parts):
            win = pl.ds(c * rows, rows)
            for k, slot in ((2, 0), (0, 1)):
                sums[k, win, :] = chip_sum(k, c).astype(BF)
                pass_on(k, c, slot, a)
        for c in range(parts):
            win = pl.ds(c * rows, rows)
            sums[1, win, :] = (chip_sum(1, c) + wait_in(0, c)).astype(BF)
            pass_on(1, c, 2, b)
        for c in range(parts):
            win = pl.ds(c * rows, rows)
            out_ref[win, :] = chip_sum(3, c) + wait_in(1, c)
        for c in range(parts):
            win = pl.ds(c * rows, rows)
            out_ref[win, :] += wait_in(2, c)
    else:
        for c in range(parts):
            win = pl.ds(c * rows, rows)
            for k in range(half - 1):
                sums[k, win, :] = chip_sum(k, c).astype(BF)
                pass_on(k, c, k, 2 * others[k] + core)
        for c in range(parts):
            win = pl.ds(c * rows, rows)
            out_ref[win, :] = chip_sum(half - 1, c)
            for k in range(half - 1):
                out_ref[win, :] += wait_in(k, c)
    for cp in started:
        cp.wait_send()


def plane_scatter(n, cid, partial):
    half = n // 2
    rows, width = partial.shape[0] // n, partial.shape[1]
    parts = 4 if n == 8 else 1
    return pl.pallas_call(
        functools.partial(scatter_kernel, n, parts),
        out_shape=jax.ShapeDtypeStruct((rows, width), F32),
        in_specs=[ANY],
        out_specs=VMEM,
        scratch_shapes=[
            pltpu.VMEM((half, rows, width), BF),
            pltpu.VMEM((half, rows, width), BF),
            pltpu.VMEM((half - 1, rows, width), BF),
            pltpu.VMEM((half - 1, rows, width), BF),
            pltpu.SemaphoreType.DMA((half, parts)),
            pltpu.SemaphoreType.DMA((half, parts)),
            pltpu.SemaphoreType.DMA((half, parts)),
            pltpu.SemaphoreType.DMA((half - 1, parts)),
            pltpu.SemaphoreType.DMA((half - 1, parts)),
        ],
        compiler_params=pltpu.CompilerParams(collective_id=cid, has_side_effects=True),
        name=f"plane_scatter_{cid}",
    )(partial.reshape(n, rows, width))


def attend_kernel(blocks, blk, tile, inv_ref, q_ref, k_ref, v_ref, o_ref, p_ref, qn, kn, vn, ot):
    length = blocks * blk
    for i in range(blocks):
        src, dst = pl.ds(pl.multiple_of(inv_ref[i] * blk, blk), blk), pl.ds(i * blk, blk)
        qn[dst, :] = q_ref[src, :]
        kn[dst, :] = k_ref[src, :]
        vn[dst, :] = v_ref[src, :]
    v_turned = vn[...].astype(F32).T.astype(BF)
    lane = lax.broadcasted_iota(jnp.int32, (1, 128), 1)
    above = lax.broadcasted_iota(jnp.int32, (tile, tile), 0) > lax.broadcasted_iota(
        jnp.int32, (tile, tile), 1
    )
    for i in range(length // tile):
        cols = pl.ds(i * tile, tile)
        keys = (i + 1) * tile
        for h in range(2):
            here = (lane // 64) == h
            q = jnp.where(here, qn[cols, :].astype(F32) * 0.125, 0.0).astype(BF)
            last = jnp.where(above, -1e30, dot(kn[pl.ds(i * tile, tile), :], q, NT))
            top = jnp.max(last, axis=0, keepdims=True)
            if i:
                early = dot(kn[pl.ds(0, i * tile), :], q, NT)
                top = jnp.maximum(top, jnp.max(early, axis=0, keepdims=True))
            last = jnp.exp(last - top)
            total = jnp.sum(last, axis=0, keepdims=True)
            if i:
                early = jnp.exp(early - top)
                total = total + jnp.sum(early, axis=0, keepdims=True)
            scale = 1.0 / total
            last = (last * scale).astype(BF)
            p_ref[h, pl.ds(i * tile, tile), cols] = last
            half = slice(64 * h, 64 * h + 64)
            o = dot(v_turned[half, i * tile : keys], last)
            if i:
                early = (early * scale).astype(BF)
                p_ref[h, pl.ds(0, i * tile), cols] = early
                o = o + dot(v_turned[half, : i * tile], early)
            ot[half, cols] = o
    o_nat = ot[...].T
    for i in range(blocks):
        o_ref[pl.ds(pl.multiple_of(inv_ref[i] * blk, blk), blk), :] = o_nat[
            i * blk : (i + 1) * blk, :
        ].astype(BF)


def attend(qkv, inv, blk):
    length = qkv.shape[0]
    cols = qkv.shape[1] // 3
    pairs = cols // 128
    blocks = inv.shape[0]
    tile = 256
    piece = lambda off: pl.BlockSpec((length, 128), lambda p, s: (0, off * pairs + p))
    return pl.pallas_call(
        functools.partial(attend_kernel, blocks, blk, tile),
        out_shape=[
            jax.ShapeDtypeStruct((length, cols), BF),
            jax.ShapeDtypeStruct((2 * pairs, length, length), BF),
        ],
        grid_spec=pltpu.PrefetchScalarGridSpec(
            num_scalar_prefetch=1,
            grid=(pairs,),
            in_specs=[piece(0), piece(1), piece(2)],
            out_specs=[
                pl.BlockSpec((length, 128), lambda p, s: (0, p)),
                pl.BlockSpec((2, length, length), lambda p, s: (p, 0, 0)),
            ],
            scratch_shapes=[
                pltpu.VMEM((length, 128), BF),
                pltpu.VMEM((length, 128), BF),
                pltpu.VMEM((length, 128), BF),
                pltpu.VMEM((128, length), F32),
            ],
        ),
        compiler_params=pltpu.CompilerParams(vmem_limit_bytes=60 * 1024 * 1024),
        name="attend",
    )(inv, qkv, qkv, qkv)


def attend_back_kernel(
    blocks, blk, tile, pairs, inv_ref, q_ref, k_ref, v_ref, g_ref, o_ref, p_ref, out_ref,
    qn, kn, vn, gn, on, dqt, dk, dv,
):
    length = blocks * blk
    for i in range(blocks):
        src, dst = pl.ds(pl.multiple_of(inv_ref[i] * blk, blk), blk), pl.ds(i * blk, blk)
        qn[dst, :] = q_ref[src, :]
        kn[dst, :] = k_ref[src, :]
        vn[dst, :] = v_ref[src, :]
        gn[dst, :] = g_ref[src, :]
        on[dst, :] = o_ref[src, :]
    k_turned = kn[...].astype(F32).T.astype(BF)
    prod = (gn[...].astype(F32) * on[...].astype(F32)).T
    deltas = [jnp.sum(prod[64 * h : 64 * h + 64, :], axis=0, keepdims=True) for h in range(2)]
    lane = lax.broadcasted_iota(jnp.int32, (1, 128), 1)
    dk[...] = jnp.zeros_like(dk)
    dv[...] = jnp.zeros_like(dv)
    for i in range(length // tile):
        cols = pl.ds(i * tile, tile)
        keys = (i + 1) * tile
        for h in range(2):
            here = (lane // 64) == h
            q = jnp.where(here, qn[cols, :].astype(F32), 0.0).astype(BF)
            g = jnp.where(here, gn[cols, :].astype(F32), 0.0).astype(BF)
            p = p_ref[h, pl.ds(0, keys), cols]
            dp = dot(vn[pl.ds(0, keys), :], g, NT)
            ds = (
                p.astype(F32) * (dp - deltas[h][:, i * tile : (i + 1) * tile]) * 0.125
            ).astype(BF)
            half = slice(64 * h, 64 * h + 64)
            dqt[half, cols] = dot(k_turned[half, :keys], ds)
            dk[pl.ds(0, keys), :] += dot(ds, q)
            dv[pl.ds(0, keys), :] += dot(p, g)
    dq = dqt[...].T
    pair = pl.program_id(0)
    for i in range(blocks):
        dst = pl.ds(pl.multiple_of(inv_ref[i] * blk, blk), blk)
        src = slice(i * blk, (i + 1) * blk)
        for t, val in enumerate((dq, dk, dv)):
            at = pl.ds(pl.multiple_of((t * pairs + pair) * 128, 128), 128)
            out_ref[dst, at] = val[src, :].astype(BF)


def attend_back(qkv, grad, o, p, inv, blk):
    length = qkv.shape[0]
    cols = qkv.shape[1] // 3
    pairs = cols // 128
    blocks = inv.shape[0]
    tile = 256
    piece = lambda off: pl.BlockSpec((length, 128), lambda i, s: (0, off * pairs + i))
    return pl.pallas_call(
        functools.partial(attend_back_kernel, blocks, blk, tile, pairs),
        out_shape=jax.ShapeDtypeStruct((length, 3 * cols), BF),
        grid_spec=pltpu.PrefetchScalarGridSpec(
            num_scalar_prefetch=1,
            grid=(pairs,),
            in_specs=[
                piece(0),
                piece(1),
                piece(2),
                piece(0),
                piece(0),
                pl.BlockSpec((2, length, length), lambda i, s: (i, 0, 0)),
            ],
            out_specs=pl.BlockSpec((length, 3 * cols), lambda i, s: (0, 0)),
            scratch_shapes=[pltpu.VMEM((length, 128), BF)] * 5
            + [
                pltpu.VMEM((128, length), F32),
                pltpu.VMEM((length, 128), F32),
                pltpu.VMEM((length, 128), F32),
            ],
        ),
        compiler_params=pltpu.CompilerParams(vmem_limit_bytes=60 * 1024 * 1024),
        name="attend_back",
    )(inv, qkv, qkv, qkv, grad, o, p)


def norm(values):
    centre = values - jnp.mean(values, axis=-1, keepdims=True)
    rstd = lax.rsqrt(jnp.mean(centre * centre, axis=-1, keepdims=True) + 1e-05)
    return centre * rstd, rstd


def norm_back(grad, unit, rstd, gain):
    inner = grad * gain
    return rstd * (
        inner
        - jnp.mean(inner, axis=-1, keepdims=True)
        - unit * jnp.mean(inner * unit, axis=-1, keepdims=True)
    )


def gelu(u):
    return jax.nn.gelu(u, approximate=True)


def make_body(n, nz):
    def body(
        tokens, block_table, ln1_gain, ln1_bias, qkv_weight, query_bias, value_bias,
        proj_weight, proj_bias, ln2_gain, ln2_bias, fc_weight, fc_bias, out_weight,
        out_bias, cotangent,
    ):
        ctx = lax.axis_index("ctx")
        z = lax.axis_index("fsdp")
        rows, width = tokens.shape
        blk = rows // 2
        wz = width // nz
        slots = -(-HEADS // n)
        hw = slots * (width // HEADS)
        unit_z = out_weight.shape[0]
        uw = unit_z // n
        units = uw * nz
        table = block_table.reshape(-1)
        inv = jnp.argmax(
            table[None, :] == jnp.arange(table.shape[0], dtype=table.dtype)[:, None], axis=1
        ).astype(jnp.int32)

        along_z = lambda a, axis=0: lax.all_gather(a, "fsdp", axis=axis, tiled=True)
        small = jnp.stack(
            [ln1_gain, ln1_bias, query_bias, value_bias, proj_bias, ln2_gain, ln2_bias, out_bias]
        )
        small = lax.all_gather(small, "fsdp", axis=0)
        small = small.transpose(1, 0, 2).reshape(8, width).astype(F32)
        g1, b1, qb, vb, pb, g2, b2, ob = [small[i] for i in range(8)]
        fb = along_z(lax.dynamic_slice_in_dim(fc_bias, ctx * uw, uw)).astype(F32)
        pad_cols = lambda v: lax.dynamic_slice_in_dim(jnp.pad(v, (0, n * hw - width)), ctx * hw, hw)
        qkv_bias = jnp.concatenate([pad_cols(qb), jnp.zeros((hw,), F32), pad_cols(vb)])

        padded = jnp.pad(qkv_weight, ((0, 0), (0, n * hw - width)))
        w_qkv = along_z(
            jnp.concatenate(
                [lax.dynamic_slice_in_dim(padded, t * width + ctx * hw, hw, 1) for t in range(3)],
                axis=1,
            )
        )
        w_proj = lax.psum(
            lax.dynamic_slice_in_dim(
                jnp.pad(proj_weight, ((hw, hw), (0, 0))),
                jnp.clip(ctx * hw - z * wz + hw, 0, wz + hw),
                hw,
                0,
            ),
            "fsdp",
        )
        w_fc = along_z(
            jnp.concatenate(
                [
                    lax.dynamic_slice_in_dim(fc_weight, t * unit_z + ctx * uw, uw, 1)
                    for t in range(nz)
                ],
                axis=1,
            )
        )
        w_out = along_z(lax.dynamic_slice_in_dim(out_weight, ctx * uw, uw, 0))

        x = tokens.astype(F32)
        unit1, rstd1 = norm(x)
        h1_own = (unit1 * g1 + b1).astype(BF)
        h1, cot = plane_gather(n, 1, h1_own, cotangent)
        qkv = (dot(h1, w_qkv) + qkv_bias).astype(BF)
        o, p = attend(qkv, inv, blk)
        mid = x + plane_scatter(n, 2, dot(o, w_proj).astype(BF)) + pb
        unit2, rstd2 = norm(mid)
        (h2,) = plane_gather(n, 3, (unit2 * g2 + b2).astype(BF))
        u = dot(h2, w_fc) + fb
        hidden, pull = jax.vjp(gelu, u)
        hidden = hidden.astype(BF)
        dz = dot(cot, w_out, NT)
        du = pull(dz)[0].astype(BF)
        dh2 = plane_scatter(n, 4, dot(du, w_fc, NT).astype(BF))
        dmid = cotangent.astype(F32) + norm_back(dh2, unit2, rstd2, g2)
        da_own = dmid.astype(BF)
        (da,) = plane_gather(n, 5, da_own)
        layer_out = (mid + plane_scatter(n, 6, dot(hidden, w_out).astype(BF)) + ob).astype(BF)
        TN = (((0,), (0,)), ((), ()))
        to_owner = lambda a: lax.psum_scatter(
            a.astype(BF), "fsdp", scatter_dimension=0, tiled=True
        )
        over_ctx = lambda a: lax.all_gather(a, "ctx", axis=0)
        part_out = over_ctx(to_owner(dot(hidden, cot, TN)))
        part_fc = over_ctx(to_owner(dot(h2, du, TN)))
        do = dot(da, w_proj, NT).astype(BF)
        dqkv = attend_back(qkv, do, o, p, inv, blk)
        part_qkv = over_ctx(to_owner(dot(h1, dqkv, TN)))
        part_proj = over_ctx(lax.psum(dot(o, da, TN).astype(BF), "fsdp"))
        dh1 = plane_scatter(n, 7, dot(dqkv, w_qkv, NT).astype(BF))
        grad_tokens = (dmid + norm_back(dh1, unit1, rstd1, g1)).astype(BF)

        grad_out = part_out.reshape(unit_z, width).astype(F32)
        grad_fc = (
            part_fc.reshape(n, wz, nz, uw)
            .transpose(1, 2, 0, 3)
            .reshape(wz, nz * unit_z)
            .astype(F32)
        )
        grad_qkv = (
            part_qkv.reshape(n, wz, 3, hw)
            .transpose(1, 2, 0, 3)
            .reshape(wz, 3, n * hw)[:, :, :width]
            .reshape(wz, 3 * width)
            .astype(F32)
        )
        grad_proj = lax.dynamic_slice_in_dim(
            part_proj.reshape(n * hw, width), z * wz, wz, 0
        ).astype(F32)

        put = lambda v, at, size: lax.dynamic_update_slice_in_dim(
            jnp.zeros((size,), F32), v, at, 0
        )
        col_sum = lambda a: jnp.sum(a.astype(F32), axis=0)
        bias_cols = col_sum(dqkv)
        dfb = col_sum(du).reshape(nz, uw)
        packed = jnp.concatenate(
            [
                col_sum(dh1 * unit1),
                col_sum(dh1),
                col_sum(da_own),
                col_sum(dh2 * unit2),
                col_sum(dh2),
                col_sum(cotangent),
                put(bias_cols[:hw], ctx * hw, n * hw),
                put(bias_cols[2 * hw :], ctx * hw, n * hw),
                lax.dynamic_update_slice_in_dim(
                    jnp.zeros((nz, unit_z), F32), dfb, ctx * uw, 1
                ).reshape(-1),
            ]
        )
        packed = lax.psum(packed, ("fsdp", "ctx"))
        mine = lambda i: lax.dynamic_slice_in_dim(packed, i + z * wz, wz, 0)
        base = 6 * width
        gfb = lax.dynamic_slice_in_dim(packed, base + 2 * n * hw + z * unit_z, unit_z, 0)
        return (
            layer_out,
            grad_tokens,
            mine(0),
            mine(width),
            grad_qkv,
            mine(base),
            mine(base + n * hw),
            grad_proj,
            mine(2 * width),
            mine(3 * width),
            mine(4 * width),
            grad_fc,
            gfb,
            grad_out,
            mine(5 * width),
        )

    return body


def solution(mesh):
    both = P(("fsdp", "ctx"), None)
    vec, mat = P("fsdp"), P("fsdp", None)
    placed = (both, P(), vec, vec, mat, vec, vec, mat, vec, vec, vec, mat, vec, mat, vec, both)
    outs = (both, both, vec, vec, mat, vec, vec, mat, vec, vec, vec, mat, vec, mat, vec)
    return jax.shard_map(
        make_body(mesh.shape["ctx"], mesh.shape["fsdp"]),
        mesh=mesh,
        in_specs=placed,
        out_specs=outs,
        check_vma=False,
    )
```

```python
import functools

import jax
import jax.numpy as jnp
from jax import lax
from jax.experimental import pallas as pl
from jax.experimental.pallas import tpu as pltpu
from jax.sharding import PartitionSpec as P

HEADS = 25
BF = jnp.bfloat16
F32 = jnp.float32
MESH = pl.DeviceIdType.MESH
ANY = pl.BlockSpec(memory_space=pl.ANY)
VMEM = pl.BlockSpec(memory_space=pltpu.VMEM)
NN = (((1,), (0,)), ((), ()))
NT = (((1,), (1,)), ((), ()))
TN = (((0,), (0,)), ((), ()))


def dot(a, b, dims=NN):
    return lax.dot_general(a, b, dims, preferred_element_type=F32)


def places(n):
    me = lax.axis_index("ctx")
    core = lax.rem(me, 2)
    chip = me // 2
    sib = me + 1 - 2 * core
    if n == 8:
        across = chip + 1 - 2 * lax.rem(chip, 2)
        along = lax.rem(chip + 2, 4)
        first = across * (1 - core) + along * core
        second = along * (1 - core) + across * core
        others = [first, second, 3 - chip]
    else:
        half = n // 2
        others = [lax.rem(chip + d, half) for d in range(1, half)]
    return me, core, chip, sib, others


def twin(square, k):
    return 1 - k if square and k < 2 else k


def signal(sem, **device):
    pl.semaphore_signal(sem, inc=1, device_id=device, device_id_type=MESH)


def greet(devices, planes=()):
    barrier = pltpu.get_barrier_semaphore()
    for device in devices:
        signal(barrier, ctx=device)
    for plane in planes:
        signal(barrier, fsdp=plane)
    pl.semaphore_wait(barrier, len(devices) + len(planes))


def send(src, dst, ssem, rsem, **device):
    return pltpu.make_async_remote_copy(
        src_ref=src,
        dst_ref=dst,
        send_sem=ssem,
        recv_sem=rsem,
        device_id=device,
        device_id_type=MESH,
    )


def merge(*lists):
    keyed = []
    for t, steps in enumerate(lists):
        keyed += [((i + 0.5) / len(steps), t, i, step) for i, step in enumerate(steps)]
    for item in sorted(keyed, key=lambda k: k[:3]):
        item[3]()


class Gather:
    def __init__(self, n, src, out, sems):
        self.n, self.src, self.out = n, src, out
        self.own_s, self.sib_s, self.sib_r, self.far_s, self.far_r = sems
        self.parts = src.shape[0]
        self.square = n == 8
        self.me, self.core, self.chip, self.sib, self.others = places(n)
        half = n // 2
        if self.square:
            self.froms = self.others
        else:
            self.froms = [lax.rem(self.chip + half - d, half) for d in range(1, half)]
        self.peers = self.others[:2] if self.square else self.others
        self.started = []

    @staticmethod
    def sems(n, parts):
        dma = pltpu.SemaphoreType.DMA
        far = n // 2 - 1
        return [dma((parts,)), dma((far + 1, parts)), dma((far + 1, parts)), dma((far, parts)), dma((far, parts))]

    def go(self, copy):
        copy.start()
        self.started.append(copy)

    def start(self):
        self.locals = []
        for c in range(self.parts):
            piece = self.src.at[c]
            for d, p in enumerate(self.peers):
                self.go(
                    send(
                        piece,
                        self.out.at[self.me, c],
                        self.far_s.at[d, c],
                        self.far_r.at[d, c],
                        ctx=2 * p + self.core,
                    )
                )
            self.go(
                send(
                    piece, self.out.at[self.me, c], self.sib_s.at[0, c], self.sib_r.at[0, c], ctx=self.sib
                )
            )
            own = pltpu.make_async_copy(piece, self.out.at[self.me, c], self.own_s.at[c])
            own.start()
            self.locals.append(own)

    def arrived(self, d, c):
        piece = self.out.at[2 * self.froms[d] + self.core, c]
        send(piece, piece, self.far_s.at[d, c], self.far_r.at[d, c], ctx=self.sib).wait_recv()
        if self.square and d == 0:
            self.go(
                send(
                    piece,
                    piece,
                    self.far_s.at[2, c],
                    self.far_r.at[2, c],
                    ctx=2 * self.others[1] + self.core,
                )
            )
        e = twin(self.square, d) + 1
        self.go(send(piece, piece, self.sib_s.at[e, c], self.sib_r.at[e, c], ctx=self.sib))

    def steps(self):
        todo = []
        for c in range(self.parts):
            for d in range(2 if self.square else len(self.others)):
                todo.append(functools.partial(self.arrived, d, c))
            if self.square and c:
                todo.append(functools.partial(self.arrived, 2, c - 1))
        if self.square:
            todo.append(functools.partial(self.arrived, 2, self.parts - 1))
        return todo

    def finish(self):
        for own in self.locals:
            own.wait()
        for d in range(len(self.others) + 1):
            chip = self.chip if d == 0 else self.froms[d - 1]
            for c in range(self.parts):
                piece = self.out.at[2 * chip + 1 - self.core, c]
                send(
                    piece, piece, self.sib_s.at[d, c], self.sib_r.at[d, c], ctx=self.sib
                ).wait_recv()
        for copy in self.started:
            copy.wait_send()


class Relay:
    def __init__(self, nz, z, lo, hi, count, src, out, sems, lead):
        self.nz, self.z, self.lo, self.hi, self.count = nz, z, lo, hi, count
        self.src, self.out, self.lead = src, out, lead
        self.own_s, self.up_s, self.down_s, self.recv = sems

    @staticmethod
    def sems(blocks):
        return [pltpu.SemaphoreType.DMA((blocks,)) for _ in range(4)]

    def up(self, src, b):
        return send(src, self.out.at[b], self.up_s.at[b], self.recv.at[b], fsdp=self.z + 1)

    def down(self, src, b):
        return send(src, self.out.at[b], self.down_s.at[b], self.recv.at[b], fsdp=self.z - 1)

    def own(self, b):
        return pltpu.make_async_copy(self.src.at[b - self.lead], self.out.at[b], self.own_s.at[b])

    def start(self):
        lo, hi = self.lo, self.hi

        def body(i, carry):
            u, d = hi - 1 - i, lo + i

            @pl.when(self.z < self.nz - 1)
            def _():
                self.up(self.src.at[u - self.lead], u).start()

            @pl.when(self.z > 0)
            def _():
                self.down(self.src.at[d - self.lead], d).start()

            self.own(d).start()
            return carry

        lax.fori_loop(0, hi - lo, body, 0)

    def step(self, i):
        b = self.lo - 1 - i

        @pl.when(b >= 0)
        def _():
            self.up(self.out.at[b], b).wait_recv()

            @pl.when(self.z < self.nz - 1)
            def _():
                self.up(self.out.at[b], b).start()

        e = self.hi + i

        @pl.when(e < self.count)
        def _():
            self.down(self.out.at[e], e).wait_recv()

            @pl.when(self.z > 0)
            def _():
                self.down(self.out.at[e], e).start()

    def steps(self, most):
        return [functools.partial(self.step, i) for i in range(most)]

    def finish(self):
        def sent(b, carry):
            @pl.when((self.z < self.nz - 1) & (b < self.hi))
            def _():
                self.up(self.out.at[b], b).wait_send()

            @pl.when((self.z > 0) & (b >= self.lo))
            def _():
                self.down(self.out.at[b], b).wait_send()

            @pl.when((b >= self.lo) & (b < self.hi))
            def _():
                self.own(b).wait()

            return carry

        lax.fori_loop(0, self.count, sent, 0)


def others_of(z, nz):
    return [lax.rem(z + d, nz) for d in range(1, nz)]


def entry_kernel(n, nz, tok, cot, small, wq, wp, h1_all, cot_all, vec, wq_all, wp_all, *scratch):
    h1, inbox, zeros, small_s, small_r, zero_s = scratch[:6]
    g_h, g_c = scratch[6:11], scratch[11:16]
    r_q, r_p = scratch[16:20], scratch[20:24]
    me, core, chip, sib, others = places(n)
    z = lax.axis_index("fsdp")
    planes = others_of(z, nz)
    greet([sib] + [2 * p + core for p in (others[:2] if n == 8 else others)], planes)
    width = tok.shape[1]
    wz = small.shape[1]
    for d, plane in enumerate(planes):
        send(small, inbox.at[z], small_s.at[d], small_r.at[d], fsdp=plane).start()
    inbox[z] = small[...]
    gather_c = Gather(n, cot, cot_all, g_c)
    gather_c.start()
    k = wq.shape[0]
    relay_q = Relay(nz, z, z * k, (z + 1) * k, nz * k, wq, wq_all, r_q, z * k)
    relay_q.start()
    share, blocks = wp.shape[0], wp_all.shape[0]
    base = me * blocks
    valid = jnp.clip(nz * share - base, 0, blocks)
    lo = jnp.clip(z * share - base, 0, valid)
    hi = jnp.clip((z + 1) * share - base, 0, valid)
    relay_p = Relay(nz, z, lo, hi, valid, wp, wp_all, r_p, z * share - base)
    relay_p.start()
    zeros[...] = jnp.zeros_like(zeros)

    def clear(b, carry):
        pltpu.make_async_copy(zeros, wp_all.at[b], zero_s.at[b]).start()
        return carry

    lax.fori_loop(valid, blocks, clear, 0)
    for d in range(nz - 1):
        came = lax.rem(z + nz - 1 - d, nz)
        send(small, inbox.at[came], small_s.at[d], small_r.at[d], fsdp=planes[d]).wait_recv()
    for p in range(nz):
        vec[:, p * wz : (p + 1) * wz] = inbox[p].astype(F32)
    gain, shift = vec[0:1, :], vec[1:2, :]
    parts, rows = h1.shape[0], h1.shape[1]
    for c in range(parts):
        unit, _ = norm(tok[c * rows : (c + 1) * rows, :].astype(F32))
        h1[c] = (unit * gain + shift).astype(BF)
    gather_h = Gather(n, h1, h1_all, g_h)
    gather_h.start()
    merge(
        gather_c.steps() + gather_h.steps(),
        relay_q.steps(nz * k - k) + relay_p.steps(blocks),
    )
    gather_c.finish()
    gather_h.finish()
    relay_q.finish()
    relay_p.finish()

    def cleared(b, carry):
        pltpu.make_async_copy(zeros, wp_all.at[b], zero_s.at[b]).wait()
        return carry

    lax.fori_loop(valid, blocks, cleared, 0)
    for d, plane in enumerate(planes):
        send(small, inbox.at[z], small_s.at[d], small_r.at[d], fsdp=plane).wait_send()


def entry(n, nz, tokens, cot, small, wq, wp, hw):
    rows, width = tokens.shape
    parts = 4 if n == 8 else 1
    dma = pltpu.SemaphoreType.DMA
    k, blocks = wq.shape[0], hw // 8
    shape = jax.ShapeDtypeStruct
    piece = (parts, rows // parts, width)
    return pl.pallas_call(
        functools.partial(entry_kernel, n, nz),
        out_shape=[
            shape((n,) + piece, BF),
            shape((n,) + piece, BF),
            shape((small.shape[0], width), F32),
            shape((nz * k,) + wq.shape[1:], BF),
            shape((blocks, 8, width), BF),
        ],
        in_specs=[VMEM] * 5,
        out_specs=[ANY, ANY, VMEM, ANY, ANY],
        scratch_shapes=[
            pltpu.VMEM(piece, BF),
            pltpu.VMEM((nz,) + small.shape, BF),
            pltpu.VMEM((8, width), BF),
            dma((nz - 1,)),
            dma((nz - 1,)),
            dma((blocks,)),
        ]
        + Gather.sems(n, parts)
        + Gather.sems(n, parts)
        + Relay.sems(nz * k)
        + Relay.sems(blocks),
        compiler_params=pltpu.CompilerParams(collective_id=1, has_side_effects=True),
        name="entry",
    )(tokens, cot.reshape(piece), small, wq, wp)


def gather_kernel(n, count, *refs):
    ins, outs, sems = refs[:count], refs[count : 2 * count], refs[2 * count :]
    me, core, chip, sib, others = places(n)
    greet([sib] + [2 * p + core for p in (others[:2] if n == 8 else others)])
    gathers = [Gather(n, ins[j], outs[j], sems[5 * j : 5 * j + 5]) for j in range(count)]
    for g in gathers:
        g.start()
    for g in gathers:
        for step in g.steps():
            step()
    for g in gathers:
        g.finish()


def plane_gather(n, cid, *arrays):
    count = len(arrays)
    sems = []
    for a in arrays:
        sems += Gather.sems(n, a.shape[0])
    return pl.pallas_call(
        functools.partial(gather_kernel, n, count),
        out_shape=[jax.ShapeDtypeStruct((n,) + a.shape, a.dtype) for a in arrays],
        in_specs=[VMEM] * count,
        out_specs=[ANY] * count,
        scratch_shapes=sems,
        compiler_params=pltpu.CompilerParams(collective_id=cid, has_side_effects=True),
        name=f"plane_gather_{cid}",
    )(*arrays)


class Scatter:
    def __init__(self, n, dims, a, w, out, scratch):
        self.n, self.dims, self.a, self.w, self.out = n, dims, a, w, out
        self.part, self.theirs, self.sums, self.inbox = scratch[:4]
        self.sib_s, self.sib_r, self.far_s, self.far_r = scratch[4:]
        self.me, self.core, self.chip, self.sib, self.others = places(n)
        self.square = n == 8
        self.half = n // 2
        self.parts = self.sib_s.shape[1]
        self.full = self.part.shape[2]
        self.rows = self.full // self.parts
        if self.square:
            first, second = [2 * p + self.core for p in self.others[:2]]
            self.ends = [(0, 0, first), (1, 1, first), (2, 2, second)]
        else:
            self.ends = [(k, k, 2 * self.others[k] + self.core) for k in range(self.half - 1)]

    @staticmethod
    def scratch(n, rows, width):
        dma = pltpu.SemaphoreType.DMA
        half, parts = n // 2, 2 if n == 8 else 1
        return [
            pltpu.VMEM((half, 2, rows, width), BF),
            pltpu.VMEM((half, rows, width), BF),
            pltpu.VMEM((half - 1, rows, width), BF),
            pltpu.VMEM((half - 1, rows, width), BF),
            dma((half, parts)),
            dma((half, parts)),
            dma((half - 1, parts)),
            dma((half - 1, parts)),
        ]

    def chip_at(self, k):
        if not self.square:
            return lax.rem(self.chip + 1 + k, self.half)
        x, y = lax.rem(self.chip, 2), self.chip // 2
        first, second = 1 - lax.rem(k, 3) // 2, 1 - lax.rem(k, 2)
        dx = first * (1 - self.core) + second * self.core
        dy = second * (1 - self.core) + first * self.core
        far = (k < 3).astype(jnp.int32)
        dx, dy = dx * far, dy * far
        return (y + dy - 2 * y * dy) * 2 + x + dx - 2 * x * dx

    def twin_at(self, k):
        if not self.square:
            return k
        return k + jnp.where(k == 1, 1, 0) - jnp.where(k == 2, 1, 0)

    def win(self, c):
        return pl.ds(c * self.rows, self.rows)

    def to_sib(self, k, c):
        e = self.twin_at(k)
        return send(
            self.part.at[k, 1 - self.core, self.win(c)],
            self.theirs.at[e, self.win(c)],
            self.sib_s.at[e, c],
            self.sib_r.at[e, c],
            ctx=self.sib,
        )

    def chip_sum(self, k, c):
        win = self.win(c)
        piece = self.theirs.at[k, win]
        send(piece, piece, self.sib_s.at[k, c], self.sib_r.at[k, c], ctx=self.sib).wait_recv()
        return self.part[k, self.core, win, :].astype(F32) + self.theirs[k, win, :].astype(F32)

    def pass_on(self, k, slot, peer, c):
        return send(
            self.sums.at[k, self.win(c)],
            self.inbox.at[slot, self.win(c)],
            self.far_s.at[slot, c],
            self.far_r.at[slot, c],
            ctx=peer,
        )

    def wait_in(self, slot, c):
        piece = self.inbox.at[slot, self.win(c)]
        send(piece, piece, self.far_s.at[slot, c], self.far_r.at[slot, c], ctx=self.sib).wait_recv()
        return self.inbox[slot, self.win(c), :].astype(F32)

    def forward(self, end, c):
        k, slot, peer = self.ends[end]
        total = self.chip_sum(k, c)
        if self.square and end == 2:
            total = total + self.wait_in(0, c)
        self.sums[k, self.win(c), :] = total.astype(BF)
        self.pass_on(k, slot, peer, c).start()

    def products(self):
        def product(k, carry):
            full = self.full
            at = pl.ds(pl.multiple_of(self.chip_at(k) * 2 * full, 2 * full), 2 * full)
            val = dot(self.a[at, :], self.w[...], self.dims).astype(BF)
            self.part[k, 0] = val[:full]
            self.part[k, 1] = val[full:]
            for c in range(self.parts):
                self.to_sib(k, c).start()

            @pl.when(k == 1)
            def _():
                for c in range(self.parts):
                    self.forward(0, c)

            return carry

        lax.fori_loop(0, self.half, product, 0)

    def own(self, c):
        self.out[self.win(c), :] = self.chip_sum(self.half - 1, c)

    def add(self, slot, c):
        self.out[self.win(c), :] += self.wait_in(slot, c)

    def steps(self):
        each = range(self.parts)
        todo = [functools.partial(self.forward, e, c) for e in range(1, self.half - 1) for c in each]
        todo += [functools.partial(self.own, c) for c in each]
        slots = (1, 2) if self.square else range(self.half - 1)
        return todo + [functools.partial(self.add, s, c) for s in slots for c in each]

    def finish(self):
        for c in range(self.parts):
            for k, slot, peer in self.ends:
                self.pass_on(k, slot, peer, c).wait_send()

        def sent(k, carry):
            for c in range(self.parts):
                self.to_sib(k, c).wait_send()
            return carry

        lax.fori_loop(0, self.half, sent, 0)


def scatter_kernel(n, dims, *refs):
    count = len(dims)
    ins, outs, scratch = refs[: 2 * count], refs[2 * count : 3 * count], refs[3 * count :]
    me, core, chip, sib, others = places(n)
    greet([sib] + [2 * p + core for p in (others[:2] if n == 8 else others)])
    jobs = [
        Scatter(n, dims[j], ins[2 * j], ins[2 * j + 1], outs[j], scratch[8 * j : 8 * j + 8])
        for j in range(count)
    ]
    steps = []
    for job in jobs:
        job.products()
        todo = job.steps()
        for step in todo[: job.parts]:
            step()
        steps += todo[job.parts :]
    for step in steps:
        step()
    for job in jobs:
        job.finish()


def plane_scatter(n, cid, *jobs):
    rows = jobs[0][0].shape[0] // n
    widths = [w.shape[1] if dims is NN else w.shape[0] for _, w, dims in jobs]
    scratch = []
    for width in widths:
        scratch += Scatter.scratch(n, rows, width)
    return pl.pallas_call(
        functools.partial(scatter_kernel, n, [job[2] for job in jobs]),
        out_shape=[jax.ShapeDtypeStruct((rows, width), F32) for width in widths],
        in_specs=[VMEM] * (2 * len(jobs)),
        out_specs=[VMEM] * len(jobs),
        scratch_shapes=scratch,
        compiler_params=pltpu.CompilerParams(
            collective_id=cid, has_side_effects=True, vmem_limit_bytes=60 * 1024 * 1024
        ),
        name=f"plane_scatter_{cid}",
    )(*[x for a, w, _ in jobs for x in (a, w)])


class Line:
    def __init__(self, nz, z, src, out, scratch):
        self.nz, self.z, self.src, self.out = nz, z, src, out
        self.mine, self.above, self.below, self.up_s, self.down_s, self.recv = scratch
        self.parts = src.shape[1]

    @staticmethod
    def scratch(shape):
        dma, lead = pltpu.SemaphoreType.DMA, shape[:2]
        return [pltpu.VMEM(shape, BF)] * 3 + [dma(lead), dma(lead), dma((2,) + lead)]

    def up(self, src, d, c):
        return send(
            src.at[d, c], self.above.at[d, c], self.up_s.at[d, c], self.recv.at[0, d, c], fsdp=self.z + 1
        )

    def down(self, src, d, c):
        return send(
            src.at[d, c], self.below.at[d, c], self.down_s.at[d, c], self.recv.at[1, d, c], fsdp=self.z - 1
        )

    def start(self):
        for d in range(self.nz - 1, 0, -1):

            @pl.when(self.z == 0)
            def _():
                for c in range(self.parts):
                    self.up(self.src, d, c).start()

            @pl.when(self.z == self.nz - 1)
            def _():
                for c in range(self.parts):
                    self.down(self.src, self.nz - 1 - d, c).start()

    def step_up(self, d, c):
        @pl.when((self.z > 0) & (self.z < d))
        def _():
            copy = self.up(self.mine, d, c)
            copy.wait_recv()
            self.mine[d, c] = (self.src[d, c].astype(F32) + self.above[d, c].astype(F32)).astype(BF)
            copy.start()

    def step_down(self, d, c):
        @pl.when((self.z < self.nz - 1) & (self.z > d))
        def _():
            copy = self.down(self.mine, d, c)
            copy.wait_recv()
            self.mine[d, c] = (self.src[d, c].astype(F32) + self.below[d, c].astype(F32)).astype(BF)
            copy.start()

    def settle(self, c):
        z = self.z
        self.out[c] = self.src[z, c]

        @pl.when(z > 0)
        def _():
            self.up(self.mine, z, c).wait_recv()
            self.out[c] = (self.out[c].astype(F32) + self.above[z, c].astype(F32)).astype(BF)

        @pl.when(z < self.nz - 1)
        def _():
            self.down(self.mine, z, c).wait_recv()
            self.out[c] = (self.out[c].astype(F32) + self.below[z, c].astype(F32)).astype(BF)

    def steps(self):
        todo = []
        for d in range(self.nz - 1, 1, -1):
            for c in range(self.parts):
                todo.append(functools.partial(self.step_up, d, c))
                todo.append(functools.partial(self.step_down, self.nz - 1 - d, c))
        return todo + [functools.partial(self.settle, c) for c in range(self.parts)]

    def finish(self):
        for d in range(self.nz):

            @pl.when(self.z < d)
            def _():
                for c in range(self.parts):
                    self.up(self.mine, d, c).wait_send()

            @pl.when(self.z > d)
            def _():
                for c in range(self.parts):
                    self.down(self.mine, d, c).wait_send()


def reduce_kernel(n, nz, gcount, dims, *refs):
    g_in, refs = refs[:gcount], refs[gcount:]
    line_in, a_in, w_in = refs[:3]
    refs = refs[3:]
    g_out, refs = refs[:gcount], refs[gcount:]
    line_out, out = refs[:2]
    refs = refs[2:]
    me, core, chip, sib, others = places(n)
    z = lax.axis_index("fsdp")
    greet([sib] + [2 * p + core for p in (others[:2] if n == 8 else others)], others_of(z, nz))
    line = Line(nz, z, line_in, line_out, refs[:6])
    line.start()
    scatter = Scatter(n, dims, a_in, w_in, out, refs[6:14])
    scatter.products()
    gathers = [
        Gather(n, g_in[j], g_out[j], refs[14 + 5 * j : 19 + 5 * j]) for j in range(gcount)
    ]
    plane_steps = []
    for g in gathers:
        g.start()
        plane_steps += g.steps()
    merge(plane_steps, line.steps(), scatter.steps())
    for job in gathers + [line, scatter]:
        job.finish()


def reduce_all(n, nz, cid, ready, partial, a, w, dims):
    rows, width = a.shape[0] // n, w.shape[0]
    scratch = Line.scratch(partial.shape) + Scatter.scratch(n, rows, width)
    for r in ready:
        scratch += Gather.sems(n, r.shape[0])
    shape = jax.ShapeDtypeStruct
    return pl.pallas_call(
        functools.partial(reduce_kernel, n, nz, len(ready), dims),
        out_shape=[shape((n,) + r.shape, BF) for r in ready]
        + [shape(partial.shape[1:], BF), shape((rows, width), F32)],
        in_specs=[VMEM] * (len(ready) + 3),
        out_specs=[ANY] * len(ready) + [VMEM] * 2,
        scratch_shapes=scratch,
        compiler_params=pltpu.CompilerParams(
            collective_id=cid, has_side_effects=True, vmem_limit_bytes=60 * 1024 * 1024
        ),
        name="reduce_all",
    )(*ready, partial, a, w)


class Vectors:
    def __init__(self, n, nz, src, out, scratch):
        self.n, self.nz, self.src, self.out = n, nz, src, out
        self.from_sib, self.chips, self.line = scratch[:3]
        self.ss, self.sr, self.cs, self.cr, self.ls, self.lr = scratch[3:]
        self.me, self.core, self.chip, self.sib, self.others = places(n)
        self.z = lax.axis_index("fsdp")
        self.planes = others_of(self.z, nz)

    @staticmethod
    def scratch(n, nz, shape):
        dma = pltpu.SemaphoreType.DMA
        half = n // 2
        return [
            pltpu.VMEM(shape, F32),
            pltpu.VMEM((half,) + shape, F32),
            pltpu.VMEM((nz,) + shape, F32),
            dma((1,)),
            dma((1,)),
            dma((half - 1,)),
            dma((half - 1,)),
            dma((nz - 1,)),
            dma((nz - 1,)),
        ]

    def to_sib(self):
        return send(self.src, self.from_sib, self.ss.at[0], self.sr.at[0], ctx=self.sib)

    def to_chip(self, d):
        at = self.chips.at[self.chip]
        return send(at, at, self.cs.at[d], self.cr.at[d], ctx=2 * self.others[d] + self.core)

    def to_plane(self, d):
        at = self.line.at[self.z]
        return send(at, at, self.ls.at[d], self.lr.at[d], fsdp=self.planes[d])

    def start(self):
        self.to_sib().start()

    def first(self):
        self.to_sib().wait_recv()
        self.chips[self.chip] = self.src[...] + self.from_sib[...]
        for d in range(self.n // 2 - 1):
            self.to_chip(d).start()

    def second(self):
        for d in range(self.n // 2 - 1):
            self.to_chip(d).wait_recv()
        total = self.chips[0]
        for k in range(1, self.n // 2):
            total = total + self.chips[k]
        self.line[self.z] = total
        for d in range(self.nz - 1):
            self.to_plane(d).start()

    def third(self):
        for d in range(self.nz - 1):
            self.to_plane(d).wait_recv()
        total = self.line[0]
        for k in range(1, self.nz):
            total = total + self.line[k]
        self.out[...] = total

    def steps(self):
        return [self.first, self.second, self.third]

    def finish(self):
        self.to_sib().wait_send()
        for d in range(self.n // 2 - 1):
            self.to_chip(d).wait_send()
        for d in range(self.nz - 1):
            self.to_plane(d).wait_send()


def last_kernel(n, nz, src, vec, out, vec_out, *scratch):
    me, core, chip, sib, others = places(n)
    z = lax.axis_index("fsdp")
    greet([sib] + [2 * p + core for p in others], others_of(z, nz))
    vectors = Vectors(n, nz, vec, vec_out, scratch[:9])
    vectors.start()
    gather = Gather(n, src, out, scratch[9:])
    gather.start()
    merge(gather.steps(), vectors.steps())
    gather.finish()
    vectors.finish()


def last_gather(n, nz, cid, array, vectors):
    shape = jax.ShapeDtypeStruct
    return pl.pallas_call(
        functools.partial(last_kernel, n, nz),
        out_shape=[shape((n,) + array.shape, BF), shape(vectors.shape, F32)],
        in_specs=[VMEM, VMEM],
        out_specs=[ANY, VMEM],
        scratch_shapes=Vectors.scratch(n, nz, vectors.shape) + Gather.sems(n, array.shape[0]),
        compiler_params=pltpu.CompilerParams(collective_id=cid, has_side_effects=True),
        name="last_gather",
    )(array, vectors)


def hidden_kernel(h_ref, w_ref, b_ref, z_ref, s_ref):
    u = dot(h_ref[...], w_ref[...]) + b_ref[...]
    root = 0.7978845608028654
    square = u * u
    inner = jnp.tanh(root * u * (1.0 + 0.044715 * square))
    z_ref[...] = (0.5 * u * (1.0 + inner)).astype(BF)
    slope = 0.5 * (1.0 + inner) + 0.5 * u * (1.0 - inner * inner) * root * (1.0 + 3 * 0.044715 * square)
    s_ref[...] = slope.astype(BF)


def hidden_back_kernel(c_ref, w_ref, s_ref, d_ref, sum_ref):
    du = (dot(c_ref[...], w_ref[...], NT) * s_ref[...].astype(F32)).astype(BF)
    d_ref[...] = du

    @pl.when(pl.program_id(0) == 0)
    def _():
        sum_ref[...] = jnp.zeros_like(sum_ref)

    sum_ref[...] += jnp.sum(du.astype(F32), axis=0, keepdims=True)


def tiled(rows, cols):
    return pl.BlockSpec((rows, cols), lambda i: (i, 0))


def fixed(rows, cols):
    return pl.BlockSpec((rows, cols), lambda i: (0, 0))


def hidden_units(h2, w_fc, bias):
    rows, width = h2.shape
    units = w_fc.shape[1]
    tile = 256
    shape = jax.ShapeDtypeStruct((rows, units), BF)
    return pl.pallas_call(
        hidden_kernel,
        grid=(rows // tile,),
        out_shape=[shape, shape],
        in_specs=[tiled(tile, width), fixed(width, units), fixed(1, units)],
        out_specs=[tiled(tile, units), tiled(tile, units)],
        name="hidden",
    )(h2, w_fc, bias)


def hidden_back(cot, w_out, slope):
    rows, width = cot.shape
    units = w_out.shape[0]
    tile = 256
    return pl.pallas_call(
        hidden_back_kernel,
        grid=(rows // tile,),
        out_shape=[
            jax.ShapeDtypeStruct((rows, units), BF),
            jax.ShapeDtypeStruct((1, units), F32),
        ],
        in_specs=[tiled(tile, width), fixed(units, width), tiled(tile, units)],
        out_specs=[tiled(tile, units), fixed(1, units)],
        name="hidden_back",
    )(cot, w_out, slope)


def join_kernel(n, nz, hw, width, fc, qp, out, fc_o, qkv_o, proj_o, out_o):
    uw = fc.shape[-1] // nz
    pw = width // n
    for c in range(n):
        for b in range(nz):
            at = b * n * uw + c * uw
            fc_o[:, at : at + uw] = fc[c, 0, :, b * uw : (b + 1) * uw].astype(F32)
        proj_o[:, c * pw : (c + 1) * pw] = qp[c, 0, :, 3 * hw : 3 * hw + pw].astype(F32)
        size = min(hw, width - c * hw)
        if size > 0:
            for t in range(3):
                at = t * width + c * hw
                qkv_o[:, at : at + size] = qp[c, 0, :, t * hw : t * hw + size].astype(F32)
    out_o[...] = out[...].astype(F32)


def join(n, nz, hw, fc, qp, out):
    tiles = 25
    width = out.shape[1]
    wz = fc.shape[1]
    split = lambda a: a.reshape(n, tiles, wz // tiles, a.shape[-1])
    fc, qp = split(fc), split(qp)
    wide = lambda a: pl.BlockSpec((n, 1, wz // tiles, a.shape[-1]), lambda i: (0, i, 0, 0))
    t, ot = wz // tiles, out.shape[0] // tiles
    cols = (nz * out.shape[0], 3 * width, width)
    shape = jax.ShapeDtypeStruct
    return pl.pallas_call(
        functools.partial(join_kernel, n, nz, hw, width),
        grid=(tiles,),
        out_shape=[shape((wz, c), F32) for c in cols] + [shape(out.shape, F32)],
        in_specs=[wide(fc), wide(qp), tiled(ot, width)],
        out_specs=[tiled(t, c) for c in cols] + [tiled(ot, width)],
        name="join",
    )(fc, qp, out)


def attend_kernel(blocks, blk, tile, inv_ref, q_ref, k_ref, v_ref, o_ref, p_ref, qn, kn, vn, ot):
    length = blocks * blk
    for i in range(blocks):
        src, dst = pl.ds(pl.multiple_of(inv_ref[i] * blk, blk), blk), pl.ds(i * blk, blk)
        qn[dst, :] = q_ref[src, :]
        kn[dst, :] = k_ref[src, :]
        vn[dst, :] = v_ref[src, :]
    v_turned = vn[...].astype(F32).T.astype(BF)
    lane = lax.broadcasted_iota(jnp.int32, (1, 128), 1)
    above = lax.broadcasted_iota(jnp.int32, (tile, tile), 0) > lax.broadcasted_iota(
        jnp.int32, (tile, tile), 1
    )
    for i in range(length // tile):
        cols = pl.ds(i * tile, tile)
        keys = (i + 1) * tile
        for h in range(2):
            here = (lane // 64) == h
            q = jnp.where(here, qn[cols, :].astype(F32) * 0.125, 0.0).astype(BF)
            last = jnp.where(above, -1e30, dot(kn[pl.ds(i * tile, tile), :], q, NT))
            top = jnp.max(last, axis=0, keepdims=True)
            if i:
                early = dot(kn[pl.ds(0, i * tile), :], q, NT)
                top = jnp.maximum(top, jnp.max(early, axis=0, keepdims=True))
            last = jnp.exp(last - top)
            total = jnp.sum(last, axis=0, keepdims=True)
            if i:
                early = jnp.exp(early - top)
                total = total + jnp.sum(early, axis=0, keepdims=True)
            scale = 1.0 / total
            last = (last * scale).astype(BF)
            p_ref[h, pl.ds(i * tile, tile), cols] = last
            half = slice(64 * h, 64 * h + 64)
            o = dot(v_turned[half, i * tile : keys], last)
            if i:
                early = (early * scale).astype(BF)
                p_ref[h, pl.ds(0, i * tile), cols] = early
                o = o + dot(v_turned[half, : i * tile], early)
            ot[half, cols] = o
    o_nat = ot[...].T
    for i in range(blocks):
        o_ref[pl.ds(pl.multiple_of(inv_ref[i] * blk, blk), blk), :] = o_nat[
            i * blk : (i + 1) * blk, :
        ].astype(BF)


def attend(qkv, inv, blk):
    length = qkv.shape[0]
    cols = qkv.shape[1] // 3
    pairs = cols // 128
    blocks = inv.shape[0]
    tile = 256
    piece = lambda off: pl.BlockSpec((length, 128), lambda p, s: (0, off * pairs + p))
    return pl.pallas_call(
        functools.partial(attend_kernel, blocks, blk, tile),
        out_shape=[
            jax.ShapeDtypeStruct((length, cols), BF),
            jax.ShapeDtypeStruct((2 * pairs, length, length), BF),
        ],
        grid_spec=pltpu.PrefetchScalarGridSpec(
            num_scalar_prefetch=1,
            grid=(pairs,),
            in_specs=[piece(0), piece(1), piece(2)],
            out_specs=[
                pl.BlockSpec((length, 128), lambda p, s: (0, p)),
                pl.BlockSpec((2, length, length), lambda p, s: (p, 0, 0)),
            ],
            scratch_shapes=[
                pltpu.VMEM((length, 128), BF),
                pltpu.VMEM((length, 128), BF),
                pltpu.VMEM((length, 128), BF),
                pltpu.VMEM((128, length), F32),
            ],
        ),
        compiler_params=pltpu.CompilerParams(vmem_limit_bytes=60 * 1024 * 1024),
        name="attend",
    )(inv, qkv, qkv, qkv)


def attend_back_kernel(
    blocks, blk, tile, pairs, inv_ref, q_ref, k_ref, v_ref, g_ref, o_ref, p_ref, out_ref,
    qn, kn, vn, gn, on, dqt, dk, dv,
):
    length = blocks * blk
    for i in range(blocks):
        src, dst = pl.ds(pl.multiple_of(inv_ref[i] * blk, blk), blk), pl.ds(i * blk, blk)
        qn[dst, :] = q_ref[src, :]
        kn[dst, :] = k_ref[src, :]
        vn[dst, :] = v_ref[src, :]
        gn[dst, :] = g_ref[src, :]
        on[dst, :] = o_ref[src, :]
    k_turned = kn[...].astype(F32).T.astype(BF)
    prod = (gn[...].astype(F32) * on[...].astype(F32)).T
    deltas = [jnp.sum(prod[64 * h : 64 * h + 64, :], axis=0, keepdims=True) for h in range(2)]
    lane = lax.broadcasted_iota(jnp.int32, (1, 128), 1)
    dk[...] = jnp.zeros_like(dk)
    dv[...] = jnp.zeros_like(dv)
    for i in range(length // tile):
        cols = pl.ds(i * tile, tile)
        keys = (i + 1) * tile
        for h in range(2):
            here = (lane // 64) == h
            q = jnp.where(here, qn[cols, :].astype(F32), 0.0).astype(BF)
            g = jnp.where(here, gn[cols, :].astype(F32), 0.0).astype(BF)
            p = p_ref[h, pl.ds(0, keys), cols]
            dp = dot(vn[pl.ds(0, keys), :], g, NT)
            ds = (
                p.astype(F32) * (dp - deltas[h][:, i * tile : (i + 1) * tile]) * 0.125
            ).astype(BF)
            half = slice(64 * h, 64 * h + 64)
            dqt[half, cols] = dot(k_turned[half, :keys], ds)
            dk[pl.ds(0, keys), :] += dot(ds, q)
            dv[pl.ds(0, keys), :] += dot(p, g)
    dq = dqt[...].T
    pair = pl.program_id(0)
    for i in range(blocks):
        dst = pl.ds(pl.multiple_of(inv_ref[i] * blk, blk), blk)
        src = slice(i * blk, (i + 1) * blk)
        for t, val in enumerate((dq, dk, dv)):
            at = pl.ds(pl.multiple_of((t * pairs + pair) * 128, 128), 128)
            out_ref[dst, at] = val[src, :].astype(BF)


def attend_back(qkv, grad, o, p, inv, blk):
    length = qkv.shape[0]
    cols = qkv.shape[1] // 3
    pairs = cols // 128
    blocks = inv.shape[0]
    tile = 256
    piece = lambda off: pl.BlockSpec((length, 128), lambda i, s: (0, off * pairs + i))
    return pl.pallas_call(
        functools.partial(attend_back_kernel, blocks, blk, tile, pairs),
        out_shape=jax.ShapeDtypeStruct((length, 3 * cols), BF),
        grid_spec=pltpu.PrefetchScalarGridSpec(
            num_scalar_prefetch=1,
            grid=(pairs,),
            in_specs=[
                piece(0),
                piece(1),
                piece(2),
                piece(0),
                piece(0),
                pl.BlockSpec((2, length, length), lambda i, s: (i, 0, 0)),
            ],
            out_specs=pl.BlockSpec((length, 3 * cols), lambda i, s: (0, 0)),
            scratch_shapes=[pltpu.VMEM((length, 128), BF)] * 5
            + [
                pltpu.VMEM((128, length), F32),
                pltpu.VMEM((length, 128), F32),
                pltpu.VMEM((length, 128), F32),
            ],
        ),
        compiler_params=pltpu.CompilerParams(vmem_limit_bytes=60 * 1024 * 1024),
        name="attend_back",
    )(inv, qkv, qkv, qkv, grad, o, p)


def norm(values):
    centre = values - jnp.mean(values, axis=-1, keepdims=True)
    rstd = lax.rsqrt(jnp.mean(centre * centre, axis=-1, keepdims=True) + 1e-05)
    return centre * rstd, rstd


def norm_back(grad, unit, rstd, gain):
    inner = grad * gain
    return rstd * (
        inner
        - jnp.mean(inner, axis=-1, keepdims=True)
        - unit * jnp.mean(inner * unit, axis=-1, keepdims=True)
    )


def make_body(n, nz):
    def body(
        tokens, block_table, ln1_gain, ln1_bias, qkv_weight, query_bias, value_bias,
        proj_weight, proj_bias, ln2_gain, ln2_bias, fc_weight, fc_bias, out_weight,
        out_bias, cotangent,
    ):
        ctx = lax.axis_index("ctx")
        z = lax.axis_index("fsdp")
        rows, width = tokens.shape
        blk = rows // 2
        wz = width // nz
        slots = -(-HEADS // n)
        hw = slots * (width // HEADS)
        unit_z = out_weight.shape[0]
        uw = unit_z // n
        units = uw * nz
        table = block_table.reshape(-1)
        inv = jnp.argmax(
            table[None, :] == jnp.arange(table.shape[0], dtype=table.dtype)[:, None], axis=1
        ).astype(jnp.int32)

        take = lambda a, at, size, axis=0: lax.dynamic_slice_in_dim(a, at, size, axis)
        parts = 5
        padded = jnp.pad(qkv_weight, ((0, 0), (0, n * hw - width)))
        wq_own = jnp.concatenate(
            [take(padded, t * width + ctx * hw, hw, 1) for t in range(3)], axis=1
        ).reshape(parts, wz // parts, 3 * hw)
        wfc_own = jnp.concatenate(
            [take(fc_weight, t * unit_z + ctx * uw, uw, 1) for t in range(nz)], axis=1
        )
        wout_own = take(out_weight, ctx * uw, uw)
        small = jnp.stack(
            [ln1_gain, ln1_bias, query_bias, value_bias, proj_bias, ln2_gain, ln2_bias, out_bias]
            + [jnp.pad(take(fc_bias, ctx * uw, uw), (0, wz - uw))]
            + [jnp.zeros_like(ln1_gain)] * 7
        )
        h1, cot, small, w_qkv, w_proj = entry(
            n, nz, tokens, cotangent, small, wq_own, proj_weight.reshape(wz // 8, 8, width), hw
        )
        small, wfc_own, wout_own = lax.optimization_barrier((small, wfc_own, wout_own))
        w_fc = lax.all_gather(wfc_own, "fsdp", axis=0, tiled=True)
        w_out = lax.all_gather(wout_own, "fsdp", axis=0, tiled=True)
        length = n * rows
        h1, cot = h1.reshape(length, width), cot.reshape(length, width)
        w_qkv, w_proj = w_qkv.reshape(width, 3 * hw), w_proj.reshape(hw, width)
        g1, b1, qb, vb, pb, g2, b2, ob = [small[i] for i in range(8)]
        fb = small[8].reshape(nz, wz)[:, :uw].reshape(-1)
        pad_cols = lambda v: take(jnp.pad(v, (0, n * hw - width)), ctx * hw, hw)
        qkv_bias = jnp.concatenate([pad_cols(qb), jnp.zeros((hw,), F32), pad_cols(vb)])

        cut = 2 if n == 8 else 1
        pieces = lambda a: a.reshape(cut, a.shape[0] // cut, a.shape[1])
        x = tokens.astype(F32)
        unit1, rstd1 = norm(x)
        qkv = (dot(h1, w_qkv) + qkv_bias).astype(BF)
        o, p = attend(qkv, inv, blk)
        mid = x + plane_scatter(n, 5, (o, w_proj, NN))[0] + pb
        unit2, rstd2 = norm(mid)
        h2, o_all = plane_gather(n, 2, pieces((unit2 * g2 + b2).astype(BF)), pieces(o))
        h2 = h2.reshape(length, width)
        hidden, slope = hidden_units(h2, w_fc, fb.reshape(1, units))
        part_out = dot(hidden, cot, TN).astype(BF)
        du, dfb = hidden_back(cot, w_out, slope)
        part_fc = dot(h2, du, TN).astype(BF)
        du, hidden, part_out, part_fc = lax.optimization_barrier((du, hidden, part_out, part_fc))
        to_owner = lambda a: lax.psum_scatter(a, "fsdp", scatter_dimension=0, tiled=True)
        sum_out, sum_fc = to_owner(part_out), to_owner(part_fc)
        dh2, summed = plane_scatter(n, 6, (du, w_fc, NT), (hidden, w_out, NN))
        layer_out = (mid + summed + ob).astype(BF)
        dmid = cotangent.astype(F32) + norm_back(dh2, unit2, rstd2, g2)
        da_own = dmid.astype(BF)
        (da,) = plane_gather(n, 3, pieces(da_own))
        da = da.reshape(length, width)
        do = dot(da, w_proj, NT).astype(BF)
        dqkv = attend_back(qkv, do, o, p, inv, blk)
        part_qkv = dot(h1, dqkv, TN).astype(BF)
        pw = width // n
        part_proj = jnp.einsum(
            "ntk,td->nkd",
            o_all.reshape(n, length, hw),
            take(da, ctx * pw, pw, 1),
            preferred_element_type=F32,
        )
        part_proj = part_proj.reshape(n * hw, pw)[:width].astype(BF)
        spare = -(3 * hw + pw) % 128
        part_attn = jnp.concatenate(
            [part_qkv, part_proj, jnp.zeros((width, spare), BF)], axis=1
        ).reshape(nz, parts, wz // parts, 3 * hw + pw + spare)
        tail_parts = lambda a: a.reshape(parts, a.shape[0] // parts, a.shape[1])
        all_fc, all_out, sum_attn, dh1 = reduce_all(
            n, nz, 9, [tail_parts(sum_fc), tail_parts(sum_out)], part_attn, dqkv, w_qkv, NT
        )
        grad_tokens = (dmid + norm_back(dh1, unit1, rstd1, g1)).astype(BF)

        col_sum = lambda a: jnp.sum(a.astype(F32), axis=0)
        put = lambda v, size: lax.dynamic_update_slice_in_dim(
            jnp.zeros((size,), F32), v, ctx * v.shape[0], 0
        )
        bias_cols = col_sum(dqkv)
        dfb = dfb.reshape(nz, uw)
        rows_of = [
            col_sum(dh1 * unit1),
            col_sum(dh1),
            put(bias_cols[:hw], n * hw)[:width],
            put(bias_cols[2 * hw :], n * hw)[:width],
            col_sum(da_own),
            col_sum(dh2 * unit2),
            col_sum(dh2),
            col_sum(cotangent),
        ]
        wide_fb = lax.dynamic_update_slice_in_dim(jnp.zeros((nz, unit_z), F32), dfb, ctx * uw, 1)
        wide_fb = jnp.pad(wide_fb, ((0, 8 - nz % 8 if nz % 8 else 0), (0, width - unit_z)))
        vectors = jnp.concatenate([jnp.stack(rows_of), wide_fb])

        all_attn, vectors = last_gather(n, nz, 4, sum_attn, vectors)
        whole_rows = lambda a: a.reshape(n, a.shape[1] * a.shape[2], a.shape[3])
        grad_fc, grad_qkv, grad_proj, grad_out = join(
            n, nz, hw, whole_rows(all_fc), whole_rows(all_attn), all_out.reshape(unit_z, width)
        )
        mine = take(vectors[:8], z * wz, wz, 1)
        gfb = take(vectors[8 : 8 + nz], z, 1).reshape(-1)[:unit_z]
        return (
            layer_out,
            grad_tokens,
            mine[0],
            mine[1],
            grad_qkv,
            mine[2],
            mine[3],
            grad_proj,
            mine[4],
            mine[5],
            mine[6],
            grad_fc,
            gfb,
            grad_out,
            mine[7],
        )

    return body


def solution(mesh):
    both = P(("fsdp", "ctx"), None)
    vec, mat = P("fsdp"), P("fsdp", None)
    placed = (both, P(), vec, vec, mat, vec, vec, mat, vec, vec, vec, mat, vec, mat, vec, both)
    outs = (both, both, vec, vec, mat, vec, vec, mat, vec, vec, vec, mat, vec, mat, vec)
    return jax.shard_map(
        make_body(mesh.shape["ctx"], mesh.shape["fsdp"]),
        mesh=mesh,
        in_specs=placed,
        out_specs=outs,
        check_vma=False,
    )
```

```python
import functools
import math

import jax
import jax.numpy as jnp
from jax import lax
from jax.experimental import pallas as pl
from jax.experimental.pallas import tpu as pltpu
from jax.sharding import PartitionSpec as P

HEADS = 25
BF = jnp.bfloat16
F32 = jnp.float32
MESH = pl.DeviceIdType.MESH
ANY = pl.BlockSpec(memory_space=pl.ANY)
VMEM = pl.BlockSpec(memory_space=pltpu.VMEM)
NN = (((1,), (0,)), ((), ()))
NT = (((1,), (1,)), ((), ()))
TN = (((0,), (0,)), ((), ()))


def dot(a, b, dims=NN):
    return lax.dot_general(a, b, dims, preferred_element_type=F32)


def places(n):
    me = lax.axis_index("ctx")
    core = lax.rem(me, 2)
    chip = me // 2
    sib = me + 1 - 2 * core
    if n == 8:
        across = chip + 1 - 2 * lax.rem(chip, 2)
        along = lax.rem(chip + 2, 4)
        first = across * (1 - core) + along * core
        second = along * (1 - core) + across * core
        others = [first, second, 3 - chip]
    else:
        half = n // 2
        others = [lax.rem(chip + d, half) for d in range(1, half)]
    return me, core, chip, sib, others


def twin(square, k):
    return 1 - k if square and k < 2 else k


def signal(sem, **device):
    pl.semaphore_signal(sem, inc=1, device_id=device, device_id_type=MESH)


def greet(devices, planes=()):
    barrier = pltpu.get_barrier_semaphore()
    for device in devices:
        signal(barrier, ctx=device)
    for plane in planes:
        signal(barrier, fsdp=plane)
    pl.semaphore_wait(barrier, len(devices) + len(planes))


def send(src, dst, ssem, rsem, **device):
    return pltpu.make_async_remote_copy(
        src_ref=src,
        dst_ref=dst,
        send_sem=ssem,
        recv_sem=rsem,
        device_id=device,
        device_id_type=MESH,
    )


def merge(*lists, scales=None):
    keyed = []
    for t, steps in enumerate(lists):
        scale = scales[t] if scales else 1.0
        keyed += [((i + 0.5) * scale / len(steps), t, i, step) for i, step in enumerate(steps)]
    for item in sorted(keyed, key=lambda k: k[:3]):
        item[3]()


class Gather:
    def __init__(self, n, src, out, sems):
        self.n, self.src, self.out = n, src, out
        self.own_s, self.sib_s, self.sib_r, self.far_s, self.far_r = sems
        self.parts = src.shape[0]
        self.square = n == 8
        self.me, self.core, self.chip, self.sib, self.others = places(n)
        half = n // 2
        if self.square:
            self.froms = self.others
        else:
            self.froms = [lax.rem(self.chip + half - d, half) for d in range(1, half)]
        self.peers = self.others[:2] if self.square else self.others
        self.started = []

    @staticmethod
    def sems(n, parts):
        dma = pltpu.SemaphoreType.DMA
        far = n // 2 - 1
        return [dma((parts,)), dma((far + 1, parts)), dma((far + 1, parts)), dma((far, parts)), dma((far, parts))]

    def own_sends(self, c):
        piece, slot = self.src.at[c], self.out.at[self.me, c]
        copies = [
            send(piece, slot, self.far_s.at[d, c], self.far_r.at[d, c], ctx=2 * p + self.core)
            for d, p in enumerate(self.peers)
        ]
        copies.append(send(piece, slot, self.sib_s.at[0, c], self.sib_r.at[0, c], ctx=self.sib))
        return copies + [pltpu.make_async_copy(piece, slot, self.own_s.at[c])]

    def go(self, copy):
        copy.start()
        self.started.append(copy)

    def start(self):
        for c in range(self.parts):
            self.start_part(c)

    def start_part(self, c):
        for copy in self.own_sends(c):
            copy.start()

    def arrived(self, d, c):
        piece = self.out.at[2 * self.froms[d] + self.core, c]
        send(piece, piece, self.far_s.at[d, c], self.far_r.at[d, c], ctx=self.sib).wait_recv()
        if self.square and d == 0:
            self.go(
                send(
                    piece,
                    piece,
                    self.far_s.at[2, c],
                    self.far_r.at[2, c],
                    ctx=2 * self.others[1] + self.core,
                )
            )
        e = twin(self.square, d) + 1
        self.go(send(piece, piece, self.sib_s.at[e, c], self.sib_r.at[e, c], ctx=self.sib))

    def steps(self):
        todo = []
        for c in range(self.parts):
            for d in range(2 if self.square else len(self.others)):
                todo.append(functools.partial(self.arrived, d, c))
            if self.square and c:
                todo.append(functools.partial(self.arrived, 2, c - 1))
        if self.square:
            todo.append(functools.partial(self.arrived, 2, self.parts - 1))
        return todo

    def finish(self):
        for c in range(self.parts):
            *far, own = self.own_sends(c)
            own.wait()
            for copy in far:
                copy.wait_send()
        for d in range(len(self.others) + 1):
            chip = self.chip if d == 0 else self.froms[d - 1]
            for c in range(self.parts):
                piece = self.out.at[2 * chip + 1 - self.core, c]
                send(
                    piece, piece, self.sib_s.at[d, c], self.sib_r.at[d, c], ctx=self.sib
                ).wait_recv()
        for copy in self.started:
            copy.wait_send()


class Relay:
    def __init__(self, nz, z, lo, hi, count, src, out, sems, lead):
        self.nz, self.z, self.lo, self.hi, self.count = nz, z, lo, hi, count
        self.src, self.out, self.lead = src, out, lead
        self.own_s, self.up_s, self.down_s, self.recv = sems

    @staticmethod
    def sems(blocks):
        return [pltpu.SemaphoreType.DMA((blocks,)) for _ in range(4)]

    def up(self, src, b):
        return send(src, self.out.at[b], self.up_s.at[b], self.recv.at[b], fsdp=self.z + 1)

    def down(self, src, b):
        return send(src, self.out.at[b], self.down_s.at[b], self.recv.at[b], fsdp=self.z - 1)

    def own(self, b):
        return pltpu.make_async_copy(self.src.at[b - self.lead], self.out.at[b], self.own_s.at[b])

    def start(self):
        lo, hi = self.lo, self.hi

        def body(i, carry):
            u, d = hi - 1 - i, lo + i

            @pl.when(self.z < self.nz - 1)
            def _():
                self.up(self.src.at[u - self.lead], u).start()

            @pl.when(self.z > 0)
            def _():
                self.down(self.src.at[d - self.lead], d).start()

            self.own(d).start()
            return carry

        lax.fori_loop(0, hi - lo, body, 0)

    def step(self, i):
        b = self.lo - 1 - i

        @pl.when(b >= 0)
        def _():
            self.up(self.out.at[b], b).wait_recv()

            @pl.when(self.z < self.nz - 1)
            def _():
                self.up(self.out.at[b], b).start()

        e = self.hi + i

        @pl.when(e < self.count)
        def _():
            self.down(self.out.at[e], e).wait_recv()

            @pl.when(self.z > 0)
            def _():
                self.down(self.out.at[e], e).start()

    def steps(self, most):
        return [functools.partial(self.step, i) for i in range(most)]

    def finish(self):
        def sent(b, carry):
            @pl.when((self.z < self.nz - 1) & (b < self.hi))
            def _():
                self.up(self.out.at[b], b).wait_send()

            @pl.when((self.z > 0) & (b >= self.lo))
            def _():
                self.down(self.out.at[b], b).wait_send()

            @pl.when((b >= self.lo) & (b < self.hi))
            def _():
                self.own(b).wait()

            return carry

        lax.fori_loop(0, self.count, sent, 0)


def others_of(z, nz):
    return [lax.rem(z + d, nz) for d in range(1, nz)]


def entry_kernel(
    n, nz, tok_t, cot_t, small, wq, wp, h1_all, cot_all, vec, wq_all, wp_all, tok, cot_own, *scratch
):
    cot, h1, inbox, zeros, small_s, small_r, zero_s = scratch[:7]
    g_h, g_c = scratch[7:12], scratch[12:17]
    r_q, r_p = scratch[17:21], scratch[21:25]
    me, core, chip, sib, others = places(n)
    z = lax.axis_index("fsdp")
    planes = others_of(z, nz)
    greet([sib] + [2 * p + core for p in (others[:2] if n == 8 else others)], planes)
    wz = small.shape[1]
    for d, plane in enumerate(planes):
        send(small, inbox.at[z], small_s.at[d], small_r.at[d], fsdp=plane).start()
    inbox[z] = small[...]
    k = wq.shape[0]
    relay_q = Relay(nz, z, z * k, (z + 1) * k, nz * k, wq, wq_all, r_q, z * k)
    relay_q.start()
    parts, rows = h1.shape[0], h1.shape[1]
    turned = cot_t[...].astype(F32).T.astype(BF)
    cot_own[...] = turned
    for c in range(parts):
        cot[c] = turned[c * rows : (c + 1) * rows, :]
    gather_c = Gather(n, cot, cot_all, g_c)
    gather_c.start()
    tok[...] = tok_t[...].astype(F32).T.astype(BF)
    share, blocks = wp.shape[0], wp_all.shape[0]
    base = me * blocks
    valid = jnp.clip(nz * share - base, 0, blocks)
    lo = jnp.clip(z * share - base, 0, valid)
    hi = jnp.clip((z + 1) * share - base, 0, valid)
    relay_p = Relay(nz, z, lo, hi, valid, wp, wp_all, r_p, z * share - base)
    relay_p.start()
    zeros[...] = jnp.zeros_like(zeros)

    def clear(b, carry):
        pltpu.make_async_copy(zeros, wp_all.at[b], zero_s.at[b]).start()
        return carry

    lax.fori_loop(valid, blocks, clear, 0)
    for d in range(nz - 1):
        came = lax.rem(z + nz - 1 - d, nz)
        send(small, inbox.at[came], small_s.at[d], small_r.at[d], fsdp=planes[d]).wait_recv()
    for p in range(nz):
        vec[:, p * wz : (p + 1) * wz] = inbox[p].astype(F32)
    gain, shift = vec[0:1, :], vec[1:2, :]
    gather_h = Gather(n, h1, h1_all, g_h)
    for c in range(parts):
        unit, _ = norm(tok[c * rows : (c + 1) * rows, :].astype(F32))
        h1[c] = (unit * gain + shift).astype(BF)
        gather_h.start_part(c)
    merge(
        gather_c.steps() + gather_h.steps(),
        relay_q.steps(nz * k - k) + relay_p.steps(blocks),
    )
    gather_c.finish()
    gather_h.finish()
    relay_q.finish()
    relay_p.finish()

    def cleared(b, carry):
        pltpu.make_async_copy(zeros, wp_all.at[b], zero_s.at[b]).wait()
        return carry

    lax.fori_loop(valid, blocks, cleared, 0)
    for d, plane in enumerate(planes):
        send(small, inbox.at[z], small_s.at[d], small_r.at[d], fsdp=plane).wait_send()


def entry(n, nz, tokens, cot, small, wq, wp, hw):
    rows, width = tokens.shape
    parts = 2 if n == 8 else 1
    dma = pltpu.SemaphoreType.DMA
    k, tile = wq.shape[0], wp.shape[1]
    blocks = hw // tile
    shape = jax.ShapeDtypeStruct
    piece = (parts, rows // parts, width)
    return pl.pallas_call(
        functools.partial(entry_kernel, n, nz),
        out_shape=[
            shape((n,) + piece, BF),
            shape((n,) + piece, BF),
            shape((small.shape[0], width), F32),
            shape((nz * k,) + wq.shape[1:], BF),
            shape((blocks, tile, width), BF),
            shape((rows, width), BF),
            shape((rows, width), BF),
        ],
        in_specs=[VMEM] * 5,
        out_specs=[ANY, ANY, VMEM, ANY, ANY, VMEM, VMEM],
        scratch_shapes=[
            pltpu.VMEM(piece, BF),
            pltpu.VMEM(piece, BF),
            pltpu.VMEM((nz,) + small.shape, BF),
            pltpu.VMEM((tile, width), BF),
            dma((nz - 1,)),
            dma((nz - 1,)),
            dma((blocks,)),
        ]
        + Gather.sems(n, parts)
        + Gather.sems(n, parts)
        + Relay.sems(nz * k)
        + Relay.sems(blocks),
        compiler_params=pltpu.CompilerParams(collective_id=1, has_side_effects=True),
        name="entry",
    )(tokens.T, cot.T, small, wq, wp)


class Scatter:
    def __init__(self, n, dims, a, w, scratch):
        self.n, self.dims, self.a, self.w = n, dims, a, w
        self.part, self.theirs, self.sums, self.inbox = scratch[:4]
        self.sib_s, self.sib_r, self.far_s, self.far_r = scratch[4:]
        self.me, self.core, self.chip, self.sib, self.others = places(n)
        self.square = n == 8
        self.half = n // 2
        self.parts = self.sib_s.shape[1]
        self.full = self.part.shape[2]
        self.rows = self.full // self.parts
        if self.square:
            first, second = [2 * p + self.core for p in self.others[:2]]
            self.ends = [(0, 0, first), (1, 1, first), (2, 2, second)]
        else:
            self.ends = [(k, k, 2 * self.others[k] + self.core) for k in range(self.half - 1)]

    @staticmethod
    def scratch(n, rows, width):
        dma = pltpu.SemaphoreType.DMA
        half, parts = n // 2, 4 if n == 8 else 1
        return [
            pltpu.VMEM((half, 2, rows, width), BF),
            pltpu.VMEM((half, rows, width), BF),
            pltpu.VMEM((half - 1, rows, width), BF),
            pltpu.VMEM((half - 1, rows, width), BF),
            dma((half, parts)),
            dma((half, parts)),
            dma((half - 1, parts)),
            dma((half - 1, parts)),
        ]

    def chip_at(self, k):
        if not self.square:
            return lax.rem(self.chip + 1 + k, self.half)
        x, y = lax.rem(self.chip, 2), self.chip // 2
        first, second = 1 - lax.rem(k, 3) // 2, 1 - lax.rem(k, 2)
        dx = first * (1 - self.core) + second * self.core
        dy = second * (1 - self.core) + first * self.core
        far = (k < 3).astype(jnp.int32)
        dx, dy = dx * far, dy * far
        return (y + dy - 2 * y * dy) * 2 + x + dx - 2 * x * dx

    def twin_at(self, k):
        if not self.square:
            return k
        return k + jnp.where(k == 1, 1, 0) - jnp.where(k == 2, 1, 0)

    def win(self, c):
        return pl.ds(c * self.rows, self.rows)

    def to_sib(self, k, c):
        e = self.twin_at(k)
        return send(
            self.part.at[k, 1 - self.core, self.win(c)],
            self.theirs.at[e, self.win(c)],
            self.sib_s.at[e, c],
            self.sib_r.at[e, c],
            ctx=self.sib,
        )

    def chip_sum(self, k, c):
        win = self.win(c)
        piece = self.theirs.at[k, win]
        send(piece, piece, self.sib_s.at[k, c], self.sib_r.at[k, c], ctx=self.sib).wait_recv()
        return self.part[k, self.core, win, :].astype(F32) + self.theirs[k, win, :].astype(F32)

    def pass_on(self, k, slot, peer, c):
        return send(
            self.sums.at[k, self.win(c)],
            self.inbox.at[slot, self.win(c)],
            self.far_s.at[slot, c],
            self.far_r.at[slot, c],
            ctx=peer,
        )

    def wait_in(self, slot, c):
        piece = self.inbox.at[slot, self.win(c)]
        send(piece, piece, self.far_s.at[slot, c], self.far_r.at[slot, c], ctx=self.sib).wait_recv()
        return self.inbox[slot, self.win(c), :].astype(F32)

    def forward(self, end, c):
        k, slot, peer = self.ends[end]
        total = self.chip_sum(k, c)
        if self.square and end == 2:
            total = total + self.wait_in(0, c)
        self.sums[k, self.win(c), :] = total.astype(BF)
        self.pass_on(k, slot, peer, c).start()

    def products(self):
        def product(k, carry):
            full = self.full
            at = pl.ds(pl.multiple_of(self.chip_at(k) * 2 * full, 2 * full), 2 * full)
            val = dot(self.a[at, :], self.w[...], self.dims).astype(BF)
            self.part[k, 0] = val[:full]
            self.part[k, 1] = val[full:]
            for c in range(self.parts):
                self.to_sib(k, c).start()

            @pl.when(k == 1)
            def _():
                for c in range(self.parts):
                    self.forward(0, c)

            return carry

        lax.fori_loop(0, self.half, product, 0)

    def forwards(self):
        each = range(self.parts)
        return [functools.partial(self.forward, e, c) for e in range(1, self.half - 1) for c in each]

    def total(self, c):
        val = self.chip_sum(self.half - 1, c)
        for slot in (1, 2) if self.square else range(self.half - 1):
            val = val + self.wait_in(slot, c)
        return val

    def finish(self):
        for c in range(self.parts):
            for k, slot, peer in self.ends:
                self.pass_on(k, slot, peer, c).wait_send()

        def sent(k, carry):
            for c in range(self.parts):
                self.to_sib(k, c).wait_send()
            return carry

        lax.fori_loop(0, self.half, sent, 0)


class Line:
    def __init__(self, nz, z, src, out, scratch):
        self.nz, self.z, self.src, self.out = nz, z, src, out
        self.mine, self.above, self.below, self.load_s, self.up_s, self.down_s, self.recv = scratch
        self.parts = src.shape[1]

    @staticmethod
    def scratch(shape):
        dma, lead = pltpu.SemaphoreType.DMA, shape[:2]
        return [pltpu.VMEM(shape, BF)] * 3 + [dma((1,)), dma(lead), dma(lead), dma((2,) + lead)]

    def up(self, src, d, c):
        return send(
            src.at[d, c], self.above.at[d, c], self.up_s.at[d, c], self.recv.at[0, d, c], fsdp=self.z + 1
        )

    def down(self, src, d, c):
        return send(
            src.at[d, c], self.below.at[d, c], self.down_s.at[d, c], self.recv.at[1, d, c], fsdp=self.z - 1
        )

    def start(self):
        for d in range(self.nz - 1, 0, -1):

            @pl.when(self.z == 0)
            def _():
                for c in range(self.parts):
                    self.up(self.src, d, c).start()

            @pl.when(self.z == self.nz - 1)
            def _():
                for c in range(self.parts):
                    self.down(self.src, self.nz - 1 - d, c).start()

        self.load = pltpu.make_async_copy(self.src, self.mine, self.load_s.at[0])
        self.load.start()

    def loaded(self):
        self.load.wait()

    def pass_up(self, d, c):
        copy = self.up(self.mine, d, c)
        copy.wait_recv()
        self.mine[d, c] = self.mine[d, c] + self.above[d, c]
        copy.start()

    def pass_down(self, d, c):
        copy = self.down(self.mine, d, c)
        copy.wait_recv()
        self.mine[d, c] = self.mine[d, c] + self.below[d, c]
        copy.start()

    def settle(self, place, c):
        z, top = place, self.nz - 1
        total = self.mine[z, c].astype(F32)
        if z > 0:
            self.up(self.mine, z, c).wait_recv()
            total = total + self.above[z, c].astype(F32)
        if z < top:
            self.down(self.mine, z, c).wait_recv()
            total = total + self.below[z, c].astype(F32)
        self.out[c] = total.astype(BF)

    def steps(self, after=None):
        top, parts = self.nz - 1, self.parts
        slots = {}

        def put(time, place, fn):
            slots.setdefault(time, {}).setdefault(place, []).append(fn)

        for place in range(self.nz):
            for k in range(1, self.nz):
                for c in range(parts):
                    at = (k - 1) * parts + c
                    if 0 < place < top - k + 1:
                        put(at + place, place, functools.partial(self.pass_up, top - k + 1, c))
                    if k - 1 < place < top:
                        put(at + top - place, place, functools.partial(self.pass_down, k - 1, c))
            for c in range(parts):
                up = (top - place) * parts + c + place if place > 0 else 0
                down = place * parts + c + top - place if place < top else 0
                put(max(up, down), place, functools.partial(self.settle, place, c))
                if after:
                    put(max(up, down), place, functools.partial(after, c))

        def run(work):
            for place, fns in sorted(work.items()):

                @pl.when(self.z == place)
                def _():
                    for fn in fns:
                        fn()

        return [self.loaded] + [functools.partial(run, slots[t]) for t in sorted(slots)]

    def finish(self):
        for d in range(self.nz):

            @pl.when(self.z < d)
            def _():
                for c in range(self.parts):
                    self.up(self.mine, d, c).wait_send()

            @pl.when(self.z > d)
            def _():
                for c in range(self.parts):
                    self.down(self.mine, d, c).wait_send()


class Vectors:
    def __init__(self, n, nz, src, out, scratch):
        self.n, self.nz, self.src, self.out = n, nz, src, out
        self.from_sib, self.chips, self.line = scratch[:3]
        self.ss, self.sr, self.cs, self.cr, self.ls, self.lr = scratch[3:]
        self.me, self.core, self.chip, self.sib, self.others = places(n)
        self.z = lax.axis_index("fsdp")
        self.planes = others_of(self.z, nz)

    @staticmethod
    def scratch(n, nz, shape):
        dma = pltpu.SemaphoreType.DMA
        half = n // 2
        return [
            pltpu.VMEM(shape, F32),
            pltpu.VMEM((half,) + shape, F32),
            pltpu.VMEM((nz,) + shape, F32),
            dma((1,)),
            dma((1,)),
            dma((half - 1,)),
            dma((half - 1,)),
            dma((nz - 1,)),
            dma((nz - 1,)),
        ]

    def to_sib(self):
        return send(self.src, self.from_sib, self.ss.at[0], self.sr.at[0], ctx=self.sib)

    def to_chip(self, d):
        at = self.chips.at[self.chip]
        return send(at, at, self.cs.at[d], self.cr.at[d], ctx=2 * self.others[d] + self.core)

    def to_plane(self, d):
        at = self.line.at[self.z]
        return send(at, at, self.ls.at[d], self.lr.at[d], fsdp=self.planes[d])

    def start(self):
        self.to_sib().start()

    def first(self):
        self.to_sib().wait_recv()
        self.chips[self.chip] = self.src[...] + self.from_sib[...]
        for d in range(self.n // 2 - 1):
            self.to_chip(d).start()

    def second(self):
        for d in range(self.n // 2 - 1):
            self.to_chip(d).wait_recv()
        total = self.chips[0]
        for k in range(1, self.n // 2):
            total = total + self.chips[k]
        self.line[self.z] = total
        for d in range(self.nz - 1):
            self.to_plane(d).start()

    def third(self):
        for d in range(self.nz - 1):
            self.to_plane(d).wait_recv()
        total = self.line[0]
        for k in range(1, self.nz):
            total = total + self.line[k]
        self.out[...] = total

    def steps(self):
        return [self.first, self.second, self.third]

    def finish(self):
        self.to_sib().wait_send()
        for d in range(self.n // 2 - 1):
            self.to_chip(d).wait_send()
        for d in range(self.nz - 1):
            self.to_plane(d).wait_send()


def beside(n):
    me, core, chip, sib, others = places(n)
    return [sib] + [2 * p + core for p in (others[:2] if n == 8 else others)]


def call(kernel, cid, name, ins, in_specs, outs, out_specs, scratch):
    return pl.pallas_call(
        kernel,
        out_shape=[jax.ShapeDtypeStruct(*o) for o in outs],
        in_specs=in_specs,
        out_specs=out_specs,
        scratch_shapes=scratch,
        compiler_params=pltpu.CompilerParams(
            collective_id=cid, has_side_effects=True, vmem_limit_bytes=60 * 1024 * 1024
        ),
        name=name,
    )(*ins)


def middle_kernel(n, o, w, tok, vec, mid, h2_all, h2, *scratch):
    greet(beside(n))
    scatter = Scatter(n, NN, o, w, scratch[:8])
    gather = Gather(n, h2, h2_all, scratch[8:])
    scatter.products()
    for step in scatter.forwards():
        step()
    for c in range(gather.parts):
        win = scatter.win(c)
        val = tok[win, :].astype(F32) + scatter.total(c) + vec[4:5, :]
        mid[win, :] = val
        h2[c] = (norm(val)[0] * vec[5:6, :] + vec[6:7, :]).astype(BF)
        gather.start_part(c)
    for step in gather.steps():
        step()
    gather.finish()
    scatter.finish()


def middle(n, cid, o, w, tok, vec):
    rows, width = tok.shape
    parts = 4 if n == 8 else 1
    piece = (parts, rows // parts, width)
    return call(
        functools.partial(middle_kernel, n),
        cid,
        "middle",
        (o, w, tok, vec),
        [VMEM] * 4,
        [((rows, width), F32), ((n,) + piece, BF)],
        [VMEM, ANY],
        [pltpu.VMEM(piece, BF)] + Scatter.scratch(n, rows, width) + Gather.sems(n, parts),
    )


def spread_kernel(n, src, all_ref, *sems):
    greet(beside(n))
    gather = Gather(n, src, all_ref, sems)
    gather.start()
    for step in gather.steps():
        step()
    gather.finish()


def spread(n, cid, array):
    return call(
        functools.partial(spread_kernel, n),
        cid,
        "spread",
        (array,),
        [VMEM],
        [((n,) + array.shape, BF)],
        [ANY],
        Gather.sems(n, array.shape[0]),
    )[0]


def turn_kernel(n, du, w_fc, hid, w_out, mid, cot, vec, da_all, dmid, layer, sums, da, *scratch):
    greet(beside(n))
    back = Scatter(n, NT, du, w_fc, scratch[:8])
    ahead = Scatter(n, NN, hid, w_out, scratch[8:16])
    gather = Gather(n, da, da_all, scratch[16:])
    back.products()
    todo = back.forwards()
    for step in todo[: back.parts]:
        step()
    ahead.products()
    for step in todo[back.parts :]:
        step()
    sums[...] = jnp.zeros_like(sums)
    for c in range(gather.parts):
        win = back.win(c)
        grad = back.total(c)
        unit, rstd = norm(mid[win, :])
        up = cot[win, :].astype(F32)
        val = up + norm_back(grad, unit, rstd, vec[5:6, :])
        dmid[win, :] = val
        low = val.astype(BF)
        da[c] = low
        gather.start_part(c)
        for row, term in ((4, low.astype(F32)), (5, grad * unit), (6, grad), (7, up)):
            sums[row : row + 1, :] += jnp.sum(term, axis=0, keepdims=True)
    merge(gather.steps(), ahead.forwards())
    for c in range(gather.parts):
        win = ahead.win(c)
        layer[win, :] = (mid[win, :] + ahead.total(c) + vec[7:8, :]).astype(BF)
    gather.finish()
    back.finish()
    ahead.finish()


def turn(n, cid, du, w_fc, hidden, w_out, mid, cot, vec):
    rows, width = mid.shape
    parts = 4 if n == 8 else 1
    piece = (parts, rows // parts, width)
    return call(
        functools.partial(turn_kernel, n),
        cid,
        "turn",
        (du, w_fc, hidden, w_out, mid, cot, vec),
        [VMEM] * 7,
        [((n,) + piece, BF), ((rows, width), F32), ((rows, width), BF), ((8, width), F32)],
        [ANY, VMEM, VMEM, VMEM],
        [pltpu.VMEM(piece, BF)]
        + Scatter.scratch(n, rows, width)
        + Scatter.scratch(n, rows, width)
        + Gather.sems(n, parts),
    )


def tail_kernel(
    n, nz, fc, out, part, dqkv, w_qkv, tok, dmid, vec, v_in, fc_all, out_all, attn_all, g_tok, v_out,
    v_own, attn, *scratch,
):
    z = lax.axis_index("fsdp")
    me, core, chip, sib, others = places(n)
    greet([sib] + [2 * p + core for p in others], others_of(z, nz))
    line = Line(nz, z, part, attn, scratch[:7])
    line.start()
    scatter = Scatter(n, NT, dqkv, w_qkv, scratch[7:15])
    vectors = Vectors(n, nz, v_own, v_out, scratch[15:24])
    fc_g = Gather(n, fc, fc_all, scratch[24:29])
    out_g = Gather(n, out, out_all, scratch[29:34])
    attn_g = Gather(n, attn, attn_all, scratch[34:39])
    v_own[...] = v_in[...]
    scatter.products()
    todo = scatter.forwards()
    for step in todo[: scatter.parts]:
        step()
    fc_g.start()

    def rest(c):
        win = scatter.win(c)
        grad = scatter.total(c)
        unit, rstd = norm(tok[win, :].astype(F32))
        g_tok[win, :] = (dmid[win, :] + norm_back(grad, unit, rstd, vec[0:1, :])).astype(BF)
        v_own[0:1, :] += jnp.sum(grad * unit, axis=0, keepdims=True)
        v_own[1:2, :] += jnp.sum(grad, axis=0, keepdims=True)

    first = todo[scatter.parts :] + [functools.partial(rest, c) for c in range(scatter.parts)]
    first += [vectors.start, vectors.first, vectors.second]
    fc_steps = fc_g.steps()
    half = len(fc_steps) // 2
    second = fc_steps[:half] + [out_g.start] + fc_steps[half:] + out_g.steps()
    third = line.steps(attn_g.start_part)
    merge(first, second, third, scales=(0.6, 1.0, 0.9))
    for step in attn_g.steps() + [vectors.third]:
        step()
    for job in (fc_g, out_g, attn_g, scatter, line, vectors):
        job.finish()


def tail(n, nz, cid, fc, out, part, dqkv, w_qkv, tok, dmid, vec, v_in):
    rows, width = tok.shape
    attn = part.shape[1:]
    return call(
        functools.partial(tail_kernel, n, nz),
        cid,
        "tail",
        (fc, out, part, dqkv, w_qkv, tok, dmid, vec, v_in),
        [VMEM, VMEM, ANY] + [VMEM] * 6,
        [((n,) + fc.shape, BF), ((n,) + out.shape, BF), ((n,) + attn, BF), (tok.shape, BF), (v_in.shape, F32)],
        [ANY, ANY, ANY, VMEM, VMEM],
        [pltpu.VMEM(v_in.shape, F32), pltpu.VMEM(attn, BF)]
        + Line.scratch(part.shape)
        + Scatter.scratch(n, rows, width)
        + Vectors.scratch(n, nz, v_in.shape)
        + Gather.sems(n, fc.shape[0])
        + Gather.sems(n, out.shape[0])
        + Gather.sems(n, attn[0]),
    )


def outer_kernel(x_ref, y_ref, out_ref):
    out_ref[...] = dot(x_ref[...], y_ref[...], TN).astype(BF)


def outer(x, y):
    rows, m = x.shape
    tile = 256
    return pl.pallas_call(
        outer_kernel,
        grid=(pl.cdiv(m, tile),),
        out_shape=jax.ShapeDtypeStruct((m, y.shape[1]), BF),
        in_specs=[pl.BlockSpec((rows, tile), lambda i: (0, i)), fixed(*y.shape)],
        out_specs=tiled(tile, y.shape[1]),
        name="outer",
    )(x, y)


def attn_outer_kernel(x_ref, y_ref, o_ref, a_ref, out_ref):
    cols, pw = y_ref.shape[1], a_ref.shape[1]
    out_ref[:, :cols] = dot(x_ref[...], y_ref[...], TN).astype(BF)
    out_ref[:, cols : cols + pw] = dot(o_ref[0], a_ref[...], TN).astype(BF)
    out_ref[:, cols + pw :] = jnp.zeros((out_ref.shape[0], out_ref.shape[1] - cols - pw), BF)


def attn_outer(h1, dqkv, o_all, da_cols):
    rows, m = h1.shape
    tile = o_all.shape[2]
    cols, pw = dqkv.shape[1], da_cols.shape[1]
    total = -(-(cols + pw) // 128) * 128
    return pl.pallas_call(
        attn_outer_kernel,
        grid=(pl.cdiv(m, tile),),
        out_shape=jax.ShapeDtypeStruct((m, total), BF),
        in_specs=[
            pl.BlockSpec((rows, tile), lambda i: (0, i)),
            fixed(rows, cols),
            pl.BlockSpec((1, rows, tile), lambda i: (i, 0, 0)),
            fixed(rows, pw),
        ],
        out_specs=tiled(tile, total),
        name="attn_outer",
    )(h1, dqkv, o_all, da_cols)


def hidden_kernel(h_ref, w_ref, b_ref, z_ref, s_ref):
    u = dot(h_ref[...], w_ref[...]) + b_ref[...]
    root = 0.7978845608028654
    square = u * u
    inner = jnp.tanh(root * u * (1.0 + 0.044715 * square))
    z_ref[...] = (0.5 * u * (1.0 + inner)).astype(BF)
    slope = 0.5 * (1.0 + inner) + 0.5 * u * (1.0 - inner * inner) * root * (1.0 + 3 * 0.044715 * square)
    s_ref[...] = slope.astype(BF)


def hidden_back_kernel(c_ref, w_ref, s_ref, d_ref, sum_ref):
    du = (dot(c_ref[...], w_ref[...], NT) * s_ref[...].astype(F32)).astype(BF)
    d_ref[...] = du

    @pl.when(pl.program_id(0) == 0)
    def _():
        sum_ref[...] = jnp.zeros_like(sum_ref)

    sum_ref[...] += jnp.sum(du.astype(F32), axis=0, keepdims=True)


def tiled(rows, cols):
    return pl.BlockSpec((rows, cols), lambda i: (i, 0))


def fixed(rows, cols):
    return pl.BlockSpec((rows, cols), lambda i: (0, 0))


def hidden_units(h2, w_fc, bias):
    rows, width = h2.shape
    units = w_fc.shape[1]
    tile = 256
    shape = jax.ShapeDtypeStruct((rows, units), BF)
    return pl.pallas_call(
        hidden_kernel,
        grid=(rows // tile,),
        out_shape=[shape, shape],
        in_specs=[tiled(tile, width), fixed(width, units), fixed(1, units)],
        out_specs=[tiled(tile, units), tiled(tile, units)],
        name="hidden",
    )(h2, w_fc, bias)


def hidden_back(cot, w_out, slope):
    rows, width = cot.shape
    units = w_out.shape[0]
    tile = 256
    return pl.pallas_call(
        hidden_back_kernel,
        grid=(rows // tile,),
        out_shape=[
            jax.ShapeDtypeStruct((rows, units), BF),
            jax.ShapeDtypeStruct((1, units), F32),
        ],
        in_specs=[tiled(tile, width), fixed(units, width), tiled(tile, units)],
        out_specs=[tiled(tile, units), fixed(1, units)],
        name="hidden_back",
    )(cot, w_out, slope)


def join_kernel(n, nz, hw, width, fc, qp, out, fc_o, qkv_o, proj_o, out_o):
    uw = fc.shape[-1] // nz
    pw = width // n
    for c in range(n):
        for b in range(nz):
            at = b * n * uw + c * uw
            fc_o[:, at : at + uw] = fc[c, 0, :, b * uw : (b + 1) * uw].astype(F32)
        proj_o[:, c * pw : (c + 1) * pw] = qp[c, 0, :, 3 * hw : 3 * hw + pw].astype(F32)
        size = min(hw, width - c * hw)
        if size > 0:
            for t in range(3):
                at = t * width + c * hw
                qkv_o[:, at : at + size] = qp[c, 0, :, t * hw : t * hw + size].astype(F32)
    out_o[...] = out[...].astype(F32)


def join(n, nz, hw, fc, qp, out):
    tiles = 25
    width = out.shape[1]
    wz = fc.shape[1]
    split = lambda a: a.reshape(n, tiles, wz // tiles, a.shape[-1])
    fc, qp = split(fc), split(qp)
    wide = lambda a: pl.BlockSpec((n, 1, wz // tiles, a.shape[-1]), lambda i: (0, i, 0, 0))
    t, ot = wz // tiles, out.shape[0] // tiles
    cols = (nz * out.shape[0], 3 * width, width)
    shape = jax.ShapeDtypeStruct
    return pl.pallas_call(
        functools.partial(join_kernel, n, nz, hw, width),
        grid=(tiles,),
        out_shape=[shape((wz, c), F32) for c in cols] + [shape(out.shape, F32)],
        in_specs=[wide(fc), wide(qp), tiled(ot, width)],
        out_specs=[tiled(t, c) for c in cols] + [tiled(ot, width)],
        name="join",
    )(fc, qp, out)


def attend_kernel(blocks, blk, tile, inv_ref, q_ref, k_ref, v_ref, o_ref, p_ref, qn, kn, vn, ot):
    length = blocks * blk
    for i in range(blocks):
        src, dst = pl.ds(pl.multiple_of(inv_ref[i] * blk, blk), blk), pl.ds(i * blk, blk)
        qn[dst, :] = q_ref[src, :]
        kn[dst, :] = k_ref[src, :]
        vn[dst, :] = v_ref[src, :]
    v_turned = vn[...].astype(F32).T.astype(BF)
    lane = lax.broadcasted_iota(jnp.int32, (1, 128), 1)
    above = lax.broadcasted_iota(jnp.int32, (tile, tile), 0) > lax.broadcasted_iota(
        jnp.int32, (tile, tile), 1
    )
    for i in range(length // tile):
        cols = pl.ds(i * tile, tile)
        keys = (i + 1) * tile
        for h in range(2):
            here = (lane // 64) == h
            q = jnp.where(here, qn[cols, :].astype(F32) * 0.125, 0.0).astype(BF)
            last = jnp.where(above, -1e30, dot(kn[pl.ds(i * tile, tile), :], q, NT))
            top = jnp.max(last, axis=0, keepdims=True)
            if i:
                early = dot(kn[pl.ds(0, i * tile), :], q, NT)
                top = jnp.maximum(top, jnp.max(early, axis=0, keepdims=True))
            last = jnp.exp(last - top)
            total = jnp.sum(last, axis=0, keepdims=True)
            if i:
                early = jnp.exp(early - top)
                total = total + jnp.sum(early, axis=0, keepdims=True)
            scale = 1.0 / total
            last = (last * scale).astype(BF)
            p_ref[h, pl.ds(i * tile, tile), cols] = last
            half = slice(64 * h, 64 * h + 64)
            o = dot(v_turned[half, i * tile : keys], last)
            if i:
                early = (early * scale).astype(BF)
                p_ref[h, pl.ds(0, i * tile), cols] = early
                o = o + dot(v_turned[half, : i * tile], early)
            ot[half, cols] = o
    o_nat = ot[...].T
    for i in range(blocks):
        o_ref[pl.ds(pl.multiple_of(inv_ref[i] * blk, blk), blk), :] = o_nat[
            i * blk : (i + 1) * blk, :
        ].astype(BF)


def attend(qkv, inv, blk):
    length = qkv.shape[0]
    cols = qkv.shape[1] // 3
    pairs = cols // 128
    blocks = inv.shape[0]
    tile = 256
    piece = lambda off: pl.BlockSpec((length, 128), lambda p, s: (0, off * pairs + p))
    return pl.pallas_call(
        functools.partial(attend_kernel, blocks, blk, tile),
        out_shape=[
            jax.ShapeDtypeStruct((length, cols), BF),
            jax.ShapeDtypeStruct((2 * pairs, length, length), BF),
        ],
        grid_spec=pltpu.PrefetchScalarGridSpec(
            num_scalar_prefetch=1,
            grid=(pairs,),
            in_specs=[piece(0), piece(1), piece(2)],
            out_specs=[
                pl.BlockSpec((length, 128), lambda p, s: (0, p)),
                pl.BlockSpec((2, length, length), lambda p, s: (p, 0, 0)),
            ],
            scratch_shapes=[
                pltpu.VMEM((length, 128), BF),
                pltpu.VMEM((length, 128), BF),
                pltpu.VMEM((length, 128), BF),
                pltpu.VMEM((128, length), F32),
            ],
        ),
        compiler_params=pltpu.CompilerParams(vmem_limit_bytes=60 * 1024 * 1024),
        name="attend",
    )(inv, qkv, qkv, qkv)


def attend_back_kernel(
    blocks, blk, tile, pairs, inv_ref, q_ref, k_ref, v_ref, g_ref, o_ref, p_ref, out_ref, sum_ref,
    qn, kn, vn, gn, on, dqt, dk, dv,
):
    length = blocks * blk
    for i in range(blocks):
        src, dst = pl.ds(pl.multiple_of(inv_ref[i] * blk, blk), blk), pl.ds(i * blk, blk)
        qn[dst, :] = q_ref[src, :]
        kn[dst, :] = k_ref[src, :]
        vn[dst, :] = v_ref[src, :]
        gn[dst, :] = g_ref[src, :]
        on[dst, :] = o_ref[src, :]
    k_turned = kn[...].astype(F32).T.astype(BF)
    prod = (gn[...].astype(F32) * on[...].astype(F32)).T
    deltas = [jnp.sum(prod[64 * h : 64 * h + 64, :], axis=0, keepdims=True) for h in range(2)]
    lane = lax.broadcasted_iota(jnp.int32, (1, 128), 1)
    dk[...] = jnp.zeros_like(dk)
    dv[...] = jnp.zeros_like(dv)
    for i in range(length // tile):
        cols = pl.ds(i * tile, tile)
        keys = (i + 1) * tile
        for h in range(2):
            here = (lane // 64) == h
            q = jnp.where(here, qn[cols, :].astype(F32), 0.0).astype(BF)
            g = jnp.where(here, gn[cols, :].astype(F32), 0.0).astype(BF)
            p = p_ref[h, pl.ds(0, keys), cols]
            dp = dot(vn[pl.ds(0, keys), :], g, NT)
            ds = (
                p.astype(F32) * (dp - deltas[h][:, i * tile : (i + 1) * tile]) * 0.125
            ).astype(BF)
            half = slice(64 * h, 64 * h + 64)
            dqt[half, cols] = dot(k_turned[half, :keys], ds)
            dk[pl.ds(0, keys), :] += dot(ds, q)
            dv[pl.ds(0, keys), :] += dot(p, g)
    dq = dqt[...].T
    pair = pl.program_id(0)
    for t, val in enumerate((dq, dk[...], dv[...])):
        at = pl.ds(pl.multiple_of((t * pairs + pair) * 128, 128), 128)
        sum_ref[:, at] = jnp.sum(val.astype(BF).astype(F32), axis=0, keepdims=True)
    for i in range(blocks):
        dst = pl.ds(pl.multiple_of(inv_ref[i] * blk, blk), blk)
        src = slice(i * blk, (i + 1) * blk)
        for t, val in enumerate((dq, dk, dv)):
            at = pl.ds(pl.multiple_of((t * pairs + pair) * 128, 128), 128)
            out_ref[dst, at] = val[src, :].astype(BF)


def attend_back(qkv, grad, o, p, inv, blk):
    length = qkv.shape[0]
    cols = qkv.shape[1] // 3
    pairs = cols // 128
    blocks = inv.shape[0]
    tile = 256
    piece = lambda off: pl.BlockSpec((length, 128), lambda i, s: (0, off * pairs + i))
    return pl.pallas_call(
        functools.partial(attend_back_kernel, blocks, blk, tile, pairs),
        out_shape=[
            jax.ShapeDtypeStruct((length, 3 * cols), BF),
            jax.ShapeDtypeStruct((1, 3 * cols), F32),
        ],
        grid_spec=pltpu.PrefetchScalarGridSpec(
            num_scalar_prefetch=1,
            grid=(pairs,),
            in_specs=[
                piece(0),
                piece(1),
                piece(2),
                piece(0),
                piece(0),
                pl.BlockSpec((2, length, length), lambda i, s: (i, 0, 0)),
            ],
            out_specs=[
                pl.BlockSpec((length, 3 * cols), lambda i, s: (0, 0)),
                pl.BlockSpec((1, 3 * cols), lambda i, s: (0, 0)),
            ],
            scratch_shapes=[pltpu.VMEM((length, 128), BF)] * 5
            + [
                pltpu.VMEM((128, length), F32),
                pltpu.VMEM((length, 128), F32),
                pltpu.VMEM((length, 128), F32),
            ],
        ),
        compiler_params=pltpu.CompilerParams(vmem_limit_bytes=60 * 1024 * 1024),
        name="attend_back",
    )(inv, qkv, qkv, qkv, grad, o, p)


def norm(values):
    centre = values - jnp.mean(values, axis=-1, keepdims=True)
    rstd = lax.rsqrt(jnp.mean(centre * centre, axis=-1, keepdims=True) + 1e-05)
    return centre * rstd, rstd


def norm_back(grad, unit, rstd, gain):
    inner = grad * gain
    return rstd * (
        inner
        - jnp.mean(inner, axis=-1, keepdims=True)
        - unit * jnp.mean(inner * unit, axis=-1, keepdims=True)
    )


def make_body(n, nz):
    def body(
        tokens, block_table, ln1_gain, ln1_bias, qkv_weight, query_bias, value_bias,
        proj_weight, proj_bias, ln2_gain, ln2_bias, fc_weight, fc_bias, out_weight,
        out_bias, cotangent,
    ):
        ctx = lax.axis_index("ctx")
        z = lax.axis_index("fsdp")
        rows, width = tokens.shape
        blk = rows // 2
        wz = width // nz
        slots = -(-HEADS // n)
        hw = slots * (width // HEADS)
        unit_z = out_weight.shape[0]
        uw = unit_z // n
        units = uw * nz
        table = block_table.reshape(-1)
        inv = jnp.argmax(
            table[None, :] == jnp.arange(table.shape[0], dtype=table.dtype)[:, None], axis=1
        ).astype(jnp.int32)

        take = lambda a, at, size, axis=0: lax.dynamic_slice_in_dim(a, at, size, axis)
        parts = 5
        padded = jnp.pad(qkv_weight, ((0, 0), (0, n * hw - width)))
        wq_own = jnp.concatenate(
            [take(padded, t * width + ctx * hw, hw, 1) for t in range(3)], axis=1
        ).reshape(parts, wz // parts, 3 * hw)
        row = lax.broadcasted_iota(jnp.int32, (16, wz), 0)
        small = jnp.zeros((16, wz), BF)
        for i, v in enumerate(
            [ln1_gain, ln1_bias, query_bias, value_bias, proj_bias, ln2_gain, ln2_bias, out_bias]
            + [jnp.pad(take(fc_bias, ctx * uw, uw), (0, wz - uw))]
        ):
            small = jnp.where(row == i, v[None, :], small)
        tile = math.gcd(wz, hw)
        h1, cot, small, w_qkv, w_proj, tok_own, cot_own = entry(
            n, nz, tokens, cotangent, small, wq_own, proj_weight.reshape(wz // tile, tile, width), hw
        )
        small, fc_weight, out_weight = lax.optimization_barrier((small, fc_weight, out_weight))
        wfc_own = jnp.concatenate(
            [take(fc_weight, t * unit_z + ctx * uw, uw, 1) for t in range(nz)], axis=1
        )
        w_fc = lax.all_gather(wfc_own, "fsdp", axis=0, tiled=True)
        w_out = lax.all_gather(take(out_weight, ctx * uw, uw), "fsdp", axis=0, tiled=True)
        length = n * rows
        flat = lambda a: a.reshape(length, a.shape[-1])
        h1, cot = flat(h1), flat(cot)
        w_qkv, w_proj = w_qkv.reshape(width, 3 * hw), w_proj.reshape(hw, width)
        fb = small[8].reshape(nz, wz)[:, :uw].reshape(1, units)
        pad_cols = lambda v: take(jnp.pad(v, (0, n * hw - width)), ctx * hw, hw)
        qkv_bias = jnp.concatenate([pad_cols(small[2]), jnp.zeros((hw,), F32), pad_cols(small[3])])

        qkv = (dot(h1, w_qkv) + qkv_bias).astype(BF)
        o, p = attend(qkv, inv, blk)
        mid, h2 = middle(n, 2, o, w_proj, tok_own, small)
        h2 = flat(h2)
        hidden, slope = hidden_units(h2, w_fc, fb)
        part_out = dot(hidden, cot, TN).astype(BF)
        in_parts = lambda a: a.reshape(nz, parts, a.shape[0] // nz // parts, a.shape[1])
        o, part_out = lax.optimization_barrier((o, part_out))
        o_all = spread(n, 3, o.reshape(4, length // 4, hw))
        w_out, o_all = lax.optimization_barrier((w_out, o_all))
        to_owner = lambda a: lax.psum_scatter(a, "fsdp", scatter_dimension=0, tiled=True)
        sum_out = to_owner(part_out)
        du, dfb = hidden_back(cot, w_out, slope)
        part_fc = outer(h2, du)
        du, part_fc = lax.optimization_barrier((du, part_fc))
        sum_fc = to_owner(part_fc)
        da, dmid, layer_out, sums = turn(n, 4, du, w_fc, hidden, w_out, mid, cot_own, small)
        da = flat(da)
        do = dot(da, w_proj, NT).astype(BF)
        dqkv, bias_cols = attend_back(qkv, do, o, p, inv, blk)
        pw = width // n
        part_attn = attn_outer(h1, dqkv, o_all.reshape(n, length, hw), take(da, ctx * pw, pw, 1))

        put = lambda v, size: lax.dynamic_update_slice_in_dim(
            jnp.zeros((1, size), F32), v, ctx * v.shape[1], 1
        )
        biases = jnp.concatenate(
            [put(bias_cols[:, :hw], n * hw), put(bias_cols[:, 2 * hw :], n * hw)]
        )[:, :width]
        wide_fb = lax.dynamic_update_slice_in_dim(
            jnp.zeros((nz, unit_z), F32), dfb.reshape(nz, uw), ctx * uw, 1
        )
        vectors = jnp.concatenate(
            [sums + jnp.pad(biases, ((2, 4), (0, 0))), jnp.pad(wide_fb, ((0, -nz % 8), (0, width - unit_z)))]
        )
        all_fc, all_out, all_attn, grad_tokens, vectors = tail(
            n,
            nz,
            5,
            sum_fc.reshape(parts, wz // parts, units),
            sum_out.reshape(parts, uw // parts, width),
            in_parts(part_attn),
            dqkv,
            w_qkv,
            tok_own,
            dmid,
            small,
            vectors,
        )
        whole_rows = lambda a: a.reshape(n, a.shape[1] * a.shape[2], a.shape[3])
        grad_fc, grad_qkv, grad_proj, grad_out = join(
            n, nz, hw, whole_rows(all_fc), whole_rows(all_attn), all_out.reshape(unit_z, width)
        )
        mine = take(vectors[:8], z * wz, wz, 1)
        gfb = take(vectors[8 : 8 + nz], z, 1).reshape(-1)[:unit_z]
        return (
            layer_out,
            grad_tokens,
            mine[0],
            mine[1],
            grad_qkv,
            mine[2],
            mine[3],
            grad_proj,
            mine[4],
            mine[5],
            mine[6],
            grad_fc,
            gfb,
            grad_out,
            mine[7],
        )

    return body


def solution(mesh):
    both = P(("fsdp", "ctx"), None)
    vec, mat = P("fsdp"), P("fsdp", None)
    placed = (both, P(), vec, vec, mat, vec, vec, mat, vec, vec, vec, mat, vec, mat, vec, both)
    outs = (both, both, vec, vec, mat, vec, vec, mat, vec, vec, vec, mat, vec, mat, vec)
    return jax.shard_map(
        make_body(mesh.shape["ctx"], mesh.shape["fsdp"]),
        mesh=mesh,
        in_specs=placed,
        out_specs=outs,
        check_vma=False,
    )
```

```python
import functools
import math

import jax
import jax.numpy as jnp
from jax import lax
from jax.experimental import pallas as pl
from jax.experimental.pallas import tpu as pltpu
from jax.sharding import PartitionSpec as P

HEADS = 25
BF = jnp.bfloat16
F32 = jnp.float32
MESH = pl.DeviceIdType.MESH
ANY = pl.BlockSpec(memory_space=pl.ANY)
VMEM = pl.BlockSpec(memory_space=pltpu.VMEM)
NN = (((1,), (0,)), ((), ()))
NT = (((1,), (1,)), ((), ()))
TN = (((0,), (0,)), ((), ()))


def dot(a, b, dims=NN):
    return lax.dot_general(a, b, dims, preferred_element_type=F32)


def places(n):
    me = lax.axis_index("ctx")
    core = lax.rem(me, 2)
    chip = me // 2
    sib = me + 1 - 2 * core
    if n == 8:
        across = chip + 1 - 2 * lax.rem(chip, 2)
        along = lax.rem(chip + 2, 4)
        first = across * (1 - core) + along * core
        second = along * (1 - core) + across * core
        others = [first, second, 3 - chip]
    else:
        half = n // 2
        others = [lax.rem(chip + d, half) for d in range(1, half)]
    return me, core, chip, sib, others


def twin(square, k):
    return 1 - k if square and k < 2 else k


def signal(sem, **device):
    pl.semaphore_signal(sem, inc=1, device_id=device, device_id_type=MESH)


def greet(devices, planes=()):
    barrier = pltpu.get_barrier_semaphore()
    for device in devices:
        signal(barrier, ctx=device)
    for plane in planes:
        signal(barrier, fsdp=plane)
    pl.semaphore_wait(barrier, len(devices) + len(planes))


def send(src, dst, ssem, rsem, **device):
    return pltpu.make_async_remote_copy(
        src_ref=src,
        dst_ref=dst,
        send_sem=ssem,
        recv_sem=rsem,
        device_id=device,
        device_id_type=MESH,
    )


def merge(*lists, scales=None):
    keyed = []
    for t, steps in enumerate(lists):
        scale = scales[t] if scales else 1.0
        keyed += [((i + 0.5) * scale / len(steps), t, i, step) for i, step in enumerate(steps)]
    for item in sorted(keyed, key=lambda k: k[:3]):
        item[3]()


def timed(*lists):
    keyed = [(time, t, i, step) for t, steps in enumerate(lists) for i, (time, step) in enumerate(steps)]
    for item in sorted(keyed, key=lambda k: k[:3]):
        item[3]()


def spaced(steps, start, stop):
    return [(start + (stop - start) * (i + 0.5) / len(steps), step) for i, step in enumerate(steps)]


class Gather:
    def __init__(self, n, src, out, sems):
        self.n, self.src, self.out = n, src, out
        self.own_s, self.sib_s, self.sib_r, self.far_s, self.far_r = sems
        self.parts = src.shape[0]
        self.square = n == 8
        self.me, self.core, self.chip, self.sib, self.others = places(n)
        half = n // 2
        if self.square:
            self.froms = self.others
        else:
            self.froms = [lax.rem(self.chip + half - d, half) for d in range(1, half)]
        self.peers = self.others[:2] if self.square else self.others
        self.started = []

    @staticmethod
    def sems(n, parts):
        dma = pltpu.SemaphoreType.DMA
        far = n // 2 - 1
        return [dma((parts,)), dma((far + 1, parts)), dma((far + 1, parts)), dma((far, parts)), dma((far, parts))]

    def own_sends(self, c):
        piece, slot = self.src.at[c], self.out.at[self.me, c]
        copies = [
            send(piece, slot, self.far_s.at[d, c], self.far_r.at[d, c], ctx=2 * p + self.core)
            for d, p in enumerate(self.peers)
        ]
        copies.append(send(piece, slot, self.sib_s.at[0, c], self.sib_r.at[0, c], ctx=self.sib))
        return copies + [pltpu.make_async_copy(piece, slot, self.own_s.at[c])]

    def go(self, copy):
        copy.start()
        self.started.append(copy)

    def start(self):
        for c in range(self.parts):
            self.start_part(c)

    def start_part(self, c):
        for copy in self.own_sends(c):
            copy.start()

    def arrived(self, d, c):
        piece = self.out.at[2 * self.froms[d] + self.core, c]
        send(piece, piece, self.far_s.at[d, c], self.far_r.at[d, c], ctx=self.sib).wait_recv()
        if self.square and d == 0:
            self.go(
                send(
                    piece,
                    piece,
                    self.far_s.at[2, c],
                    self.far_r.at[2, c],
                    ctx=2 * self.others[1] + self.core,
                )
            )
        e = twin(self.square, d) + 1
        self.go(send(piece, piece, self.sib_s.at[e, c], self.sib_r.at[e, c], ctx=self.sib))

    def steps(self):
        todo = []
        for c in range(self.parts):
            for d in range(2 if self.square else len(self.others)):
                todo.append(functools.partial(self.arrived, d, c))
            if self.square and c:
                todo.append(functools.partial(self.arrived, 2, c - 1))
        if self.square:
            todo.append(functools.partial(self.arrived, 2, self.parts - 1))
        return todo

    def timed_steps(self, begin, wait, relay):
        todo = []
        for c in range(self.parts):
            for d in range(len(self.others)):
                late = relay if self.square and d == 2 else 0
                todo.append((begin(c) + wait + late, functools.partial(self.arrived, d, c)))
        return todo

    def finish(self):
        for c in range(self.parts):
            *far, own = self.own_sends(c)
            own.wait()
            for copy in far:
                copy.wait_send()
        for d in range(len(self.others) + 1):
            chip = self.chip if d == 0 else self.froms[d - 1]
            for c in range(self.parts):
                piece = self.out.at[2 * chip + 1 - self.core, c]
                send(
                    piece, piece, self.sib_s.at[d, c], self.sib_r.at[d, c], ctx=self.sib
                ).wait_recv()
        for copy in self.started:
            copy.wait_send()


class Relay:
    def __init__(self, nz, z, lo, hi, count, src, out, sems, lead):
        self.nz, self.z, self.lo, self.hi, self.count = nz, z, lo, hi, count
        self.src, self.out, self.lead = src, out, lead
        self.own_s, self.up_s, self.down_s, self.recv = sems

    @staticmethod
    def sems(blocks):
        return [pltpu.SemaphoreType.DMA((blocks,)) for _ in range(4)]

    def up(self, src, b):
        return send(src, self.out.at[b], self.up_s.at[b], self.recv.at[b], fsdp=self.z + 1)

    def down(self, src, b):
        return send(src, self.out.at[b], self.down_s.at[b], self.recv.at[b], fsdp=self.z - 1)

    def own(self, b):
        return pltpu.make_async_copy(self.src.at[b - self.lead], self.out.at[b], self.own_s.at[b])

    def start(self):
        lo, hi = self.lo, self.hi

        def body(i, carry):
            u, d = hi - 1 - i, lo + i

            @pl.when(self.z < self.nz - 1)
            def _():
                self.up(self.src.at[u - self.lead], u).start()

            @pl.when(self.z > 0)
            def _():
                self.down(self.src.at[d - self.lead], d).start()

            self.own(d).start()
            return carry

        lax.fori_loop(0, hi - lo, body, 0)

    def step(self, i):
        b = self.lo - 1 - i

        @pl.when(b >= 0)
        def _():
            self.up(self.out.at[b], b).wait_recv()

            @pl.when(self.z < self.nz - 1)
            def _():
                self.up(self.out.at[b], b).start()

        e = self.hi + i

        @pl.when(e < self.count)
        def _():
            self.down(self.out.at[e], e).wait_recv()

            @pl.when(self.z > 0)
            def _():
                self.down(self.out.at[e], e).start()

    def steps(self, most):
        return [functools.partial(self.step, i) for i in range(most)]

    def finish(self):
        def sent(b, carry):
            @pl.when((self.z < self.nz - 1) & (b < self.hi))
            def _():
                self.up(self.out.at[b], b).wait_send()

            @pl.when((self.z > 0) & (b >= self.lo))
            def _():
                self.down(self.out.at[b], b).wait_send()

            @pl.when((b >= self.lo) & (b < self.hi))
            def _():
                self.own(b).wait()

            return carry

        lax.fori_loop(0, self.count, sent, 0)


def others_of(z, nz):
    return [lax.rem(z + d, nz) for d in range(1, nz)]


def entry_kernel(
    n, nz, tok_t, cot_t, small, wq, wp, fc_hbm, out_hbm, h1_all, cot_all, vec, wq_all, wp_all, tok, cot_own,
    fc_own, out_own, *scratch
):
    cot, h1, inbox, zeros, fc_all, load_s, small_s, small_r, zero_s = scratch[:9]
    g_h, g_c = scratch[9:14], scratch[14:19]
    r_q, r_p = scratch[19:23], scratch[23:27]
    loads = [
        pltpu.make_async_copy(fc_hbm, fc_all, load_s.at[0]),
        pltpu.make_async_copy(out_hbm.at[lax.axis_index("ctx")], out_own, load_s.at[1]),
    ]
    me, core, chip, sib, others = places(n)
    z = lax.axis_index("fsdp")
    planes = others_of(z, nz)
    greet([sib] + [2 * p + core for p in (others[:2] if n == 8 else others)], planes)
    wz = small.shape[1]
    for d, plane in enumerate(planes):
        send(small, inbox.at[z], small_s.at[d], small_r.at[d], fsdp=plane).start()
    inbox[z] = small[...]
    k = wq.shape[0]
    relay_q = Relay(nz, z, z * k, (z + 1) * k, nz * k, wq, wq_all, r_q, z * k)
    relay_q.start()
    parts, rows = h1.shape[0], h1.shape[1]
    turned = cot_t[...].astype(F32).T.astype(BF)
    cot_own[...] = turned
    for c in range(parts):
        cot[c] = turned[c * rows : (c + 1) * rows, :]
    gather_c = Gather(n, cot, cot_all, g_c)
    gather_c.start()
    tok[...] = tok_t[...].astype(F32).T.astype(BF)
    share, blocks = wp.shape[0], wp_all.shape[0]
    base = me * blocks
    valid = jnp.clip(nz * share - base, 0, blocks)
    lo = jnp.clip(z * share - base, 0, valid)
    hi = jnp.clip((z + 1) * share - base, 0, valid)
    relay_p = Relay(nz, z, lo, hi, valid, wp, wp_all, r_p, z * share - base)
    relay_p.start()
    zeros[...] = jnp.zeros_like(zeros)

    def clear(b, carry):
        pltpu.make_async_copy(zeros, wp_all.at[b], zero_s.at[b]).start()
        return carry

    lax.fori_loop(valid, blocks, clear, 0)
    for d in range(nz - 1):
        came = lax.rem(z + nz - 1 - d, nz)
        send(small, inbox.at[came], small_s.at[d], small_r.at[d], fsdp=planes[d]).wait_recv()
    for p in range(nz):
        vec[:, p * wz : (p + 1) * wz] = inbox[p].astype(F32)
    gain, shift = vec[0:1, :], vec[1:2, :]
    gather_h = Gather(n, h1, h1_all, g_h)
    for c in range(parts):
        unit, _ = norm(tok[c * rows : (c + 1) * rows, :].astype(F32))
        h1[c] = (unit * gain + shift).astype(BF)
        gather_h.start_part(c)
    for load in loads:
        load.start()

    def columns():
        for load in loads:
            load.wait()
        uw = fc_own.shape[-1] // nz
        for place in range(n):

            @pl.when(me == place)
            def _():
                def tile(i, carry):
                    for t in range(nz):
                        at = (t * n + place) * uw
                        fc_own[i, :, t * uw : (t + 1) * uw] = fc_all[i, :, at : at + uw]
                    return carry

                lax.fori_loop(0, fc_own.shape[0], tile, 0)

    steps = gather_c.steps() + gather_h.steps()
    merge(
        steps[:4] + [columns] + steps[4:],
        relay_q.steps(nz * k - k) + relay_p.steps(blocks),
    )
    gather_c.finish()
    gather_h.finish()
    relay_q.finish()
    relay_p.finish()

    def cleared(b, carry):
        pltpu.make_async_copy(zeros, wp_all.at[b], zero_s.at[b]).wait()
        return carry

    lax.fori_loop(valid, blocks, cleared, 0)
    for d, plane in enumerate(planes):
        send(small, inbox.at[z], small_s.at[d], small_r.at[d], fsdp=plane).wait_send()


def entry(n, nz, tokens, cot, small, wq, wp, fc, out, hw):
    rows, width = tokens.shape
    parts = 2 if n == 8 else 1
    dma = pltpu.SemaphoreType.DMA
    k, tile = wq.shape[0], wp.shape[1]
    blocks = hw // tile
    shape = jax.ShapeDtypeStruct
    piece = (parts, rows // parts, width)
    return pl.pallas_call(
        functools.partial(entry_kernel, n, nz),
        out_shape=[
            shape((n,) + piece, BF),
            shape((n,) + piece, BF),
            shape((small.shape[0], width), F32),
            shape((nz * k,) + wq.shape[1:], BF),
            shape((blocks, tile, width), BF),
            shape((rows, width), BF),
            shape((rows, width), BF),
            shape(fc.shape[:2] + (fc.shape[2] // n,), BF),
            shape(out.shape[1:], BF),
        ],
        in_specs=[VMEM] * 5 + [ANY, ANY],
        out_specs=[ANY, ANY, VMEM, ANY, ANY] + [VMEM] * 4,
        scratch_shapes=[
            pltpu.VMEM(piece, BF),
            pltpu.VMEM(piece, BF),
            pltpu.VMEM((nz,) + small.shape, BF),
            pltpu.VMEM((tile, width), BF),
            pltpu.VMEM(fc.shape, BF),
            dma((2,)),
            dma((nz - 1,)),
            dma((nz - 1,)),
            dma((blocks,)),
        ]
        + Gather.sems(n, parts)
        + Gather.sems(n, parts)
        + Relay.sems(nz * k)
        + Relay.sems(blocks),
        compiler_params=pltpu.CompilerParams(
            collective_id=1, has_side_effects=True, vmem_limit_bytes=60 * 1024 * 1024
        ),
        name="entry",
    )(tokens.T, cot.T, small, wq, wp, fc, out)


class Scatter:
    def __init__(self, n, dims, a, w, scratch):
        self.n, self.dims, self.a, self.w = n, dims, a, w
        self.part, self.theirs, self.sums, self.inbox = scratch[:4]
        self.sib_s, self.sib_r, self.far_s, self.far_r = scratch[4:]
        self.me, self.core, self.chip, self.sib, self.others = places(n)
        self.square = n == 8
        self.half = n // 2
        self.parts = self.sib_s.shape[1]
        self.full = self.part.shape[2]
        self.rows = self.full // self.parts
        if self.square:
            first, second = [2 * p + self.core for p in self.others[:2]]
            self.ends = [(0, 0, first), (1, 1, first), (2, 2, second)]
        else:
            self.ends = [(k, k, 2 * self.others[k] + self.core) for k in range(self.half - 1)]

    @staticmethod
    def scratch(n, rows, width):
        dma = pltpu.SemaphoreType.DMA
        half, parts = n // 2, 4 if n == 8 else 1
        return [
            pltpu.VMEM((half, 2, rows, width), BF),
            pltpu.VMEM((half, rows, width), BF),
            pltpu.VMEM((half - 1, rows, width), BF),
            pltpu.VMEM((half - 1, rows, width), BF),
            dma((half, parts)),
            dma((half, parts)),
            dma((half - 1, parts)),
            dma((half - 1, parts)),
        ]

    def chip_at(self, k):
        if not self.square:
            return lax.rem(self.chip + 1 + k, self.half)
        x, y = lax.rem(self.chip, 2), self.chip // 2
        first, second = 1 - lax.rem(k, 3) // 2, 1 - lax.rem(k, 2)
        dx = first * (1 - self.core) + second * self.core
        dy = second * (1 - self.core) + first * self.core
        far = (k < 3).astype(jnp.int32)
        dx, dy = dx * far, dy * far
        return (y + dy - 2 * y * dy) * 2 + x + dx - 2 * x * dx

    def twin_at(self, k):
        if not self.square:
            return k
        return k + jnp.where(k == 1, 1, 0) - jnp.where(k == 2, 1, 0)

    def win(self, c):
        return pl.ds(c * self.rows, self.rows)

    def to_sib(self, k, c):
        e = self.twin_at(k)
        return send(
            self.part.at[k, 1 - self.core, self.win(c)],
            self.theirs.at[e, self.win(c)],
            self.sib_s.at[e, c],
            self.sib_r.at[e, c],
            ctx=self.sib,
        )

    def chip_sum(self, k, c):
        win = self.win(c)
        piece = self.theirs.at[k, win]
        send(piece, piece, self.sib_s.at[k, c], self.sib_r.at[k, c], ctx=self.sib).wait_recv()
        return self.part[k, self.core, win, :].astype(F32) + self.theirs[k, win, :].astype(F32)

    def pass_on(self, k, slot, peer, c):
        return send(
            self.sums.at[k, self.win(c)],
            self.inbox.at[slot, self.win(c)],
            self.far_s.at[slot, c],
            self.far_r.at[slot, c],
            ctx=peer,
        )

    def wait_in(self, slot, c):
        piece = self.inbox.at[slot, self.win(c)]
        send(piece, piece, self.far_s.at[slot, c], self.far_r.at[slot, c], ctx=self.sib).wait_recv()
        return self.inbox[slot, self.win(c), :].astype(F32)

    def forward(self, end, c):
        k, slot, peer = self.ends[end]
        total = self.chip_sum(k, c)
        if self.square and end == 2:
            total = total + self.wait_in(0, c)
        self.sums[k, self.win(c), :] = total.astype(BF)
        self.pass_on(k, slot, peer, c).start()

    def products(self):
        def product(k, carry):
            full = self.full
            at = pl.ds(pl.multiple_of(self.chip_at(k) * 2 * full, 2 * full), 2 * full)
            val = dot(self.a[at, :], self.w[...], self.dims).astype(BF)
            self.part[k, 0] = val[:full]
            self.part[k, 1] = val[full:]
            for c in range(self.parts):
                self.to_sib(k, c).start()

            @pl.when(k == 1)
            def _():
                for c in range(self.parts):
                    self.forward(0, c)

            return carry

        lax.fori_loop(0, self.half, product, 0)

    def forwards(self):
        each = range(self.parts)
        return [functools.partial(self.forward, e, c) for e in range(1, self.half - 1) for c in each]

    def total(self, c):
        val = self.chip_sum(self.half - 1, c)
        for slot in (1, 2) if self.square else range(self.half - 1):
            val = val + self.wait_in(slot, c)
        return val

    def finish(self):
        for c in range(self.parts):
            for k, slot, peer in self.ends:
                self.pass_on(k, slot, peer, c).wait_send()

        def sent(k, carry):
            for c in range(self.parts):
                self.to_sib(k, c).wait_send()
            return carry

        lax.fori_loop(0, self.half, sent, 0)


class Line:
    def __init__(self, nz, z, src, out, scratch):
        self.nz, self.z, self.src, self.out = nz, z, src, out
        self.mine, self.above, self.below, self.load_s, self.up_s, self.down_s, self.recv = scratch
        self.parts = src.shape[1]

    @staticmethod
    def scratch(shape):
        dma, lead = pltpu.SemaphoreType.DMA, shape[:2]
        return [pltpu.VMEM(shape, BF)] * 3 + [dma((1,)), dma(lead), dma(lead), dma((2,) + lead)]

    def up(self, src, d, c):
        return send(
            src.at[d, c], self.above.at[d, c], self.up_s.at[d, c], self.recv.at[0, d, c], fsdp=self.z + 1
        )

    def down(self, src, d, c):
        return send(
            src.at[d, c], self.below.at[d, c], self.down_s.at[d, c], self.recv.at[1, d, c], fsdp=self.z - 1
        )

    def start(self):
        top = self.nz - 1

        @pl.when(self.z == 0)
        def _():
            for c in range(self.parts):
                for k in range(top):
                    self.up(self.src, top - k, c).start()

        @pl.when(self.z == top)
        def _():
            for c in range(self.parts):
                for k in range(top):
                    self.down(self.src, k, c).start()

        self.load = pltpu.make_async_copy(self.src, self.mine, self.load_s.at[0])
        self.load.start()

    def loaded(self):
        self.load.wait()

    def pass_up(self, d, c):
        copy = self.up(self.mine, d, c)
        copy.wait_recv()
        self.mine[d, c] = self.mine[d, c] + self.above[d, c]
        copy.start()

    def pass_down(self, d, c):
        copy = self.down(self.mine, d, c)
        copy.wait_recv()
        self.mine[d, c] = self.mine[d, c] + self.below[d, c]
        copy.start()

    def settle(self, place, c):
        z, top = place, self.nz - 1
        total = self.mine[z, c].astype(F32)
        if z > 0:
            self.up(self.mine, z, c).wait_recv()
            total = total + self.above[z, c].astype(F32)
        if z < top:
            self.down(self.mine, z, c).wait_recv()
            total = total + self.below[z, c].astype(F32)
        self.out[c] = total.astype(BF)

    def timed_steps(self, after):
        top = self.nz - 1
        slots = {}

        def put(time, place, fn):
            slots.setdefault(time, {}).setdefault(place, []).append(fn)

        for c in range(self.parts):
            for place in range(self.nz):
                for k in range(top):
                    at = c * top + k
                    if 0 < place < top - k:
                        put(at + place, place, functools.partial(self.pass_up, top - k, c))
                    if k < place < top:
                        put(at + top - place, place, functools.partial(self.pass_down, k, c))
                put((c + 1) * top, place, functools.partial(self.settle, place, c))
                put((c + 1) * top, place, functools.partial(after, c))

        def run(work):
            for place, fns in sorted(work.items()):

                @pl.when(self.z == place)
                def _():
                    for fn in fns:
                        fn()

        return [(0, self.loaded)] + [(t, functools.partial(run, slots[t])) for t in sorted(slots)]

    def finish(self):
        for d in range(self.nz):

            @pl.when(self.z < d)
            def _():
                for c in range(self.parts):
                    self.up(self.mine, d, c).wait_send()

            @pl.when(self.z > d)
            def _():
                for c in range(self.parts):
                    self.down(self.mine, d, c).wait_send()


class Vectors:
    def __init__(self, n, nz, src, out, scratch):
        self.n, self.nz, self.src, self.out = n, nz, src, out
        self.low, self.from_sib, self.chips, self.line = scratch[:4]
        self.ss, self.sr, self.cs, self.cr, self.ls, self.lr = scratch[4:]
        self.me, self.core, self.chip, self.sib, self.others = places(n)
        self.z = lax.axis_index("fsdp")
        self.planes = others_of(self.z, nz)

    @staticmethod
    def scratch(n, nz, shape):
        dma = pltpu.SemaphoreType.DMA
        half = n // 2
        return [
            pltpu.VMEM(shape, BF),
            pltpu.VMEM(shape, BF),
            pltpu.VMEM((half,) + shape, BF),
            pltpu.VMEM((nz,) + shape, BF),
            dma((1,)),
            dma((1,)),
            dma((half - 1,)),
            dma((half - 1,)),
            dma((nz - 1,)),
            dma((nz - 1,)),
        ]

    def to_sib(self):
        return send(self.low, self.from_sib, self.ss.at[0], self.sr.at[0], ctx=self.sib)

    def to_chip(self, d):
        at = self.chips.at[self.chip]
        return send(at, at, self.cs.at[d], self.cr.at[d], ctx=2 * self.others[d] + self.core)

    def to_plane(self, d):
        at = self.line.at[self.z]
        return send(at, at, self.ls.at[d], self.lr.at[d], fsdp=self.planes[d])

    def start(self):
        self.low[...] = self.src[...].astype(BF)
        self.to_sib().start()

    def first(self):
        self.to_sib().wait_recv()
        self.chips[self.chip] = self.low[...] + self.from_sib[...]
        for d in range(self.n // 2 - 1):
            self.to_chip(d).start()

    def second(self):
        for d in range(self.n // 2 - 1):
            self.to_chip(d).wait_recv()
        total = self.chips[0].astype(F32)
        for k in range(1, self.n // 2):
            total = total + self.chips[k].astype(F32)
        self.line[self.z] = total.astype(BF)
        for d in range(self.nz - 1):
            self.to_plane(d).start()

    def third(self):
        for d in range(self.nz - 1):
            self.to_plane(d).wait_recv()
        total = self.line[0].astype(F32)
        for k in range(1, self.nz):
            total = total + self.line[k].astype(F32)
        self.out[...] = total

    def steps(self):
        return [self.first, self.second, self.third]

    def finish(self):
        self.to_sib().wait_send()
        for d in range(self.n // 2 - 1):
            self.to_chip(d).wait_send()
        for d in range(self.nz - 1):
            self.to_plane(d).wait_send()


def beside(n):
    me, core, chip, sib, others = places(n)
    return [sib] + [2 * p + core for p in (others[:2] if n == 8 else others)]


def call(kernel, cid, name, ins, in_specs, outs, out_specs, scratch):
    return pl.pallas_call(
        kernel,
        out_shape=[jax.ShapeDtypeStruct(*o) for o in outs],
        in_specs=in_specs,
        out_specs=out_specs,
        scratch_shapes=scratch,
        compiler_params=pltpu.CompilerParams(
            collective_id=cid, has_side_effects=True, vmem_limit_bytes=60 * 1024 * 1024
        ),
        name=name,
    )(*ins)


def middle_kernel(n, o, w, tok, vec, mid, h2_all, h2, *scratch):
    greet(beside(n))
    scatter = Scatter(n, NN, o, w, scratch[:8])
    gather = Gather(n, h2, h2_all, scratch[8:])
    scatter.products()
    for step in scatter.forwards():
        step()
    for c in range(gather.parts):
        win = scatter.win(c)
        val = tok[win, :].astype(F32) + scatter.total(c) + vec[4:5, :]
        mid[win, :] = val
        h2[c] = (norm(val)[0] * vec[5:6, :] + vec[6:7, :]).astype(BF)
        gather.start_part(c)
    for step in gather.steps():
        step()
    gather.finish()
    scatter.finish()


def middle(n, cid, o, w, tok, vec):
    rows, width = tok.shape
    parts = 4 if n == 8 else 1
    piece = (parts, rows // parts, width)
    return call(
        functools.partial(middle_kernel, n),
        cid,
        "middle",
        (o, w, tok, vec),
        [VMEM] * 4,
        [((rows, width), F32), ((n,) + piece, BF)],
        [VMEM, ANY],
        [pltpu.VMEM(piece, BF)] + Scatter.scratch(n, rows, width) + Gather.sems(n, parts),
    )


def spread_kernel(n, src, all_ref, *sems):
    greet(beside(n))
    gather = Gather(n, src, all_ref, sems)
    gather.start()
    for step in gather.steps():
        step()
    gather.finish()


def spread(n, cid, array):
    return call(
        functools.partial(spread_kernel, n),
        cid,
        "spread",
        (array,),
        [VMEM],
        [((n,) + array.shape, BF)],
        [ANY],
        Gather.sems(n, array.shape[0]),
    )[0]


def turn_kernel(n, du, w_fc, hid, w_out, mid, cot, vec, da_all, dmid, layer, sums, da, *scratch):
    greet(beside(n))
    back = Scatter(n, NT, du, w_fc, scratch[:8])
    ahead = Scatter(n, NN, hid, w_out, scratch[8:16])
    gather = Gather(n, da, da_all, scratch[16:])
    back.products()
    todo = back.forwards()
    for step in todo[: back.parts]:
        step()
    ahead.products()
    for step in todo[back.parts :]:
        step()
    sums[...] = jnp.zeros_like(sums)
    for c in range(gather.parts):
        win = back.win(c)
        grad = back.total(c)
        unit, rstd = norm(mid[win, :])
        up = cot[win, :].astype(F32)
        val = up + norm_back(grad, unit, rstd, vec[5:6, :])
        dmid[win, :] = val
        low = val.astype(BF)
        da[c] = low
        gather.start_part(c)
        for row, term in ((4, low.astype(F32)), (5, grad * unit), (6, grad), (7, up)):
            sums[row : row + 1, :] += jnp.sum(term, axis=0, keepdims=True)
    merge(gather.steps(), ahead.forwards())
    for c in range(gather.parts):
        win = ahead.win(c)
        layer[win, :] = (mid[win, :] + ahead.total(c) + vec[7:8, :]).astype(BF)
    gather.finish()
    back.finish()
    ahead.finish()


def turn(n, cid, du, w_fc, hidden, w_out, mid, cot, vec):
    rows, width = mid.shape
    parts = 4 if n == 8 else 1
    piece = (parts, rows // parts, width)
    return call(
        functools.partial(turn_kernel, n),
        cid,
        "turn",
        (du, w_fc, hidden, w_out, mid, cot, vec),
        [VMEM] * 7,
        [((n,) + piece, BF), ((rows, width), F32), ((rows, width), BF), ((8, width), F32)],
        [ANY, VMEM, VMEM, VMEM],
        [pltpu.VMEM(piece, BF)]
        + Scatter.scratch(n, rows, width)
        + Scatter.scratch(n, rows, width)
        + Gather.sems(n, parts),
    )


def tail_kernel(
    n, nz, fc, part, dqkv, w_qkv, tok, dmid, vec, v_in, fc_all, attn_all, g_tok, v_out,
    v_own, attn, fc_v, dqkv_v, w_v, load_s, *scratch,
):
    z = lax.axis_index("fsdp")
    me, core, chip, sib, others = places(n)
    greet([sib] + [2 * p + core for p in others], others_of(z, nz))
    line = Line(nz, z, part, attn, scratch[:7])
    line.start()
    loads = [
        pltpu.make_async_copy(src, dst, load_s.at[i])
        for i, (src, dst) in enumerate([(dqkv, dqkv_v), (w_qkv, w_v), (fc, fc_v)])
    ]
    for load in loads:
        load.start()
    fc, dqkv, w_qkv = fc_v, dqkv_v, w_v
    scatter = Scatter(n, NT, dqkv, w_qkv, scratch[7:15])
    vectors = Vectors(n, nz, v_own, v_out, scratch[15:25])
    fc_g = Gather(n, fc, fc_all, scratch[25:30])
    attn_g = Gather(n, attn, attn_all, scratch[30:35])
    v_own[...] = v_in[...]
    for load in loads[:2]:
        load.wait()
    scatter.products()
    todo = scatter.forwards()
    for step in todo[: scatter.parts]:
        step()
    loads[2].wait()

    def rest(c):
        win = scatter.win(c)
        grad = scatter.total(c)
        unit, rstd = norm(tok[win, :].astype(F32))
        g_tok[win, :] = (dmid[win, :] + norm_back(grad, unit, rstd, vec[0:1, :])).astype(BF)
        v_own[0:1, :] += jnp.sum(grad * unit, axis=0, keepdims=True)
        v_own[1:2, :] += jnp.sum(grad, axis=0, keepdims=True)

    top = nz - 1
    last = attn_g.parts * top
    part_at = functools.partial
    fc_at = lambda c: 4.0 + 2.0 * c
    timed(
        spaced(todo[scatter.parts :], 1.0, 4.0),
        spaced([part_at(rest, c) for c in range(scatter.parts)], 4.5, 7.0),
        [(7.1, vectors.start), (7.8, vectors.first), (11.0, vectors.second), (last + 3.0, vectors.third)],
        [(fc_at(c), part_at(fc_g.start_part, c)) for c in range(fc_g.parts)],
        fc_g.timed_steps(fc_at, 2.2, 1.6),
        line.timed_steps(attn_g.start_part),
        attn_g.timed_steps(lambda c: (c + 1) * top, 2.2, 1.6),
    )
    for job in (fc_g, attn_g, scatter, line, vectors):
        job.finish()


def tail(n, nz, cid, fc, part, dqkv, w_qkv, tok, dmid, vec, v_in):
    rows, width = tok.shape
    attn = part.shape[1:]
    return call(
        functools.partial(tail_kernel, n, nz),
        cid,
        "tail",
        (fc, part, dqkv, w_qkv, tok, dmid, vec, v_in),
        [ANY] * 4 + [VMEM] * 4,
        [((n,) + fc.shape, BF), ((n,) + attn, BF), (tok.shape, BF), (v_in.shape, F32)],
        [ANY, ANY, VMEM, VMEM],
        [pltpu.VMEM(v_in.shape, F32), pltpu.VMEM(attn, BF)]
        + [pltpu.VMEM(a.shape, BF) for a in (fc, dqkv, w_qkv)]
        + [pltpu.SemaphoreType.DMA((3,))]
        + Line.scratch(part.shape)
        + Scatter.scratch(n, rows, width)
        + Vectors.scratch(n, nz, v_in.shape)
        + Gather.sems(n, fc.shape[0])
        + Gather.sems(n, attn[0]),
    )


def outer_kernel(x_ref, y_ref, out_ref):
    out_ref[...] = dot(x_ref[...], y_ref[...], TN).astype(BF)


def outer(x, y):
    rows, m = x.shape
    tile = 256
    return pl.pallas_call(
        outer_kernel,
        grid=(pl.cdiv(m, tile),),
        out_shape=jax.ShapeDtypeStruct((m, y.shape[1]), BF),
        in_specs=[pl.BlockSpec((rows, tile), lambda i: (0, i)), fixed(*y.shape)],
        out_specs=tiled(tile, y.shape[1]),
        name="outer",
    )(x, y)


def hidden_kernel(h_ref, w_ref, b_ref, z_ref, s_ref):
    u = dot(h_ref[...], w_ref[...]) + b_ref[...]
    root = 0.7978845608028654
    square = u * u
    inner = jnp.tanh(root * u * (1.0 + 0.044715 * square))
    z_ref[...] = (0.5 * u * (1.0 + inner)).astype(BF)
    slope = 0.5 * (1.0 + inner) + 0.5 * u * (1.0 - inner * inner) * root * (1.0 + 3 * 0.044715 * square)
    s_ref[...] = slope.astype(BF)


def hidden_back_kernel(c_ref, w_ref, s_ref, d_ref, sum_ref):
    du = (dot(c_ref[...], w_ref[...], NT) * s_ref[...].astype(F32)).astype(BF)
    d_ref[...] = du

    @pl.when(pl.program_id(0) == 0)
    def _():
        sum_ref[...] = jnp.zeros_like(sum_ref)

    sum_ref[...] += jnp.sum(du.astype(F32), axis=0, keepdims=True)


def tiled(rows, cols):
    return pl.BlockSpec((rows, cols), lambda i: (i, 0))


def fixed(rows, cols):
    return pl.BlockSpec((rows, cols), lambda i: (0, 0))


def hidden_units(h2, w_fc, bias):
    rows, width = h2.shape
    units = w_fc.shape[1]
    tile = 256
    shape = jax.ShapeDtypeStruct((rows, units), BF)
    return pl.pallas_call(
        hidden_kernel,
        grid=(rows // tile,),
        out_shape=[shape, shape],
        in_specs=[tiled(tile, width), fixed(width, units), fixed(1, units)],
        out_specs=[tiled(tile, units), tiled(tile, units)],
        name="hidden",
    )(h2, w_fc, bias)


def hidden_back(cot, w_out, slope):
    rows, width = cot.shape
    units = w_out.shape[0]
    tile = 256
    return pl.pallas_call(
        hidden_back_kernel,
        grid=(rows // tile,),
        out_shape=[
            jax.ShapeDtypeStruct((rows, units), BF),
            jax.ShapeDtypeStruct((1, units), F32),
        ],
        in_specs=[tiled(tile, width), fixed(units, width), tiled(tile, units)],
        out_specs=[tiled(tile, units), fixed(1, units)],
        name="hidden_back",
    )(cot, w_out, slope)


def join_kernel(n, nz, hw, width, fc, qp, out, fc_o, qkv_o, proj_o, out_o):
    uw = fc.shape[-1] // nz
    for c in range(n):
        for b in range(nz):
            at = b * n * uw + c * uw
            fc_o[:, at : at + uw] = fc[c, 0, :, b * uw : (b + 1) * uw].astype(F32)
        size = min(128, width - c * 128)
        if size > 0:
            proj_o[:, c * 128 : c * 128 + size] = qp[c, 0, :, 3 * hw : 3 * hw + size].astype(F32)
        size = min(hw, width - c * hw)
        if size > 0:
            for t in range(3):
                at = t * width + c * hw
                qkv_o[:, at : at + size] = qp[c, 0, :, t * hw : t * hw + size].astype(F32)
    if 128 * n < width:
        proj_o[:, 128 * n :] = qp[n - 1, 0, :, : width - 128 * n].astype(F32)
    out_o[...] = out[...].astype(F32)


def join(n, nz, hw, fc, qp, out):
    tiles = 25
    width = out.shape[1]
    wz = fc.shape[1]
    split = lambda a: a.reshape(n, tiles, wz // tiles, a.shape[-1])
    fc, qp = split(fc), split(qp)
    wide = lambda a: pl.BlockSpec((n, 1, wz // tiles, a.shape[-1]), lambda i: (0, i, 0, 0))
    t, ot = wz // tiles, out.shape[0] // tiles
    cols = (n * fc.shape[-1], 3 * width, width)
    shape = jax.ShapeDtypeStruct
    return pl.pallas_call(
        functools.partial(join_kernel, n, nz, hw, width),
        grid=(tiles,),
        out_shape=[shape((wz, c), F32) for c in cols] + [shape(out.shape, F32)],
        in_specs=[wide(fc), wide(qp), tiled(ot, width)],
        out_specs=[tiled(t, c) for c in cols] + [tiled(ot, width)],
        name="join",
    )(fc, qp, out)


def attend_kernel(blocks, blk, tile, inv_ref, q_ref, k_ref, v_ref, o_ref, p_ref, qn, kn, vn, on, ot):
    length = blocks * blk
    for i in range(blocks):
        src, dst = pl.ds(pl.multiple_of(inv_ref[i] * blk, blk), blk), pl.ds(i * blk, blk)
        qn[dst, :] = q_ref[src, :]
        kn[dst, :] = k_ref[src, :]
        vn[dst, :] = v_ref[src, :]
    v_turned = vn[...].astype(F32).T.astype(BF)
    lane = lax.broadcasted_iota(jnp.int32, (1, 128), 1)
    above = lax.broadcasted_iota(jnp.int32, (tile, tile), 0) > lax.broadcasted_iota(
        jnp.int32, (tile, tile), 1
    )
    for i in range(length // tile):
        cols = pl.ds(i * tile, tile)
        keys = (i + 1) * tile
        for h in range(2):
            here = (lane // 64) == h
            q = jnp.where(here, qn[cols, :].astype(F32) * 0.125, 0.0).astype(BF)
            last = jnp.where(above, -1e30, dot(kn[pl.ds(i * tile, tile), :], q, NT))
            top = jnp.max(last, axis=0, keepdims=True)
            if i:
                early = dot(kn[pl.ds(0, i * tile), :], q, NT)
                top = jnp.maximum(top, jnp.max(early, axis=0, keepdims=True))
            last = jnp.exp(last - top)
            total = jnp.sum(last, axis=0, keepdims=True)
            if i:
                early = jnp.exp(early - top)
                total = total + jnp.sum(early, axis=0, keepdims=True)
            scale = 1.0 / total
            last = (last * scale).astype(BF)
            p_ref[h, pl.ds(i * tile, tile), cols] = last
            half = slice(64 * h, 64 * h + 64)
            o = dot(v_turned[half, i * tile : keys], last)
            if i:
                early = (early * scale).astype(BF)
                p_ref[h, pl.ds(0, i * tile), cols] = early
                o = o + dot(v_turned[half, : i * tile], early)
            ot[half, cols] = o
    on[...] = ot[...].T.astype(BF)
    for i in range(blocks):
        o_ref[pl.ds(pl.multiple_of(inv_ref[i] * blk, blk), blk), :] = on[i * blk : (i + 1) * blk, :]


def attend(qkv, inv, blk):
    length = qkv.shape[0]
    cols = qkv.shape[1] // 3
    pairs = cols // 128
    blocks = inv.shape[0]
    tile = 256
    piece = lambda off: pl.BlockSpec((length, 128), lambda p, s: (0, off * pairs + p))
    return pl.pallas_call(
        functools.partial(attend_kernel, blocks, blk, tile),
        out_shape=[
            jax.ShapeDtypeStruct((length, cols), BF),
            jax.ShapeDtypeStruct((2 * pairs, length, length), BF),
        ]
        + [jax.ShapeDtypeStruct((length, cols), BF)] * 4,
        grid_spec=pltpu.PrefetchScalarGridSpec(
            num_scalar_prefetch=1,
            grid=(pairs,),
            in_specs=[piece(0), piece(1), piece(2)],
            out_specs=[
                pl.BlockSpec((length, 128), lambda p, s: (0, p)),
                pl.BlockSpec((2, length, length), lambda p, s: (p, 0, 0)),
            ]
            + [pl.BlockSpec((length, 128), lambda p, s: (0, p))] * 4,
            scratch_shapes=[pltpu.VMEM((128, length), F32)],
        ),
        compiler_params=pltpu.CompilerParams(vmem_limit_bytes=60 * 1024 * 1024),
        name="attend",
    )(inv, qkv, qkv, qkv)


def order_kernel(blocks, blk, table, x, out):
    for i in range(blocks):
        src = pl.ds(pl.multiple_of(table[i] * blk, blk), blk)
        out[i * blk : (i + 1) * blk, :] = x[src, :]


def order(x, table, blk):
    return pl.pallas_call(
        functools.partial(order_kernel, table.shape[0], blk),
        out_shape=jax.ShapeDtypeStruct(x.shape, x.dtype),
        in_specs=[pl.BlockSpec(memory_space=pltpu.SMEM), VMEM],
        out_specs=VMEM,
        name="order",
    )(table, x)


def heads_kernel(blocks, blk, tile, table, da, w, out, rows):
    step = pl.program_id(0)
    rows[pl.ds(pl.multiple_of(step * tile, tile), tile), :] = dot(da[...], w[...], NT).astype(BF)

    @pl.when(step == pl.num_programs(0) - 1)
    def _():
        for i in range(blocks):
            src = pl.ds(pl.multiple_of(table[i] * blk, blk), blk)
            out[i * blk : (i + 1) * blk, :] = rows[src, :]


def heads_grad(da, w_proj, table, blk):
    length, width = da.shape
    cols = w_proj.shape[0]
    tile = 256
    return pl.pallas_call(
        functools.partial(heads_kernel, table.shape[0], blk, tile),
        out_shape=jax.ShapeDtypeStruct((length, cols), BF),
        grid_spec=pltpu.PrefetchScalarGridSpec(
            num_scalar_prefetch=1,
            grid=(length // tile,),
            in_specs=[
                pl.BlockSpec((tile, width), lambda i, s: (i, 0)),
                pl.BlockSpec((cols, width), lambda i, s: (0, 0)),
            ],
            out_specs=pl.BlockSpec((length, cols), lambda i, s: (0, 0)),
            scratch_shapes=[pltpu.VMEM((length, cols), BF)],
        ),
        name="heads_grad",
    )(table, da, w_proj)


def back_kernel(
    n, tile, hw, width, ready, q, k, v, o, do, da_hbm, p_hbm, h1_hbm, all_hbm,
    ready_all, dqkv, sums, out,
    da, p, h1, o_all, dqt, dk, dv, load_s, p_s, *sems,
):
    me = lax.axis_index("ctx")
    length, cols = q.shape
    pairs = cols // 128
    slots = p.shape[0]
    greet(beside(n))
    gather = Gather(n, ready, ready_all, sems)
    gather.start()
    loads = [
        pltpu.make_async_copy(src, dst, load_s.at[i])
        for i, (src, dst) in enumerate([(da_hbm, da), (h1_hbm, h1), (all_hbm, o_all)])
    ]

    def load_p(pair):
        at = pair % slots
        return pltpu.make_async_copy(p_hbm.at[pl.ds(2 * pair, 2)], p.at[at], p_s.at[at])

    load_p(0).start()
    for load in loads:
        load.start()
    lane = lax.broadcasted_iota(jnp.int32, (1, 128), 1)
    held = {}

    def begin(pair):
        if pair + 1 < pairs and slots > 1:
            load_p(pair + 1).start()
        at = slice(pair * 128, pair * 128 + 128)
        held["k"] = k[:, at].astype(F32).T.astype(BF)
        prod = (do[:, at].astype(F32) * o[:, at].astype(F32)).T
        held["d"] = [jnp.sum(prod[64 * h : 64 * h + 64, :], axis=0, keepdims=True) for h in range(2)]
        dk[...] = jnp.zeros_like(dk)
        dv[...] = jnp.zeros_like(dv)
        load_p(pair).wait()

    def block(pair, i):
        win = pl.ds(i * tile, tile)
        at = slice(pair * 128, pair * 128 + 128)
        keys = (i + 1) * tile
        for h in range(2):
            here = (lane // 64) == h
            query = jnp.where(here, q[win, at].astype(F32), 0.0).astype(BF)
            grad = jnp.where(here, do[win, at].astype(F32), 0.0).astype(BF)
            prob = p[pair % slots, h, pl.ds(0, keys), win]
            dp = dot(v[pl.ds(0, keys), at], grad, NT)
            ds = (prob.astype(F32) * (dp - held["d"][h][:, i * tile : (i + 1) * tile]) * 0.125).astype(BF)
            half = slice(64 * h, 64 * h + 64)
            dqt[half, win] = dot(held["k"][half, :keys], ds)
            dk[pl.ds(0, keys), :] += dot(ds, query)
            dv[pl.ds(0, keys), :] += dot(prob, grad)

    def end(pair):
        for t, val in enumerate((dqt[...].T, dk[...], dv[...])):
            at = slice((t * pairs + pair) * 128, (t * pairs + pair) * 128 + 128)
            low = val.astype(BF)
            sums[:, at] = jnp.sum(low.astype(F32), axis=0, keepdims=True)
            dqkv[:, at] = low

    spare = max(0, width - 128 * n)
    whole_tiles = width // hw

    def products(rows, x, y):
        out[rows, 3 * cols :] = dot(y, da[:, pl.ds(pl.multiple_of(me * 128, 128), 128)], TN).astype(BF)

        @pl.when(me < n - 1 if spare else me < n)
        def _():
            out[rows, : 3 * cols] = dot(x, dqkv[...], TN).astype(BF)

        if spare:

            @pl.when(me == n - 1)
            def _():
                out[rows, : 3 * cols] = jnp.zeros((x.shape[1], 3 * cols), BF)
                out[rows, :spare] = dot(y, da[:, 128 * n :], TN).astype(BF)

    def weights(lo, hi):
        if lo == 0:
            for load in loads:
                load.wait()

        def body(i, carry):
            at = pl.ds(pl.multiple_of(i * hw, hw), hw)
            products(at, h1[:, at], o_all[i])
            return carry

        lax.fori_loop(lo, hi, body, 0)
        if hi == whole_tiles and width % hw:
            rest = width % hw
            at = pl.ds(hi * hw, rest)
            products(at, h1[:, at], o_all[hi, :, :rest])

    part = functools.partial
    steps = []
    for pair in range(pairs):
        steps.append((1.0, part(begin, pair)))
        steps += [(0.6 + 0.5 * i, part(block, pair, i)) for i in range(length // tile)]
        steps.append((1.0, part(end, pair)))
    steps += [(3.8, part(weights, lo, min(lo + 2, whole_tiles))) for lo in range(0, whole_tiles, 2)]
    clock, work = 0.0, []
    for size, step in steps:
        work.append((clock, step))
        clock += size
    timed(work, gather.timed_steps(lambda c: 3.5 * c, 6.0, 5.0))
    gather.finish()


def back(n, cid, ready, q, k, v, o, do, da, p, h1, o_all):
    length, hw = q.shape
    width = da.shape[1]
    if 128 * n > width:
        da = jnp.pad(da, ((0, 0), (0, 128 * n - width)))
    assert width <= 128 * n or (n - 1) * hw >= width and width - 128 * n <= 3 * hw
    dma = pltpu.SemaphoreType.DMA
    slots = min(2, hw // 128)
    return call(
        functools.partial(back_kernel, n, 256, hw, width),
        cid,
        "back",
        (ready, q, k, v, o, do, da, p, h1, o_all),
        [VMEM] * 6 + [ANY] * 4,
        [
            ((n,) + ready.shape, BF),
            ((length, 3 * hw), BF),
            ((1, 3 * hw), F32),
            ((width, 3 * hw + 128), BF),
        ],
        [ANY, VMEM, VMEM, VMEM],
        [
            pltpu.VMEM(da.shape, BF),
            pltpu.VMEM((slots, 2, length, length), BF),
            pltpu.VMEM(h1.shape, BF),
            pltpu.VMEM(o_all.shape, BF),
            pltpu.VMEM((128, length), F32),
            pltpu.VMEM((length, 128), F32),
            pltpu.VMEM((length, 128), F32),
            dma((3,)),
            dma((slots,)),
        ]
        + Gather.sems(n, ready.shape[0]),
    )


def norm(values):
    centre = values - jnp.mean(values, axis=-1, keepdims=True)
    rstd = lax.rsqrt(jnp.mean(centre * centre, axis=-1, keepdims=True) + 1e-05)
    return centre * rstd, rstd


def norm_back(grad, unit, rstd, gain):
    inner = grad * gain
    return rstd * (
        inner
        - jnp.mean(inner, axis=-1, keepdims=True)
        - unit * jnp.mean(inner * unit, axis=-1, keepdims=True)
    )


def make_body(n, nz):
    def body(
        tokens, block_table, ln1_gain, ln1_bias, qkv_weight, query_bias, value_bias,
        proj_weight, proj_bias, ln2_gain, ln2_bias, fc_weight, fc_bias, out_weight,
        out_bias, cotangent,
    ):
        ctx = lax.axis_index("ctx")
        z = lax.axis_index("fsdp")
        rows, width = tokens.shape
        blk = rows // 2
        wz = width // nz
        slots = -(-HEADS // n)
        hw = slots * (width // HEADS)
        unit_z = out_weight.shape[0]
        uw = unit_z // n
        units = uw * nz
        table = block_table.reshape(-1)
        inv = jnp.argmax(
            table[None, :] == jnp.arange(table.shape[0], dtype=table.dtype)[:, None], axis=1
        ).astype(jnp.int32)

        take = lambda a, at, size, axis=0: lax.dynamic_slice_in_dim(a, at, size, axis)
        parts = 5
        padded = jnp.pad(qkv_weight, ((0, 0), (0, n * hw - width)))
        wq_own = jnp.concatenate(
            [take(padded, t * width + ctx * hw, hw, 1) for t in range(3)], axis=1
        ).reshape(parts, wz // parts, 3 * hw)
        row = lax.broadcasted_iota(jnp.int32, (16, wz), 0)
        small = jnp.zeros((16, wz), BF)
        for i, v in enumerate(
            [ln1_gain, ln1_bias, query_bias, value_bias, proj_bias, ln2_gain, ln2_bias, out_bias]
            + [jnp.pad(take(fc_bias, ctx * uw, uw), (0, wz - uw))]
        ):
            small = jnp.where(row == i, v[None, :], small)
        tile = math.gcd(wz, hw)
        h1, cot, small, w_qkv, w_proj, tok_own, cot_own, wfc_own, wout_own = entry(
            n,
            nz,
            tokens,
            cotangent,
            small,
            wq_own,
            proj_weight.reshape(wz // tile, tile, width),
            fc_weight.reshape(25, wz // 25, fc_weight.shape[1]),
            out_weight.reshape(n, uw, width),
            hw,
        )
        w_fc = lax.all_gather(wfc_own.reshape(wz, units), "fsdp", axis=0, tiled=True)
        w_out = lax.all_gather(wout_own, "fsdp", axis=0, tiled=True)
        length = n * rows
        flat = lambda a: a.reshape(length, a.shape[-1])
        h1, cot = flat(h1), flat(cot)
        w_qkv, w_proj = w_qkv.reshape(width, 3 * hw), w_proj.reshape(hw, width)
        fb = small[8].reshape(nz, wz)[:, :uw].reshape(1, units)
        pad_cols = lambda v: take(jnp.pad(v, (0, n * hw - width)), ctx * hw, hw)
        qkv_bias = jnp.concatenate([pad_cols(small[2]), jnp.zeros((hw,), F32), pad_cols(small[3])])

        qkv = (dot(h1, w_qkv) + qkv_bias).astype(BF)
        o, p, q_pos, k_pos, v_pos, o_pos = attend(qkv, inv, blk)
        mid, h2 = middle(n, 2, o, w_proj, tok_own, small)
        h2 = flat(h2)
        hidden, slope = hidden_units(h2, w_fc, fb)
        part_out = dot(hidden, cot, TN).astype(BF)
        in_parts = lambda a: a.reshape(nz, parts, a.shape[0] // nz // parts, a.shape[1])
        o, part_out = lax.optimization_barrier((o, part_out))
        o_all = spread(n, 3, o.reshape(4, length // 4, hw))
        h1_pos = order(h1, inv, blk)
        w_out, o_all, h1_pos = lax.optimization_barrier((w_out, o_all, h1_pos))
        to_owner = lambda a: lax.psum_scatter(a, "fsdp", scatter_dimension=0, tiled=True)
        sum_out = to_owner(part_out)
        du, dfb = hidden_back(cot, w_out, slope)
        part_fc = outer(h2, du)
        du, part_fc = lax.optimization_barrier((du, part_fc))
        sum_fc = to_owner(part_fc)
        da, dmid, layer_out, sums = turn(n, 4, du, w_fc, hidden, w_out, mid, cot_own, small)
        da = flat(da)
        all_out, dqkv, bias_cols, part_attn = back(
            n,
            6,
            sum_out.reshape(parts, uw // parts, width),
            q_pos,
            k_pos,
            v_pos,
            o_pos,
            heads_grad(da, w_proj, inv, blk),
            da,
            p,
            h1_pos,
            o_all.reshape(n, length, hw),
        )
        dqkv = order(dqkv, table, blk)

        put = lambda v, size: lax.dynamic_update_slice_in_dim(
            jnp.zeros((1, size), F32), v, ctx * v.shape[1], 1
        )
        biases = jnp.concatenate(
            [put(bias_cols[:, :hw], n * hw), put(bias_cols[:, 2 * hw :], n * hw)]
        )[:, :width]
        wide_fb = lax.dynamic_update_slice_in_dim(
            jnp.zeros((nz, unit_z), F32), dfb.reshape(nz, uw), ctx * uw, 1
        )
        vectors = jnp.concatenate(
            [sums + jnp.pad(biases, ((2, 4), (0, 0))), jnp.pad(wide_fb, ((0, -nz % 8), (0, width - unit_z)))]
        )
        all_fc, all_attn, grad_tokens, vectors = tail(
            n,
            nz,
            5,
            sum_fc.reshape(parts, wz // parts, units),
            in_parts(part_attn),
            dqkv,
            w_qkv,
            tok_own,
            dmid,
            small,
            vectors,
        )
        whole_rows = lambda a: a.reshape(n, a.shape[1] * a.shape[2], a.shape[3])
        grad_fc, grad_qkv, grad_proj, grad_out = join(
            n, nz, hw, whole_rows(all_fc), whole_rows(all_attn), all_out.reshape(unit_z, width)
        )
        mine = take(vectors[:8], z * wz, wz, 1)
        gfb = take(vectors[8 : 8 + nz], z, 1).reshape(-1)[:unit_z]
        return (
            layer_out,
            grad_tokens,
            mine[0],
            mine[1],
            grad_qkv,
            mine[2],
            mine[3],
            grad_proj,
            mine[4],
            mine[5],
            mine[6],
            grad_fc,
            gfb,
            grad_out,
            mine[7],
        )

    return body


def solution(mesh):
    both = P(("fsdp", "ctx"), None)
    vec, mat = P("fsdp"), P("fsdp", None)
    placed = (both, P(), vec, vec, mat, vec, vec, mat, vec, vec, vec, mat, vec, mat, vec, both)
    outs = (both, both, vec, vec, mat, vec, vec, mat, vec, vec, vec, mat, vec, mat, vec)
    return jax.shard_map(
        make_body(mesh.shape["ctx"], mesh.shape["fsdp"]),
        mesh=mesh,
        in_specs=placed,
        out_specs=outs,
        check_vma=False,
    )
```

```python
import functools
import math

import jax
import jax.numpy as jnp
from jax import lax
from jax.experimental import pallas as pl
from jax.experimental.pallas import tpu as pltpu
from jax.sharding import PartitionSpec as P

HEADS = 25
BF = jnp.bfloat16
F32 = jnp.float32
MESH = pl.DeviceIdType.MESH
ENTRY, ATTEND, MIDDLE, SPREAD, TURN, BACK, TAIL = 60, 60, 60, 60, 60, 60, 30
HIDDEN, HIDDEN_BACK, OUTER, ORDER, HEADS_GRAD, JOIN = 60, 60, 60, 60, 60, 8
ANY = pl.BlockSpec(memory_space=pl.ANY)
VMEM = pl.BlockSpec(memory_space=pltpu.VMEM)
HBM = pl.BlockSpec(memory_space=pltpu.HBM)
NN = (((1,), (0,)), ((), ()))
NT = (((1,), (1,)), ((), ()))
TN = (((0,), (0,)), ((), ()))


def room(length, mib):
    return pltpu.CompilerParams(vmem_limit_bytes=(mib if length <= 1024 else 60) * 1024 * 1024)


def dot(a, b, dims=NN):
    return lax.dot_general(a, b, dims, preferred_element_type=F32)


def places(n):
    me = lax.axis_index("ctx")
    core = lax.rem(me, 2)
    chip = me // 2
    sib = me + 1 - 2 * core
    if n == 8:
        across = chip + 1 - 2 * lax.rem(chip, 2)
        along = lax.rem(chip + 2, 4)
        first = across * (1 - core) + along * core
        second = along * (1 - core) + across * core
        others = [first, second, 3 - chip]
    else:
        half = n // 2
        others = [lax.rem(chip + d, half) for d in range(1, half)]
    return me, core, chip, sib, others


def twin(square, k):
    return 1 - k if square and k < 2 else k


def signal(sem, **device):
    pl.semaphore_signal(sem, inc=1, device_id=device, device_id_type=MESH)


def greet(devices, planes=()):
    barrier = pltpu.get_barrier_semaphore()
    for device in devices:
        signal(barrier, ctx=device)
    for plane in planes:
        signal(barrier, fsdp=plane)
    pl.semaphore_wait(barrier, len(devices) + len(planes))


def send(src, dst, ssem, rsem, **device):
    return pltpu.make_async_remote_copy(
        src_ref=src,
        dst_ref=dst,
        send_sem=ssem,
        recv_sem=rsem,
        device_id=device,
        device_id_type=MESH,
    )


def merge(*lists, scales=None):
    keyed = []
    for t, steps in enumerate(lists):
        scale = scales[t] if scales else 1.0
        keyed += [((i + 0.5) * scale / len(steps), t, i, step) for i, step in enumerate(steps)]
    for item in sorted(keyed, key=lambda k: k[:3]):
        item[3]()


def timed(*lists):
    keyed = [(time, t, i, step) for t, steps in enumerate(lists) for i, (time, step) in enumerate(steps)]
    for item in sorted(keyed, key=lambda k: k[:3]):
        item[3]()


def spaced(steps, start, stop):
    return [(start + (stop - start) * (i + 0.5) / len(steps), step) for i, step in enumerate(steps)]


class Gather:
    def __init__(self, n, src, out, sems):
        self.n, self.src, self.out = n, src, out
        self.own_s, self.sib_s, self.sib_r, self.far_s, self.far_r = sems
        self.parts = src.shape[0]
        self.square = n == 8
        self.me, self.core, self.chip, self.sib, self.others = places(n)
        half = n // 2
        if self.square:
            self.froms = self.others
        else:
            self.froms = [lax.rem(self.chip + half - d, half) for d in range(1, half)]
        self.peers = self.others[:2] if self.square else self.others
        self.started = []

    @staticmethod
    def sems(n, parts):
        dma = pltpu.SemaphoreType.DMA
        far = n // 2 - 1
        return [dma((parts,)), dma((far + 1, parts)), dma((far + 1, parts)), dma((far, parts)), dma((far, parts))]

    def own_sends(self, c):
        piece, slot = self.src.at[c], self.out.at[self.me, c]
        copies = [
            send(piece, slot, self.far_s.at[d, c], self.far_r.at[d, c], ctx=2 * p + self.core)
            for d, p in enumerate(self.peers)
        ]
        copies.append(send(piece, slot, self.sib_s.at[0, c], self.sib_r.at[0, c], ctx=self.sib))
        return copies + [pltpu.make_async_copy(piece, slot, self.own_s.at[c])]

    def go(self, copy):
        copy.start()
        self.started.append(copy)

    def start(self):
        for c in range(self.parts):
            self.start_part(c)

    def start_part(self, c):
        for copy in self.own_sends(c):
            copy.start()

    def arrived(self, d, c):
        piece = self.out.at[2 * self.froms[d] + self.core, c]
        send(piece, piece, self.far_s.at[d, c], self.far_r.at[d, c], ctx=self.sib).wait_recv()
        if self.square and d == 0:
            self.go(
                send(
                    piece,
                    piece,
                    self.far_s.at[2, c],
                    self.far_r.at[2, c],
                    ctx=2 * self.others[1] + self.core,
                )
            )
        e = twin(self.square, d) + 1
        self.go(send(piece, piece, self.sib_s.at[e, c], self.sib_r.at[e, c], ctx=self.sib))

    def steps(self):
        todo = []
        for c in range(self.parts):
            for d in range(2 if self.square else len(self.others)):
                todo.append(functools.partial(self.arrived, d, c))
            if self.square and c:
                todo.append(functools.partial(self.arrived, 2, c - 1))
        if self.square:
            todo.append(functools.partial(self.arrived, 2, self.parts - 1))
        return todo

    def timed_steps(self, begin, wait, relay):
        todo = []
        for c in range(self.parts):
            for d in range(len(self.others)):
                late = relay if self.square and d == 2 else 0
                todo.append((begin(c) + wait + late, functools.partial(self.arrived, d, c)))
        return todo

    def finish(self):
        for c in range(self.parts):
            *far, own = self.own_sends(c)
            own.wait()
            for copy in far:
                copy.wait_send()
        for d in range(len(self.others) + 1):
            chip = self.chip if d == 0 else self.froms[d - 1]
            for c in range(self.parts):
                piece = self.out.at[2 * chip + 1 - self.core, c]
                send(
                    piece, piece, self.sib_s.at[d, c], self.sib_r.at[d, c], ctx=self.sib
                ).wait_recv()
        for copy in self.started:
            copy.wait_send()


class Relay:
    def __init__(self, nz, z, lo, hi, count, src, out, sems, lead):
        self.nz, self.z, self.lo, self.hi, self.count = nz, z, lo, hi, count
        self.src, self.out, self.lead = src, out, lead
        self.own_s, self.up_s, self.down_s, self.recv = sems

    @staticmethod
    def sems(blocks):
        return [pltpu.SemaphoreType.DMA((blocks,)) for _ in range(4)]

    def up(self, src, b):
        return send(src, self.out.at[b], self.up_s.at[b], self.recv.at[b], fsdp=self.z + 1)

    def down(self, src, b):
        return send(src, self.out.at[b], self.down_s.at[b], self.recv.at[b], fsdp=self.z - 1)

    def own(self, b):
        return pltpu.make_async_copy(self.src.at[b - self.lead], self.out.at[b], self.own_s.at[b])

    def start(self):
        lo, hi = self.lo, self.hi

        def body(i, carry):
            u, d = hi - 1 - i, lo + i

            @pl.when(self.z < self.nz - 1)
            def _():
                self.up(self.src.at[u - self.lead], u).start()

            @pl.when(self.z > 0)
            def _():
                self.down(self.src.at[d - self.lead], d).start()

            self.own(d).start()
            return carry

        lax.fori_loop(0, hi - lo, body, 0)

    def step(self, i):
        b = self.lo - 1 - i

        @pl.when(b >= 0)
        def _():
            self.up(self.out.at[b], b).wait_recv()

            @pl.when(self.z < self.nz - 1)
            def _():
                self.up(self.out.at[b], b).start()

        e = self.hi + i

        @pl.when(e < self.count)
        def _():
            self.down(self.out.at[e], e).wait_recv()

            @pl.when(self.z > 0)
            def _():
                self.down(self.out.at[e], e).start()

    def steps(self, most):
        return [functools.partial(self.step, i) for i in range(most)]

    def finish(self):
        def sent(b, carry):
            @pl.when((self.z < self.nz - 1) & (b < self.hi))
            def _():
                self.up(self.out.at[b], b).wait_send()

            @pl.when((self.z > 0) & (b >= self.lo))
            def _():
                self.down(self.out.at[b], b).wait_send()

            @pl.when((b >= self.lo) & (b < self.hi))
            def _():
                self.own(b).wait()

            return carry

        lax.fori_loop(0, self.count, sent, 0)


def others_of(z, nz):
    return [lax.rem(z + d, nz) for d in range(1, nz)]


def entry_kernel(
    n, nz, tok_t, cot_t, small, wq, wp, fc_hbm, out_hbm, h1_all, cot_all, vec, wq_all, wp_all, tok, cot_own,
    fc_own, out_own, *scratch
):
    cot, h1, inbox, zeros, fc_all, load_s, small_s, small_r, zero_s = scratch[:9]
    g_h, g_c = scratch[9:14], scratch[14:19]
    r_q, r_p = scratch[19:23], scratch[23:27]
    loads = [
        pltpu.make_async_copy(fc_hbm, fc_all, load_s.at[0]),
        pltpu.make_async_copy(out_hbm.at[lax.axis_index("ctx")], out_own, load_s.at[1]),
    ]
    me, core, chip, sib, others = places(n)
    z = lax.axis_index("fsdp")
    planes = others_of(z, nz)
    greet([sib] + [2 * p + core for p in (others[:2] if n == 8 else others)], planes)
    wz = small.shape[1]
    for d, plane in enumerate(planes):
        send(small, inbox.at[z], small_s.at[d], small_r.at[d], fsdp=plane).start()
    inbox[z] = small[...]
    k = wq.shape[0]
    relay_q = Relay(nz, z, z * k, (z + 1) * k, nz * k, wq, wq_all, r_q, z * k)
    relay_q.start()
    parts, rows = h1.shape[0], h1.shape[1]
    turned = cot_t[...].astype(F32).T.astype(BF)
    cot_own[...] = turned
    for c in range(parts):
        cot[c] = turned[c * rows : (c + 1) * rows, :]
    gather_c = Gather(n, cot, cot_all, g_c)
    gather_c.start()
    tok[...] = tok_t[...].astype(F32).T.astype(BF)
    share, blocks = wp.shape[0], wp_all.shape[0]
    base = me * blocks
    valid = jnp.clip(nz * share - base, 0, blocks)
    lo = jnp.clip(z * share - base, 0, valid)
    hi = jnp.clip((z + 1) * share - base, 0, valid)
    relay_p = Relay(nz, z, lo, hi, valid, wp, wp_all, r_p, z * share - base)
    relay_p.start()
    zeros[...] = jnp.zeros_like(zeros)

    def clear(b, carry):
        pltpu.make_async_copy(zeros, wp_all.at[b], zero_s.at[b]).start()
        return carry

    lax.fori_loop(valid, blocks, clear, 0)
    for d in range(nz - 1):
        came = lax.rem(z + nz - 1 - d, nz)
        send(small, inbox.at[came], small_s.at[d], small_r.at[d], fsdp=planes[d]).wait_recv()
    for p in range(nz):
        vec[:, p * wz : (p + 1) * wz] = inbox[p].astype(F32)
    gain, shift = vec[0:1, :], vec[1:2, :]
    gather_h = Gather(n, h1, h1_all, g_h)
    for c in range(parts):
        unit, _ = norm(tok[c * rows : (c + 1) * rows, :].astype(F32))
        h1[c] = (unit * gain + shift).astype(BF)
        gather_h.start_part(c)
    for load in loads:
        load.start()

    def columns():
        for load in loads:
            load.wait()
        uw = fc_own.shape[-1] // nz
        for place in range(n):

            @pl.when(me == place)
            def _():
                def tile(i, carry):
                    for t in range(nz):
                        at = (t * n + place) * uw
                        fc_own[i, :, t * uw : (t + 1) * uw] = fc_all[i, :, at : at + uw]
                    return carry

                lax.fori_loop(0, fc_own.shape[0], tile, 0)

    steps = gather_c.steps() + gather_h.steps()
    merge(
        steps[:4] + [columns] + steps[4:],
        relay_q.steps(nz * k - k) + relay_p.steps(blocks),
    )
    gather_c.finish()
    gather_h.finish()
    relay_q.finish()
    relay_p.finish()

    def cleared(b, carry):
        pltpu.make_async_copy(zeros, wp_all.at[b], zero_s.at[b]).wait()
        return carry

    lax.fori_loop(valid, blocks, cleared, 0)
    for d, plane in enumerate(planes):
        send(small, inbox.at[z], small_s.at[d], small_r.at[d], fsdp=plane).wait_send()


def entry(n, nz, tokens, cot, small, wq, wp, fc, out, hw):
    rows, width = tokens.shape
    parts = 2 if n == 8 else 1
    dma = pltpu.SemaphoreType.DMA
    k, tile = wq.shape[0], wp.shape[1]
    blocks = hw // tile
    shape = jax.ShapeDtypeStruct
    piece = (parts, rows // parts, width)
    return pl.pallas_call(
        functools.partial(entry_kernel, n, nz),
        out_shape=[
            shape((n,) + piece, BF),
            shape((n,) + piece, BF),
            shape((small.shape[0], width), F32),
            shape((nz * k,) + wq.shape[1:], BF),
            shape((blocks, tile, width), BF),
            shape((rows, width), BF),
            shape((rows, width), BF),
            shape(fc.shape[:2] + (fc.shape[2] // n,), BF),
            shape(out.shape[1:], BF),
        ],
        in_specs=[VMEM] * 5 + [HBM, HBM],
        out_specs=[ANY, ANY, VMEM, ANY, ANY] + [VMEM] * 4,
        scratch_shapes=[
            pltpu.VMEM(piece, BF),
            pltpu.VMEM(piece, BF),
            pltpu.VMEM((nz,) + small.shape, BF),
            pltpu.VMEM((tile, width), BF),
            pltpu.VMEM(fc.shape, BF),
            dma((2,)),
            dma((nz - 1,)),
            dma((nz - 1,)),
            dma((blocks,)),
        ]
        + Gather.sems(n, parts)
        + Gather.sems(n, parts)
        + Relay.sems(nz * k)
        + Relay.sems(blocks),
        compiler_params=pltpu.CompilerParams(
            collective_id=1, has_side_effects=True, vmem_limit_bytes=(ENTRY if n == 8 else 60) * 1024 * 1024
        ),
        name="entry",
    )(tokens.T, cot.T, small, wq, wp, fc, out)


class Scatter:
    def __init__(self, n, dims, a, w, scratch):
        self.n, self.dims, self.a, self.w = n, dims, a, w
        self.part, self.theirs, self.sums, self.inbox = scratch[:4]
        self.sib_s, self.sib_r, self.far_s, self.far_r = scratch[4:]
        self.me, self.core, self.chip, self.sib, self.others = places(n)
        self.square = n == 8
        self.half = n // 2
        self.parts = self.sib_s.shape[1]
        self.full = self.part.shape[2]
        self.rows = self.full // self.parts
        if self.square:
            first, second = [2 * p + self.core for p in self.others[:2]]
            self.ends = [(0, 0, first), (1, 1, first), (2, 2, second)]
        else:
            self.ends = [(k, k, 2 * self.others[k] + self.core) for k in range(self.half - 1)]

    @staticmethod
    def scratch(n, rows, width):
        dma = pltpu.SemaphoreType.DMA
        half, parts = n // 2, 4 if n == 8 else 1
        return [
            pltpu.VMEM((half, 2, rows, width), BF),
            pltpu.VMEM((half, rows, width), BF),
            pltpu.VMEM((half - 1, rows, width), BF),
            pltpu.VMEM((half - 1, rows, width), BF),
            dma((half, parts)),
            dma((half, parts)),
            dma((half - 1, parts)),
            dma((half - 1, parts)),
        ]

    def chip_at(self, k):
        if not self.square:
            return lax.rem(self.chip + 1 + k, self.half)
        x, y = lax.rem(self.chip, 2), self.chip // 2
        first, second = 1 - lax.rem(k, 3) // 2, 1 - lax.rem(k, 2)
        dx = first * (1 - self.core) + second * self.core
        dy = second * (1 - self.core) + first * self.core
        far = (k < 3).astype(jnp.int32)
        dx, dy = dx * far, dy * far
        return (y + dy - 2 * y * dy) * 2 + x + dx - 2 * x * dx

    def twin_at(self, k):
        if not self.square:
            return k
        return k + jnp.where(k == 1, 1, 0) - jnp.where(k == 2, 1, 0)

    def win(self, c):
        return pl.ds(c * self.rows, self.rows)

    def to_sib(self, k, c):
        e = self.twin_at(k)
        return send(
            self.part.at[k, 1 - self.core, self.win(c)],
            self.theirs.at[e, self.win(c)],
            self.sib_s.at[e, c],
            self.sib_r.at[e, c],
            ctx=self.sib,
        )

    def chip_sum(self, k, c):
        win = self.win(c)
        piece = self.theirs.at[k, win]
        send(piece, piece, self.sib_s.at[k, c], self.sib_r.at[k, c], ctx=self.sib).wait_recv()
        return self.part[k, self.core, win, :].astype(F32) + self.theirs[k, win, :].astype(F32)

    def pass_on(self, k, slot, peer, c):
        return send(
            self.sums.at[k, self.win(c)],
            self.inbox.at[slot, self.win(c)],
            self.far_s.at[slot, c],
            self.far_r.at[slot, c],
            ctx=peer,
        )

    def wait_in(self, slot, c):
        piece = self.inbox.at[slot, self.win(c)]
        send(piece, piece, self.far_s.at[slot, c], self.far_r.at[slot, c], ctx=self.sib).wait_recv()
        return self.inbox[slot, self.win(c), :].astype(F32)

    def forward(self, end, c):
        k, slot, peer = self.ends[end]
        total = self.chip_sum(k, c)
        if self.square and end == 2:
            total = total + self.wait_in(0, c)
        self.sums[k, self.win(c), :] = total.astype(BF)
        self.pass_on(k, slot, peer, c).start()

    def products(self):
        def product(k, carry):
            full = self.full
            at = pl.ds(pl.multiple_of(self.chip_at(k) * 2 * full, 2 * full), 2 * full)
            val = dot(self.a[at, :], self.w[...], self.dims).astype(BF)
            self.part[k, 0] = val[:full]
            self.part[k, 1] = val[full:]
            for c in range(self.parts):
                self.to_sib(k, c).start()

            @pl.when(k == 1)
            def _():
                for c in range(self.parts):
                    self.forward(0, c)

            return carry

        lax.fori_loop(0, self.half, product, 0)

    def forwards(self):
        each = range(self.parts)
        return [functools.partial(self.forward, e, c) for e in range(1, self.half - 1) for c in each]

    def total(self, c):
        val = self.chip_sum(self.half - 1, c)
        for slot in (1, 2) if self.square else range(self.half - 1):
            val = val + self.wait_in(slot, c)
        return val

    def finish(self):
        for c in range(self.parts):
            for k, slot, peer in self.ends:
                self.pass_on(k, slot, peer, c).wait_send()

        def sent(k, carry):
            for c in range(self.parts):
                self.to_sib(k, c).wait_send()
            return carry

        lax.fori_loop(0, self.half, sent, 0)


class Line:
    def __init__(self, nz, z, src, out, scratch):
        self.nz, self.z, self.src, self.out = nz, z, src, out
        self.mine, self.above, self.below, self.load_s, self.up_s, self.down_s, self.recv = scratch
        self.parts = src.shape[1]

    @staticmethod
    def scratch(shape):
        dma, lead = pltpu.SemaphoreType.DMA, shape[:2]
        return [pltpu.VMEM(shape, BF)] * 3 + [dma((1,)), dma(lead), dma(lead), dma((2,) + lead)]

    def up(self, src, d, c):
        return send(
            src.at[d, c], self.above.at[d, c], self.up_s.at[d, c], self.recv.at[0, d, c], fsdp=self.z + 1
        )

    def down(self, src, d, c):
        return send(
            src.at[d, c], self.below.at[d, c], self.down_s.at[d, c], self.recv.at[1, d, c], fsdp=self.z - 1
        )

    def start(self):
        top = self.nz - 1

        @pl.when(self.z == 0)
        def _():
            for c in range(self.parts):
                for k in range(top):
                    self.up(self.src, top - k, c).start()

        @pl.when(self.z == top)
        def _():
            for c in range(self.parts):
                for k in range(top):
                    self.down(self.src, k, c).start()

        self.load = pltpu.make_async_copy(self.src, self.mine, self.load_s.at[0])
        self.load.start()

    def loaded(self):
        self.load.wait()

    def pass_up(self, d, c):
        copy = self.up(self.mine, d, c)
        copy.wait_recv()
        self.mine[d, c] = self.mine[d, c] + self.above[d, c]
        copy.start()

    def pass_down(self, d, c):
        copy = self.down(self.mine, d, c)
        copy.wait_recv()
        self.mine[d, c] = self.mine[d, c] + self.below[d, c]
        copy.start()

    def settle(self, place, c):
        z, top = place, self.nz - 1
        total = self.mine[z, c].astype(F32)
        if z > 0:
            self.up(self.mine, z, c).wait_recv()
            total = total + self.above[z, c].astype(F32)
        if z < top:
            self.down(self.mine, z, c).wait_recv()
            total = total + self.below[z, c].astype(F32)
        self.out[c] = total.astype(BF)

    def timed_steps(self, after):
        top = self.nz - 1
        slots = {}

        def put(time, place, fn):
            slots.setdefault(time, {}).setdefault(place, []).append(fn)

        for c in range(self.parts):
            for place in range(self.nz):
                for k in range(top):
                    at = c * top + k
                    if 0 < place < top - k:
                        put(at + place, place, functools.partial(self.pass_up, top - k, c))
                    if k < place < top:
                        put(at + top - place, place, functools.partial(self.pass_down, k, c))
                put((c + 1) * top, place, functools.partial(self.settle, place, c))
                put((c + 1) * top, place, functools.partial(after, c))

        def run(work):
            for place, fns in sorted(work.items()):

                @pl.when(self.z == place)
                def _():
                    for fn in fns:
                        fn()

        return [(0, self.loaded)] + [(t, functools.partial(run, slots[t])) for t in sorted(slots)]

    def finish(self):
        for d in range(self.nz):

            @pl.when(self.z < d)
            def _():
                for c in range(self.parts):
                    self.up(self.mine, d, c).wait_send()

            @pl.when(self.z > d)
            def _():
                for c in range(self.parts):
                    self.down(self.mine, d, c).wait_send()


class Vectors:
    def __init__(self, n, nz, src, out, scratch):
        self.n, self.nz, self.src, self.out = n, nz, src, out
        self.low, self.from_sib, self.chips, self.line = scratch[:4]
        self.ss, self.sr, self.cs, self.cr, self.ls, self.lr = scratch[4:]
        self.me, self.core, self.chip, self.sib, self.others = places(n)
        self.z = lax.axis_index("fsdp")
        self.planes = others_of(self.z, nz)

    @staticmethod
    def scratch(n, nz, shape):
        dma = pltpu.SemaphoreType.DMA
        half = n // 2
        return [
            pltpu.VMEM(shape, BF),
            pltpu.VMEM(shape, BF),
            pltpu.VMEM((half,) + shape, BF),
            pltpu.VMEM((nz,) + shape, BF),
            dma((1,)),
            dma((1,)),
            dma((half - 1,)),
            dma((half - 1,)),
            dma((nz - 1,)),
            dma((nz - 1,)),
        ]

    def to_sib(self):
        return send(self.low, self.from_sib, self.ss.at[0], self.sr.at[0], ctx=self.sib)

    def to_chip(self, d):
        at = self.chips.at[self.chip]
        return send(at, at, self.cs.at[d], self.cr.at[d], ctx=2 * self.others[d] + self.core)

    def to_plane(self, d):
        at = self.line.at[self.z]
        return send(at, at, self.ls.at[d], self.lr.at[d], fsdp=self.planes[d])

    def start(self):
        self.low[...] = self.src[...].astype(BF)
        self.to_sib().start()

    def first(self):
        self.to_sib().wait_recv()
        self.chips[self.chip] = self.low[...] + self.from_sib[...]
        for d in range(self.n // 2 - 1):
            self.to_chip(d).start()

    def second(self):
        for d in range(self.n // 2 - 1):
            self.to_chip(d).wait_recv()
        total = self.chips[0].astype(F32)
        for k in range(1, self.n // 2):
            total = total + self.chips[k].astype(F32)
        self.line[self.z] = total.astype(BF)
        for d in range(self.nz - 1):
            self.to_plane(d).start()

    def third(self):
        for d in range(self.nz - 1):
            self.to_plane(d).wait_recv()
        total = self.line[0].astype(F32)
        for k in range(1, self.nz):
            total = total + self.line[k].astype(F32)
        self.out[...] = total

    def steps(self):
        return [self.first, self.second, self.third]

    def finish(self):
        self.to_sib().wait_send()
        for d in range(self.n // 2 - 1):
            self.to_chip(d).wait_send()
        for d in range(self.nz - 1):
            self.to_plane(d).wait_send()


def beside(n):
    me, core, chip, sib, others = places(n)
    return [sib] + [2 * p + core for p in (others[:2] if n == 8 else others)]


def call(kernel, cid, name, ins, in_specs, outs, out_specs, scratch, mib=60):
    return pl.pallas_call(
        kernel,
        out_shape=[jax.ShapeDtypeStruct(*o) for o in outs],
        in_specs=in_specs,
        out_specs=out_specs,
        scratch_shapes=scratch,
        compiler_params=pltpu.CompilerParams(
            collective_id=cid, has_side_effects=True, vmem_limit_bytes=mib * 1024 * 1024
        ),
        name=name,
    )(*ins)


def middle_kernel(n, o, w, tok, vec, mid, h2_all, h2, *scratch):
    greet(beside(n))
    scatter = Scatter(n, NN, o, w, scratch[:8])
    gather = Gather(n, h2, h2_all, scratch[8:])
    scatter.products()
    for step in scatter.forwards():
        step()
    for c in range(gather.parts):
        win = scatter.win(c)
        val = tok[win, :].astype(F32) + scatter.total(c) + vec[4:5, :]
        mid[win, :] = val
        h2[c] = (norm(val)[0] * vec[5:6, :] + vec[6:7, :]).astype(BF)
        gather.start_part(c)
    for step in gather.steps():
        step()
    gather.finish()
    scatter.finish()


def middle(n, cid, o, w, tok, vec):
    rows, width = tok.shape
    parts = 4 if n == 8 else 1
    piece = (parts, rows // parts, width)
    return call(
        functools.partial(middle_kernel, n),
        cid,
        "middle",
        (o, w, tok, vec),
        [VMEM] * 4,
        [((rows, width), F32), ((n,) + piece, BF)],
        [VMEM, ANY],
        [pltpu.VMEM(piece, BF)] + Scatter.scratch(n, rows, width) + Gather.sems(n, parts),
        MIDDLE if n == 8 else 60,
    )


def spread_kernel(n, src, all_ref, *sems):
    greet(beside(n))
    gather = Gather(n, src, all_ref, sems)
    gather.start()
    for step in gather.steps():
        step()
    gather.finish()


def spread(n, cid, array):
    return call(
        functools.partial(spread_kernel, n),
        cid,
        "spread",
        (array,),
        [VMEM],
        [((n,) + array.shape, BF)],
        [ANY],
        Gather.sems(n, array.shape[0]),
        SPREAD if n == 8 else 60,
    )[0]


def turn_kernel(n, du, w_fc, hid, w_out, mid, cot, vec, da_all, dmid, layer, sums, da, *scratch):
    greet(beside(n))
    back = Scatter(n, NT, du, w_fc, scratch[:8])
    ahead = Scatter(n, NN, hid, w_out, scratch[8:16])
    gather = Gather(n, da, da_all, scratch[16:])
    back.products()
    todo = back.forwards()
    for step in todo[: back.parts]:
        step()
    ahead.products()
    for step in todo[back.parts :]:
        step()
    sums[...] = jnp.zeros_like(sums)
    for c in range(gather.parts):
        win = back.win(c)
        grad = back.total(c)
        unit, rstd = norm(mid[win, :])
        up = cot[win, :].astype(F32)
        val = up + norm_back(grad, unit, rstd, vec[5:6, :])
        dmid[win, :] = val
        low = val.astype(BF)
        da[c] = low
        gather.start_part(c)
        for row, term in ((4, low.astype(F32)), (5, grad * unit), (6, grad), (7, up)):
            sums[row : row + 1, :] += jnp.sum(term, axis=0, keepdims=True)
    merge(gather.steps(), ahead.forwards())
    for c in range(gather.parts):
        win = ahead.win(c)
        layer[win, :] = (mid[win, :] + ahead.total(c) + vec[7:8, :]).astype(BF)
    gather.finish()
    back.finish()
    ahead.finish()


def turn(n, cid, du, w_fc, hidden, w_out, mid, cot, vec):
    rows, width = mid.shape
    parts = 4 if n == 8 else 1
    piece = (parts, rows // parts, width)
    return call(
        functools.partial(turn_kernel, n),
        cid,
        "turn",
        (du, w_fc, hidden, w_out, mid, cot, vec),
        [VMEM] * 7,
        [((n,) + piece, BF), ((rows, width), F32), ((rows, width), BF), ((8, width), F32)],
        [ANY, VMEM, VMEM, VMEM],
        [pltpu.VMEM(piece, BF)]
        + Scatter.scratch(n, rows, width)
        + Scatter.scratch(n, rows, width)
        + Gather.sems(n, parts),
        TURN if n == 8 else 60,
    )


def tail_kernel(
    n, nz, fc, part, dqkv, w_qkv, tok, dmid, vec, v_in, fc_all, attn_all, g_tok, v_out,
    v_own, attn, fc_v, dqkv_v, w_v, load_s, *scratch,
):
    z = lax.axis_index("fsdp")
    me, core, chip, sib, others = places(n)
    greet([sib] + [2 * p + core for p in others], others_of(z, nz))
    line = Line(nz, z, part, attn, scratch[:7])
    line.start()
    loads = [
        pltpu.make_async_copy(src, dst, load_s.at[i])
        for i, (src, dst) in enumerate([(dqkv, dqkv_v), (w_qkv, w_v), (fc, fc_v)])
    ]
    for load in loads:
        load.start()
    fc, dqkv, w_qkv = fc_v, dqkv_v, w_v
    scatter = Scatter(n, NT, dqkv, w_qkv, scratch[7:15])
    vectors = Vectors(n, nz, v_own, v_out, scratch[15:25])
    fc_g = Gather(n, fc, fc_all, scratch[25:30])
    attn_g = Gather(n, attn, attn_all, scratch[30:35])
    v_own[...] = v_in[...]
    for load in loads[:2]:
        load.wait()
    scatter.products()
    todo = scatter.forwards()
    for step in todo[: scatter.parts]:
        step()
    loads[2].wait()

    def rest(c):
        win = scatter.win(c)
        grad = scatter.total(c)
        unit, rstd = norm(tok[win, :].astype(F32))
        g_tok[win, :] = (dmid[win, :] + norm_back(grad, unit, rstd, vec[0:1, :])).astype(BF)
        v_own[0:1, :] += jnp.sum(grad * unit, axis=0, keepdims=True)
        v_own[1:2, :] += jnp.sum(grad, axis=0, keepdims=True)

    top = nz - 1
    last = attn_g.parts * top
    part_at = functools.partial
    fc_at = lambda c: 4.0 + 2.0 * c
    timed(
        spaced(todo[scatter.parts :], 1.0, 4.0),
        spaced([part_at(rest, c) for c in range(scatter.parts)], 4.5, 7.0),
        [(7.1, vectors.start), (7.8, vectors.first), (11.0, vectors.second), (last + 3.0, vectors.third)],
        [(fc_at(c), part_at(fc_g.start_part, c)) for c in range(fc_g.parts)],
        fc_g.timed_steps(fc_at, 2.2, 1.6),
        line.timed_steps(attn_g.start_part),
        attn_g.timed_steps(lambda c: (c + 1) * top, 2.2, 1.6),
    )
    for job in (fc_g, attn_g, scatter, line, vectors):
        job.finish()


def tail(n, nz, cid, fc, part, dqkv, w_qkv, tok, dmid, vec, v_in):
    rows, width = tok.shape
    attn = part.shape[1:]
    return call(
        functools.partial(tail_kernel, n, nz),
        cid,
        "tail",
        (fc, part, dqkv, w_qkv, tok, dmid, vec, v_in),
        [HBM] * 4 + [VMEM] * 4,
        [((n,) + fc.shape, BF), ((n,) + attn, BF), (tok.shape, BF), (v_in.shape, F32)],
        [ANY, ANY, VMEM, VMEM],
        [pltpu.VMEM(v_in.shape, F32), pltpu.VMEM(attn, BF)]
        + [pltpu.VMEM(a.shape, BF) for a in (fc, dqkv, w_qkv)]
        + [pltpu.SemaphoreType.DMA((3,))]
        + Line.scratch(part.shape)
        + Scatter.scratch(n, rows, width)
        + Vectors.scratch(n, nz, v_in.shape)
        + Gather.sems(n, fc.shape[0])
        + Gather.sems(n, attn[0]),
        TAIL if n == 8 else 60,
    )


def outer_kernel(x_ref, y_ref, out_ref):
    out_ref[...] = dot(x_ref[...], y_ref[...], TN).astype(BF)


def outer(x, y):
    rows, m = x.shape
    tile = 256
    return pl.pallas_call(
        outer_kernel,
        grid=(pl.cdiv(m, tile),),
        out_shape=jax.ShapeDtypeStruct((m, y.shape[1]), BF),
        in_specs=[pl.BlockSpec((rows, tile), lambda i: (0, i)), fixed(*y.shape)],
        out_specs=tiled(tile, y.shape[1]),
        compiler_params=room(rows, OUTER),
        name="outer",
    )(x, y)


def hidden_kernel(h_ref, w_ref, b_ref, z_ref, s_ref):
    u = dot(h_ref[...], w_ref[...]) + b_ref[...]
    root = 0.7978845608028654
    square = u * u
    inner = jnp.tanh(root * u * (1.0 + 0.044715 * square))
    z_ref[...] = (0.5 * u * (1.0 + inner)).astype(BF)
    slope = 0.5 * (1.0 + inner) + 0.5 * u * (1.0 - inner * inner) * root * (1.0 + 3 * 0.044715 * square)
    s_ref[...] = slope.astype(BF)


def hidden_back_kernel(c_ref, w_ref, s_ref, d_ref, sum_ref):
    du = (dot(c_ref[...], w_ref[...], NT) * s_ref[...].astype(F32)).astype(BF)
    d_ref[...] = du

    @pl.when(pl.program_id(0) == 0)
    def _():
        sum_ref[...] = jnp.zeros_like(sum_ref)

    sum_ref[...] += jnp.sum(du.astype(F32), axis=0, keepdims=True)


def tiled(rows, cols):
    return pl.BlockSpec((rows, cols), lambda i: (i, 0))


def fixed(rows, cols):
    return pl.BlockSpec((rows, cols), lambda i: (0, 0))


def hidden_units(h2, w_fc, bias):
    rows, width = h2.shape
    units = w_fc.shape[1]
    tile = 256
    shape = jax.ShapeDtypeStruct((rows, units), BF)
    return pl.pallas_call(
        hidden_kernel,
        grid=(rows // tile,),
        out_shape=[shape, shape],
        in_specs=[tiled(tile, width), fixed(width, units), fixed(1, units)],
        out_specs=[tiled(tile, units), tiled(tile, units)],
        compiler_params=room(rows, HIDDEN),
        name="hidden",
    )(h2, w_fc, bias)


def hidden_back(cot, w_out, slope):
    rows, width = cot.shape
    units = w_out.shape[0]
    tile = 256
    return pl.pallas_call(
        hidden_back_kernel,
        grid=(rows // tile,),
        out_shape=[
            jax.ShapeDtypeStruct((rows, units), BF),
            jax.ShapeDtypeStruct((1, units), F32),
        ],
        in_specs=[tiled(tile, width), fixed(units, width), tiled(tile, units)],
        out_specs=[tiled(tile, units), fixed(1, units)],
        compiler_params=room(rows, HIDDEN_BACK),
        name="hidden_back",
    )(cot, w_out, slope)


def join_kernel(n, nz, hw, width, fc, qp, out, fc_o, qkv_o, proj_o, out_o):
    uw = fc.shape[-1] // nz
    for c in range(n):
        for b in range(nz):
            at = b * n * uw + c * uw
            fc_o[:, at : at + uw] = fc[c, 0, :, b * uw : (b + 1) * uw].astype(F32)
        size = min(128, width - c * 128)
        if size > 0:
            proj_o[:, c * 128 : c * 128 + size] = qp[c, 0, :, 3 * hw : 3 * hw + size].astype(F32)
        size = min(hw, width - c * hw)
        if size > 0:
            for t in range(3):
                at = t * width + c * hw
                qkv_o[:, at : at + size] = qp[c, 0, :, t * hw : t * hw + size].astype(F32)
    if 128 * n < width:
        proj_o[:, 128 * n :] = qp[n - 1, 0, :, : width - 128 * n].astype(F32)
    out_o[...] = out[...].astype(F32)


def join(n, nz, hw, fc, qp, out):
    tiles = 25
    width = out.shape[1]
    wz = fc.shape[1]
    split = lambda a: a.reshape(n, tiles, wz // tiles, a.shape[-1])
    fc, qp = split(fc), split(qp)
    wide = lambda a: pl.BlockSpec((n, 1, wz // tiles, a.shape[-1]), lambda i: (0, i, 0, 0))
    t, ot = wz // tiles, out.shape[0] // tiles
    cols = (n * fc.shape[-1], 3 * width, width)
    shape = jax.ShapeDtypeStruct
    return pl.pallas_call(
        functools.partial(join_kernel, n, nz, hw, width),
        grid=(tiles,),
        out_shape=[shape((wz, c), F32) for c in cols] + [shape(out.shape, F32)],
        in_specs=[wide(fc), wide(qp), tiled(ot, width)],
        out_specs=[tiled(t, c) for c in cols] + [tiled(ot, width)],
        compiler_params=room(1024, JOIN),
        name="join",
    )(fc, qp, out)


def attend_kernel(blocks, blk, tile, inv_ref, q_ref, k_ref, v_ref, o_ref, p_ref, qn, kn, vn, on, ot):
    length = blocks * blk
    for i in range(blocks):
        src, dst = pl.ds(pl.multiple_of(inv_ref[i] * blk, blk), blk), pl.ds(i * blk, blk)
        qn[dst, :] = q_ref[src, :]
        kn[dst, :] = k_ref[src, :]
        vn[dst, :] = v_ref[src, :]
    v_turned = vn[...].astype(F32).T.astype(BF)
    lane = lax.broadcasted_iota(jnp.int32, (1, 128), 1)
    above = lax.broadcasted_iota(jnp.int32, (tile, tile), 0) > lax.broadcasted_iota(
        jnp.int32, (tile, tile), 1
    )
    for i in range(length // tile):
        cols = pl.ds(i * tile, tile)
        keys = (i + 1) * tile
        for h in range(2):
            here = (lane // 64) == h
            q = jnp.where(here, qn[cols, :].astype(F32) * 0.125, 0.0).astype(BF)
            last = jnp.where(above, -1e30, dot(kn[pl.ds(i * tile, tile), :], q, NT))
            top = jnp.max(last, axis=0, keepdims=True)
            if i:
                early = dot(kn[pl.ds(0, i * tile), :], q, NT)
                top = jnp.maximum(top, jnp.max(early, axis=0, keepdims=True))
            last = jnp.exp(last - top)
            total = jnp.sum(last, axis=0, keepdims=True)
            if i:
                early = jnp.exp(early - top)
                total = total + jnp.sum(early, axis=0, keepdims=True)
            scale = 1.0 / total
            last = (last * scale).astype(BF)
            p_ref[h, pl.ds(i * tile, tile), cols] = last
            half = slice(64 * h, 64 * h + 64)
            o = dot(v_turned[half, i * tile : keys], last)
            if i:
                early = (early * scale).astype(BF)
                p_ref[h, pl.ds(0, i * tile), cols] = early
                o = o + dot(v_turned[half, : i * tile], early)
            ot[half, cols] = o
    on[...] = ot[...].T.astype(BF)
    for i in range(blocks):
        o_ref[pl.ds(pl.multiple_of(inv_ref[i] * blk, blk), blk), :] = on[i * blk : (i + 1) * blk, :]


def attend(qkv, inv, blk):
    length = qkv.shape[0]
    cols = qkv.shape[1] // 3
    pairs = cols // 128
    blocks = inv.shape[0]
    tile = 256
    piece = lambda off: pl.BlockSpec((length, 128), lambda p, s: (0, off * pairs + p))
    return pl.pallas_call(
        functools.partial(attend_kernel, blocks, blk, tile),
        out_shape=[
            jax.ShapeDtypeStruct((length, cols), BF),
            jax.ShapeDtypeStruct((2 * pairs, length, length), BF),
        ]
        + [jax.ShapeDtypeStruct((length, cols), BF)] * 4,
        grid_spec=pltpu.PrefetchScalarGridSpec(
            num_scalar_prefetch=1,
            grid=(pairs,),
            in_specs=[piece(0), piece(1), piece(2)],
            out_specs=[
                pl.BlockSpec((length, 128), lambda p, s: (0, p)),
                pl.BlockSpec((2, length, length), lambda p, s: (p, 0, 0)),
            ]
            + [pl.BlockSpec((length, 128), lambda p, s: (0, p))] * 4,
            scratch_shapes=[pltpu.VMEM((128, length), F32)],
        ),
        compiler_params=room(length, ATTEND),
        name="attend",
    )(inv, qkv, qkv, qkv)


def order_kernel(blocks, blk, table, x, out):
    for i in range(blocks):
        src = pl.ds(pl.multiple_of(table[i] * blk, blk), blk)
        out[i * blk : (i + 1) * blk, :] = x[src, :]


def order(x, table, blk):
    return pl.pallas_call(
        functools.partial(order_kernel, table.shape[0], blk),
        out_shape=jax.ShapeDtypeStruct(x.shape, x.dtype),
        in_specs=[pl.BlockSpec(memory_space=pltpu.SMEM), VMEM],
        out_specs=VMEM,
        compiler_params=room(x.shape[0], ORDER),
        name="order",
    )(table, x)


def heads_kernel(blocks, blk, tile, table, da, w, out, rows):
    step = pl.program_id(0)
    rows[pl.ds(pl.multiple_of(step * tile, tile), tile), :] = dot(da[...], w[...], NT).astype(BF)

    @pl.when(step == pl.num_programs(0) - 1)
    def _():
        for i in range(blocks):
            src = pl.ds(pl.multiple_of(table[i] * blk, blk), blk)
            out[i * blk : (i + 1) * blk, :] = rows[src, :]


def heads_grad(da, w_proj, table, blk):
    length, width = da.shape
    cols = w_proj.shape[0]
    tile = 256
    return pl.pallas_call(
        functools.partial(heads_kernel, table.shape[0], blk, tile),
        out_shape=jax.ShapeDtypeStruct((length, cols), BF),
        grid_spec=pltpu.PrefetchScalarGridSpec(
            num_scalar_prefetch=1,
            grid=(length // tile,),
            in_specs=[
                pl.BlockSpec((tile, width), lambda i, s: (i, 0)),
                pl.BlockSpec((cols, width), lambda i, s: (0, 0)),
            ],
            out_specs=pl.BlockSpec((length, cols), lambda i, s: (0, 0)),
            scratch_shapes=[pltpu.VMEM((length, cols), BF)],
        ),
        compiler_params=room(length, HEADS_GRAD),
        name="heads_grad",
    )(table, da, w_proj)


def back_kernel(
    n, tile, hw, width, ready, q, k, v, o, do, da_hbm, p_hbm, h1_hbm, all_hbm,
    ready_all, dqkv, sums, out,
    da, p, h1, o_all, dqt, dk, dv, load_s, p_s, *sems,
):
    me = lax.axis_index("ctx")
    length, cols = q.shape
    pairs = cols // 128
    slots = p.shape[0]
    greet(beside(n))
    gather = Gather(n, ready, ready_all, sems)
    gather.start()
    loads = [
        pltpu.make_async_copy(src, dst, load_s.at[i])
        for i, (src, dst) in enumerate([(da_hbm, da), (h1_hbm, h1), (all_hbm, o_all)])
    ]

    def load_p(pair):
        at = pair % slots
        return pltpu.make_async_copy(p_hbm.at[pl.ds(2 * pair, 2)], p.at[at], p_s.at[at])

    load_p(0).start()
    for load in loads:
        load.start()
    lane = lax.broadcasted_iota(jnp.int32, (1, 128), 1)
    held = {}

    def begin(pair):
        if pair + 1 < pairs and slots > 1:
            load_p(pair + 1).start()
        at = slice(pair * 128, pair * 128 + 128)
        held["k"] = k[:, at].astype(F32).T.astype(BF)
        prod = (do[:, at].astype(F32) * o[:, at].astype(F32)).T
        held["d"] = [jnp.sum(prod[64 * h : 64 * h + 64, :], axis=0, keepdims=True) for h in range(2)]
        dk[...] = jnp.zeros_like(dk)
        dv[...] = jnp.zeros_like(dv)
        load_p(pair).wait()

    def block(pair, i):
        win = pl.ds(i * tile, tile)
        at = slice(pair * 128, pair * 128 + 128)
        keys = (i + 1) * tile
        for h in range(2):
            here = (lane // 64) == h
            query = jnp.where(here, q[win, at].astype(F32), 0.0).astype(BF)
            grad = jnp.where(here, do[win, at].astype(F32), 0.0).astype(BF)
            prob = p[pair % slots, h, pl.ds(0, keys), win]
            dp = dot(v[pl.ds(0, keys), at], grad, NT)
            ds = (prob.astype(F32) * (dp - held["d"][h][:, i * tile : (i + 1) * tile]) * 0.125).astype(BF)
            half = slice(64 * h, 64 * h + 64)
            dqt[half, win] = dot(held["k"][half, :keys], ds)
            dk[pl.ds(0, keys), :] += dot(ds, query)
            dv[pl.ds(0, keys), :] += dot(prob, grad)

    def end(pair):
        for t, val in enumerate((dqt[...].T, dk[...], dv[...])):
            at = slice((t * pairs + pair) * 128, (t * pairs + pair) * 128 + 128)
            low = val.astype(BF)
            sums[:, at] = jnp.sum(low.astype(F32), axis=0, keepdims=True)
            dqkv[:, at] = low

    spare = max(0, width - 128 * n)
    whole_tiles = width // hw

    def products(rows, x, y):
        out[rows, 3 * cols :] = dot(y, da[:, pl.ds(pl.multiple_of(me * 128, 128), 128)], TN).astype(BF)

        @pl.when(me < n - 1 if spare else me < n)
        def _():
            out[rows, : 3 * cols] = dot(x, dqkv[...], TN).astype(BF)

        if spare:

            @pl.when(me == n - 1)
            def _():
                out[rows, : 3 * cols] = jnp.zeros((x.shape[1], 3 * cols), BF)
                out[rows, :spare] = dot(y, da[:, 128 * n :], TN).astype(BF)

    def weights(lo, hi):
        if lo == 0:
            for load in loads:
                load.wait()

        def body(i, carry):
            at = pl.ds(pl.multiple_of(i * hw, hw), hw)
            products(at, h1[:, at], o_all[i])
            return carry

        lax.fori_loop(lo, hi, body, 0)
        if hi == whole_tiles and width % hw:
            rest = width % hw
            at = pl.ds(hi * hw, rest)
            products(at, h1[:, at], o_all[hi, :, :rest])

    part = functools.partial
    steps = []
    for pair in range(pairs):
        steps.append((1.0, part(begin, pair)))
        steps += [(0.6 + 0.5 * i, part(block, pair, i)) for i in range(length // tile)]
        steps.append((1.0, part(end, pair)))
    cut = whole_tiles // 2
    steps += [(5.5, part(weights, 0, cut)), (5.5, part(weights, cut, whole_tiles))]
    clock, work = 0.0, []
    for size, step in steps:
        work.append((clock, step))
        clock += size
    timed(work, gather.timed_steps(lambda c: 3.5 * c, 6.0, 5.0))
    gather.finish()


def back(n, cid, ready, q, k, v, o, do, da, p, h1, o_all):
    length, hw = q.shape
    width = da.shape[1]
    if 128 * n > width:
        da = jnp.pad(da, ((0, 0), (0, 128 * n - width)))
    assert width <= 128 * n or (n - 1) * hw >= width and width - 128 * n <= 3 * hw
    dma = pltpu.SemaphoreType.DMA
    slots = min(2, hw // 128)
    return call(
        functools.partial(back_kernel, n, 256, hw, width),
        cid,
        "back",
        (ready, q, k, v, o, do, da, p, h1, o_all),
        [VMEM] * 6 + [ANY] * 4,
        [
            ((n,) + ready.shape, BF),
            ((length, 3 * hw), BF),
            ((1, 3 * hw), F32),
            ((width, 3 * hw + 128), BF),
        ],
        [ANY, VMEM, VMEM, VMEM],
        [
            pltpu.VMEM(da.shape, BF),
            pltpu.VMEM((slots, 2, length, length), BF),
            pltpu.VMEM(h1.shape, BF),
            pltpu.VMEM(o_all.shape, BF),
            pltpu.VMEM((128, length), F32),
            pltpu.VMEM((length, 128), F32),
            pltpu.VMEM((length, 128), F32),
            dma((3,)),
            dma((slots,)),
        ]
        + Gather.sems(n, ready.shape[0]),
        BACK if n == 8 else 60,
    )


def norm(values):
    centre = values - jnp.mean(values, axis=-1, keepdims=True)
    rstd = lax.rsqrt(jnp.mean(centre * centre, axis=-1, keepdims=True) + 1e-05)
    return centre * rstd, rstd


def norm_back(grad, unit, rstd, gain):
    inner = grad * gain
    return rstd * (
        inner
        - jnp.mean(inner, axis=-1, keepdims=True)
        - unit * jnp.mean(inner * unit, axis=-1, keepdims=True)
    )


def make_body(n, nz):
    def body(
        tokens, block_table, ln1_gain, ln1_bias, qkv_weight, query_bias, value_bias,
        proj_weight, proj_bias, ln2_gain, ln2_bias, fc_weight, fc_bias, out_weight,
        out_bias, cotangent,
    ):
        ctx = lax.axis_index("ctx")
        z = lax.axis_index("fsdp")
        rows, width = tokens.shape
        blk = rows // 2
        wz = width // nz
        slots = -(-HEADS // n)
        hw = slots * (width // HEADS)
        unit_z = out_weight.shape[0]
        uw = unit_z // n
        units = uw * nz
        table = block_table.reshape(-1)
        inv = jnp.argmax(
            table[None, :] == jnp.arange(table.shape[0], dtype=table.dtype)[:, None], axis=1
        ).astype(jnp.int32)

        take = lambda a, at, size, axis=0: lax.dynamic_slice_in_dim(a, at, size, axis)
        parts = 5
        padded = jnp.pad(qkv_weight, ((0, 0), (0, n * hw - width)))
        wq_own = jnp.concatenate(
            [take(padded, t * width + ctx * hw, hw, 1) for t in range(3)], axis=1
        ).reshape(parts, wz // parts, 3 * hw)
        row = lax.broadcasted_iota(jnp.int32, (16, wz), 0)
        small = jnp.zeros((16, wz), BF)
        for i, v in enumerate(
            [ln1_gain, ln1_bias, query_bias, value_bias, proj_bias, ln2_gain, ln2_bias, out_bias]
            + [jnp.pad(take(fc_bias, ctx * uw, uw), (0, wz - uw))]
        ):
            small = jnp.where(row == i, v[None, :], small)
        tile = math.gcd(wz, hw)
        h1, cot, small, w_qkv, w_proj, tok_own, cot_own, wfc_own, wout_own = entry(
            n,
            nz,
            tokens,
            cotangent,
            small,
            wq_own,
            proj_weight.reshape(wz // tile, tile, width),
            fc_weight.reshape(25, wz // 25, fc_weight.shape[1]),
            out_weight.reshape(n, uw, width),
            hw,
        )
        w_fc = lax.all_gather(wfc_own.reshape(wz, units), "fsdp", axis=0, tiled=True)
        w_out = lax.all_gather(wout_own, "fsdp", axis=0, tiled=True)
        length = n * rows
        flat = lambda a: a.reshape(length, a.shape[-1])
        h1, cot = flat(h1), flat(cot)
        w_qkv, w_proj = w_qkv.reshape(width, 3 * hw), w_proj.reshape(hw, width)
        fb = small[8].reshape(nz, wz)[:, :uw].reshape(1, units)
        pad_cols = lambda v: take(jnp.pad(v, (0, n * hw - width)), ctx * hw, hw)
        qkv_bias = jnp.concatenate([pad_cols(small[2]), jnp.zeros((hw,), F32), pad_cols(small[3])])

        qkv = (dot(h1, w_qkv) + qkv_bias).astype(BF)
        o, p, q_pos, k_pos, v_pos, o_pos = attend(qkv, inv, blk)
        mid, h2 = middle(n, 2, o, w_proj, tok_own, small)
        h2 = flat(h2)
        hidden, slope = hidden_units(h2, w_fc, fb)
        part_out = dot(hidden, cot, TN).astype(BF)
        in_parts = lambda a: a.reshape(nz, parts, a.shape[0] // nz // parts, a.shape[1])
        o, part_out = lax.optimization_barrier((o, part_out))
        o_all = spread(n, 3, o.reshape(4, length // 4, hw))
        h1_pos = order(h1, inv, blk)
        w_out, o_all, h1_pos = lax.optimization_barrier((w_out, o_all, h1_pos))
        to_owner = lambda a: lax.psum_scatter(a, "fsdp", scatter_dimension=0, tiled=True)
        sum_out = to_owner(part_out)
        du, dfb = hidden_back(cot, w_out, slope)
        part_fc = outer(h2, du)
        du, part_fc = lax.optimization_barrier((du, part_fc))
        sum_fc = to_owner(part_fc)
        da, dmid, layer_out, sums = turn(n, 4, du, w_fc, hidden, w_out, mid, cot_own, small)
        da = flat(da)
        all_out, dqkv, bias_cols, part_attn = back(
            n,
            6,
            sum_out.reshape(parts, uw // parts, width),
            q_pos,
            k_pos,
            v_pos,
            o_pos,
            heads_grad(da, w_proj, inv, blk),
            da,
            p,
            h1_pos,
            o_all.reshape(n, length, hw),
        )
        dqkv = order(dqkv, table, blk)

        put = lambda v, size: lax.dynamic_update_slice_in_dim(
            jnp.zeros((1, size), F32), v, ctx * v.shape[1], 1
        )
        biases = jnp.concatenate(
            [put(bias_cols[:, :hw], n * hw), put(bias_cols[:, 2 * hw :], n * hw)]
        )[:, :width]
        wide_fb = lax.dynamic_update_slice_in_dim(
            jnp.zeros((nz, unit_z), F32), dfb.reshape(nz, uw), ctx * uw, 1
        )
        vectors = jnp.concatenate(
            [sums + jnp.pad(biases, ((2, 4), (0, 0))), jnp.pad(wide_fb, ((0, -nz % 8), (0, width - unit_z)))]
        )
        all_fc, all_attn, grad_tokens, vectors = tail(
            n,
            nz,
            5,
            sum_fc.reshape(parts, wz // parts, units),
            in_parts(part_attn),
            dqkv,
            w_qkv,
            tok_own,
            dmid,
            small,
            vectors,
        )
        whole_rows = lambda a: a.reshape(n, a.shape[1] * a.shape[2], a.shape[3])
        grad_fc, grad_qkv, grad_proj, grad_out = join(
            n, nz, hw, whole_rows(all_fc), whole_rows(all_attn), all_out.reshape(unit_z, width)
        )
        vectors, grad_tokens, layer_out, grad_fc = lax.optimization_barrier(
            (vectors, grad_tokens, layer_out, grad_fc)
        )
        mine = take(vectors[:8], z * wz, wz, 1)
        gfb = take(vectors[8 : 8 + nz], z, 1).reshape(-1)[:unit_z]
        return (
            layer_out,
            grad_tokens,
            mine[0],
            mine[1],
            grad_qkv,
            mine[2],
            mine[3],
            grad_proj,
            mine[4],
            mine[5],
            mine[6],
            grad_fc,
            gfb,
            grad_out,
            mine[7],
        )

    return body


def solution(mesh):
    both = P(("fsdp", "ctx"), None)
    vec, mat = P("fsdp"), P("fsdp", None)
    placed = (both, P(), vec, vec, mat, vec, vec, mat, vec, vec, vec, mat, vec, mat, vec, both)
    outs = (both, both, vec, vec, mat, vec, vec, mat, vec, vec, vec, mat, vec, mat, vec)
    return jax.shard_map(
        make_body(mesh.shape["ctx"], mesh.shape["fsdp"]),
        mesh=mesh,
        in_specs=placed,
        out_specs=outs,
        check_vma=False,
    )
```

```python
import functools
import math

import jax
import jax.numpy as jnp
from jax import lax
from jax.experimental import pallas as pl
from jax.experimental.pallas import tpu as pltpu
from jax.sharding import PartitionSpec as P

HEADS = 25
BF = jnp.bfloat16
F32 = jnp.float32
MESH = pl.DeviceIdType.MESH
ENTRY, ATTEND, MIDDLE, SPREAD, TURN, BACK, TAIL = 60, 60, 60, 60, 60, 60, 30
HIDDEN, HIDDEN_BACK, OUTER, ORDER, HEADS_GRAD, JOIN = 60, 60, 60, 9, 60, 8
ANY = pl.BlockSpec(memory_space=pl.ANY)
VMEM = pl.BlockSpec(memory_space=pltpu.VMEM)
HBM = pl.BlockSpec(memory_space=pltpu.HBM)
NN = (((1,), (0,)), ((), ()))
NT = (((1,), (1,)), ((), ()))
TN = (((0,), (0,)), ((), ()))


def room(length, mib):
    return pltpu.CompilerParams(vmem_limit_bytes=(mib if length <= 1024 else 60) * 1024 * 1024)


def dot(a, b, dims=NN):
    return lax.dot_general(a, b, dims, preferred_element_type=F32)


def places(n):
    me = lax.axis_index("ctx")
    core = lax.rem(me, 2)
    chip = me // 2
    sib = me + 1 - 2 * core
    if n == 8:
        across = chip + 1 - 2 * lax.rem(chip, 2)
        along = lax.rem(chip + 2, 4)
        first = across * (1 - core) + along * core
        second = along * (1 - core) + across * core
        others = [first, second, 3 - chip]
    else:
        half = n // 2
        others = [lax.rem(chip + d, half) for d in range(1, half)]
    return me, core, chip, sib, others


def twin(square, k):
    return 1 - k if square and k < 2 else k


def signal(sem, **device):
    pl.semaphore_signal(sem, inc=1, device_id=device, device_id_type=MESH)


def greet(devices, planes=()):
    barrier = pltpu.get_barrier_semaphore()
    for device in devices:
        signal(barrier, ctx=device)
    for plane in planes:
        signal(barrier, fsdp=plane)
    pl.semaphore_wait(barrier, len(devices) + len(planes))


def send(src, dst, ssem, rsem, **device):
    return pltpu.make_async_remote_copy(
        src_ref=src,
        dst_ref=dst,
        send_sem=ssem,
        recv_sem=rsem,
        device_id=device,
        device_id_type=MESH,
    )


def merge(*lists, scales=None):
    keyed = []
    for t, steps in enumerate(lists):
        scale = scales[t] if scales else 1.0
        keyed += [((i + 0.5) * scale / len(steps), t, i, step) for i, step in enumerate(steps)]
    for item in sorted(keyed, key=lambda k: k[:3]):
        item[3]()


def timed(*lists):
    keyed = [(time, t, i, step) for t, steps in enumerate(lists) for i, (time, step) in enumerate(steps)]
    for item in sorted(keyed, key=lambda k: k[:3]):
        item[3]()


def spaced(steps, start, stop):
    return [(start + (stop - start) * (i + 0.5) / len(steps), step) for i, step in enumerate(steps)]


class Gather:
    def __init__(self, n, src, out, sems):
        self.n, self.src, self.out = n, src, out
        self.own_s, self.sib_s, self.sib_r, self.far_s, self.far_r = sems
        self.parts = src.shape[0]
        self.square = n == 8
        self.me, self.core, self.chip, self.sib, self.others = places(n)
        half = n // 2
        if self.square:
            self.froms = self.others
        else:
            self.froms = [lax.rem(self.chip + half - d, half) for d in range(1, half)]
        self.peers = self.others[:2] if self.square else self.others
        self.started = []

    @staticmethod
    def sems(n, parts):
        dma = pltpu.SemaphoreType.DMA
        far = n // 2 - 1
        return [dma((parts,)), dma((far + 1, parts)), dma((far + 1, parts)), dma((far, parts)), dma((far, parts))]

    def own_sends(self, c):
        piece, slot = self.src.at[c], self.out.at[self.me, c]
        copies = [
            send(piece, slot, self.far_s.at[d, c], self.far_r.at[d, c], ctx=2 * p + self.core)
            for d, p in enumerate(self.peers)
        ]
        copies.append(send(piece, slot, self.sib_s.at[0, c], self.sib_r.at[0, c], ctx=self.sib))
        return copies + [pltpu.make_async_copy(piece, slot, self.own_s.at[c])]

    def go(self, copy):
        copy.start()
        self.started.append(copy)

    def start(self):
        for c in range(self.parts):
            self.start_part(c)

    def start_part(self, c):
        for copy in self.own_sends(c):
            copy.start()

    def arrived(self, d, c):
        piece = self.out.at[2 * self.froms[d] + self.core, c]
        send(piece, piece, self.far_s.at[d, c], self.far_r.at[d, c], ctx=self.sib).wait_recv()
        if self.square and d == 0:
            self.go(
                send(
                    piece,
                    piece,
                    self.far_s.at[2, c],
                    self.far_r.at[2, c],
                    ctx=2 * self.others[1] + self.core,
                )
            )
        e = twin(self.square, d) + 1
        self.go(send(piece, piece, self.sib_s.at[e, c], self.sib_r.at[e, c], ctx=self.sib))

    def steps(self):
        todo = []
        for c in range(self.parts):
            for d in range(2 if self.square else len(self.others)):
                todo.append(functools.partial(self.arrived, d, c))
            if self.square and c:
                todo.append(functools.partial(self.arrived, 2, c - 1))
        if self.square:
            todo.append(functools.partial(self.arrived, 2, self.parts - 1))
        return todo

    def timed_steps(self, begin, wait, relay):
        todo = []
        for c in range(self.parts):
            for d in range(len(self.others)):
                late = relay if self.square and d == 2 else 0
                todo.append((begin(c) + wait + late, functools.partial(self.arrived, d, c)))
        return todo

    def finish(self):
        for c in range(self.parts):
            *far, own = self.own_sends(c)
            own.wait()
            for copy in far:
                copy.wait_send()
        for d in range(len(self.others) + 1):
            chip = self.chip if d == 0 else self.froms[d - 1]
            for c in range(self.parts):
                piece = self.out.at[2 * chip + 1 - self.core, c]
                send(
                    piece, piece, self.sib_s.at[d, c], self.sib_r.at[d, c], ctx=self.sib
                ).wait_recv()
        for copy in self.started:
            copy.wait_send()


class Relay:
    def __init__(self, nz, z, lo, hi, count, src, out, sems, lead):
        self.nz, self.z, self.lo, self.hi, self.count = nz, z, lo, hi, count
        self.src, self.out, self.lead = src, out, lead
        self.own_s, self.up_s, self.down_s, self.recv = sems

    @staticmethod
    def sems(blocks):
        return [pltpu.SemaphoreType.DMA((blocks,)) for _ in range(4)]

    def up(self, src, b):
        return send(src, self.out.at[b], self.up_s.at[b], self.recv.at[b], fsdp=self.z + 1)

    def down(self, src, b):
        return send(src, self.out.at[b], self.down_s.at[b], self.recv.at[b], fsdp=self.z - 1)

    def own(self, b):
        return pltpu.make_async_copy(self.src.at[b - self.lead], self.out.at[b], self.own_s.at[b])

    def start(self):
        lo, hi = self.lo, self.hi

        def body(i, carry):
            u, d = hi - 1 - i, lo + i

            @pl.when(self.z < self.nz - 1)
            def _():
                self.up(self.src.at[u - self.lead], u).start()

            @pl.when(self.z > 0)
            def _():
                self.down(self.src.at[d - self.lead], d).start()

            self.own(d).start()
            return carry

        lax.fori_loop(0, hi - lo, body, 0)

    def step(self, i):
        b = self.lo - 1 - i

        @pl.when(b >= 0)
        def _():
            self.up(self.out.at[b], b).wait_recv()

            @pl.when(self.z < self.nz - 1)
            def _():
                self.up(self.out.at[b], b).start()

        e = self.hi + i

        @pl.when(e < self.count)
        def _():
            self.down(self.out.at[e], e).wait_recv()

            @pl.when(self.z > 0)
            def _():
                self.down(self.out.at[e], e).start()

    def steps(self, most):
        return [functools.partial(self.step, i) for i in range(most)]

    def finish(self):
        def sent(b, carry):
            @pl.when((self.z < self.nz - 1) & (b < self.hi))
            def _():
                self.up(self.out.at[b], b).wait_send()

            @pl.when((self.z > 0) & (b >= self.lo))
            def _():
                self.down(self.out.at[b], b).wait_send()

            @pl.when((b >= self.lo) & (b < self.hi))
            def _():
                self.own(b).wait()

            return carry

        lax.fori_loop(0, self.count, sent, 0)


def others_of(z, nz):
    return [lax.rem(z + d, nz) for d in range(1, nz)]


def entry_kernel(
    n, nz, tok_t, cot_t, small, wq, wp, fc_hbm, out_hbm, h1_all, cot_all, vec, wq_all, wp_all, tok, cot_own,
    fc_own, out_own, *scratch
):
    cot, h1, inbox, zeros, fc_all, load_s, small_s, small_r, zero_s = scratch[:9]
    g_h, g_c = scratch[9:14], scratch[14:19]
    r_q, r_p = scratch[19:23], scratch[23:27]
    loads = [
        pltpu.make_async_copy(fc_hbm, fc_all, load_s.at[0]),
        pltpu.make_async_copy(out_hbm.at[lax.axis_index("ctx")], out_own, load_s.at[1]),
    ]
    me, core, chip, sib, others = places(n)
    z = lax.axis_index("fsdp")
    planes = others_of(z, nz)
    greet([sib] + [2 * p + core for p in (others[:2] if n == 8 else others)], planes)
    wz = small.shape[1]
    for d, plane in enumerate(planes):
        send(small, inbox.at[z], small_s.at[d], small_r.at[d], fsdp=plane).start()
    inbox[z] = small[...]
    k = wq.shape[0]
    relay_q = Relay(nz, z, z * k, (z + 1) * k, nz * k, wq, wq_all, r_q, z * k)
    relay_q.start()
    parts, rows = h1.shape[0], h1.shape[1]
    turned = cot_t[...].astype(F32).T.astype(BF)
    cot_own[...] = turned
    for c in range(parts):
        cot[c] = turned[c * rows : (c + 1) * rows, :]
    gather_c = Gather(n, cot, cot_all, g_c)
    gather_c.start()
    tok[...] = tok_t[...].astype(F32).T.astype(BF)
    share, blocks = wp.shape[0], wp_all.shape[0]
    base = me * blocks
    valid = jnp.clip(nz * share - base, 0, blocks)
    lo = jnp.clip(z * share - base, 0, valid)
    hi = jnp.clip((z + 1) * share - base, 0, valid)
    relay_p = Relay(nz, z, lo, hi, valid, wp, wp_all, r_p, z * share - base)
    relay_p.start()
    zeros[...] = jnp.zeros_like(zeros)

    def clear(b, carry):
        pltpu.make_async_copy(zeros, wp_all.at[b], zero_s.at[b]).start()
        return carry

    lax.fori_loop(valid, blocks, clear, 0)
    for d in range(nz - 1):
        came = lax.rem(z + nz - 1 - d, nz)
        send(small, inbox.at[came], small_s.at[d], small_r.at[d], fsdp=planes[d]).wait_recv()
    for p in range(nz):
        vec[:, p * wz : (p + 1) * wz] = inbox[p].astype(F32)
    gain, shift = vec[0:1, :], vec[1:2, :]
    gather_h = Gather(n, h1, h1_all, g_h)
    for c in range(parts):
        unit, _ = norm(tok[c * rows : (c + 1) * rows, :].astype(F32))
        h1[c] = (unit * gain + shift).astype(BF)
        gather_h.start_part(c)
    for load in loads:
        load.start()

    def columns():
        for load in loads:
            load.wait()
        uw = fc_own.shape[-1] // nz
        for place in range(n):

            @pl.when(me == place)
            def _():
                def tile(i, carry):
                    for t in range(nz):
                        at = (t * n + place) * uw
                        fc_own[i, :, t * uw : (t + 1) * uw] = fc_all[i, :, at : at + uw]
                    return carry

                lax.fori_loop(0, fc_own.shape[0], tile, 0)

    steps = gather_c.steps() + gather_h.steps()
    merge(
        steps[:4] + [columns] + steps[4:],
        relay_q.steps(nz * k - k) + relay_p.steps(blocks),
    )
    gather_c.finish()
    gather_h.finish()
    relay_q.finish()
    relay_p.finish()

    def cleared(b, carry):
        pltpu.make_async_copy(zeros, wp_all.at[b], zero_s.at[b]).wait()
        return carry

    lax.fori_loop(valid, blocks, cleared, 0)
    for d, plane in enumerate(planes):
        send(small, inbox.at[z], small_s.at[d], small_r.at[d], fsdp=plane).wait_send()


def entry(n, nz, tokens, cot, small, wq, wp, fc, out, hw):
    rows, width = tokens.shape
    parts = 2 if n == 8 else 1
    dma = pltpu.SemaphoreType.DMA
    k, tile = wq.shape[0], wp.shape[1]
    blocks = hw // tile
    shape = jax.ShapeDtypeStruct
    piece = (parts, rows // parts, width)
    return pl.pallas_call(
        functools.partial(entry_kernel, n, nz),
        out_shape=[
            shape((n,) + piece, BF),
            shape((n,) + piece, BF),
            shape((small.shape[0], width), F32),
            shape((nz * k,) + wq.shape[1:], BF),
            shape((blocks, tile, width), BF),
            shape((rows, width), BF),
            shape((rows, width), BF),
            shape(fc.shape[:2] + (fc.shape[2] // n,), BF),
            shape(out.shape[1:], BF),
        ],
        in_specs=[VMEM] * 5 + [HBM, HBM],
        out_specs=[ANY, ANY, VMEM, ANY, ANY] + [VMEM] * 4,
        scratch_shapes=[
            pltpu.VMEM(piece, BF),
            pltpu.VMEM(piece, BF),
            pltpu.VMEM((nz,) + small.shape, BF),
            pltpu.VMEM((tile, width), BF),
            pltpu.VMEM(fc.shape, BF),
            dma((2,)),
            dma((nz - 1,)),
            dma((nz - 1,)),
            dma((blocks,)),
        ]
        + Gather.sems(n, parts)
        + Gather.sems(n, parts)
        + Relay.sems(nz * k)
        + Relay.sems(blocks),
        compiler_params=pltpu.CompilerParams(
            collective_id=1, has_side_effects=True, vmem_limit_bytes=(ENTRY if n == 8 else 60) * 1024 * 1024
        ),
        name="entry",
    )(tokens.T, cot.T, small, wq, wp, fc, out)


class Scatter:
    def __init__(self, n, dims, a, w, scratch):
        self.n, self.dims, self.a, self.w = n, dims, a, w
        self.part, self.theirs, self.sums, self.inbox = scratch[:4]
        self.sib_s, self.sib_r, self.far_s, self.far_r = scratch[4:]
        self.me, self.core, self.chip, self.sib, self.others = places(n)
        self.square = n == 8
        self.half = n // 2
        self.parts = self.sib_s.shape[1]
        self.full = self.part.shape[2]
        self.rows = self.full // self.parts
        if self.square:
            first, second = [2 * p + self.core for p in self.others[:2]]
            self.ends = [(0, 0, first), (1, 1, first), (2, 2, second)]
        else:
            self.ends = [(k, k, 2 * self.others[k] + self.core) for k in range(self.half - 1)]

    @staticmethod
    def scratch(n, rows, width):
        dma = pltpu.SemaphoreType.DMA
        half, parts = n // 2, 4 if n == 8 else 1
        return [
            pltpu.VMEM((half, 2, rows, width), BF),
            pltpu.VMEM((half, rows, width), BF),
            pltpu.VMEM((half - 1, rows, width), BF),
            pltpu.VMEM((half - 1, rows, width), BF),
            dma((half, parts)),
            dma((half, parts)),
            dma((half - 1, parts)),
            dma((half - 1, parts)),
        ]

    def chip_at(self, k):
        if not self.square:
            return lax.rem(self.chip + 1 + k, self.half)
        x, y = lax.rem(self.chip, 2), self.chip // 2
        first, second = 1 - lax.rem(k, 3) // 2, 1 - lax.rem(k, 2)
        dx = first * (1 - self.core) + second * self.core
        dy = second * (1 - self.core) + first * self.core
        far = (k < 3).astype(jnp.int32)
        dx, dy = dx * far, dy * far
        return (y + dy - 2 * y * dy) * 2 + x + dx - 2 * x * dx

    def twin_at(self, k):
        if not self.square:
            return k
        return k + jnp.where(k == 1, 1, 0) - jnp.where(k == 2, 1, 0)

    def win(self, c):
        return pl.ds(c * self.rows, self.rows)

    def to_sib(self, k, c):
        e = self.twin_at(k)
        return send(
            self.part.at[k, 1 - self.core, self.win(c)],
            self.theirs.at[e, self.win(c)],
            self.sib_s.at[e, c],
            self.sib_r.at[e, c],
            ctx=self.sib,
        )

    def chip_sum(self, k, c):
        win = self.win(c)
        piece = self.theirs.at[k, win]
        send(piece, piece, self.sib_s.at[k, c], self.sib_r.at[k, c], ctx=self.sib).wait_recv()
        return self.part[k, self.core, win, :].astype(F32) + self.theirs[k, win, :].astype(F32)

    def pass_on(self, k, slot, peer, c):
        return send(
            self.sums.at[k, self.win(c)],
            self.inbox.at[slot, self.win(c)],
            self.far_s.at[slot, c],
            self.far_r.at[slot, c],
            ctx=peer,
        )

    def wait_in(self, slot, c):
        piece = self.inbox.at[slot, self.win(c)]
        send(piece, piece, self.far_s.at[slot, c], self.far_r.at[slot, c], ctx=self.sib).wait_recv()
        return self.inbox[slot, self.win(c), :].astype(F32)

    def forward(self, end, c):
        k, slot, peer = self.ends[end]
        total = self.chip_sum(k, c)
        if self.square and end == 2:
            total = total + self.wait_in(0, c)
        self.sums[k, self.win(c), :] = total.astype(BF)
        self.pass_on(k, slot, peer, c).start()

    def products(self):
        def product(k, carry):
            full = self.full
            at = pl.ds(pl.multiple_of(self.chip_at(k) * 2 * full, 2 * full), 2 * full)
            val = dot(self.a[at, :], self.w[...], self.dims).astype(BF)
            self.part[k, 0] = val[:full]
            self.part[k, 1] = val[full:]
            for c in range(self.parts):
                self.to_sib(k, c).start()

            @pl.when(k == 1)
            def _():
                for c in range(self.parts):
                    self.forward(0, c)

            return carry

        lax.fori_loop(0, self.half, product, 0)

    def forwards(self):
        each = range(self.parts)
        return [functools.partial(self.forward, e, c) for e in range(1, self.half - 1) for c in each]

    def total(self, c):
        val = self.chip_sum(self.half - 1, c)
        for slot in (1, 2) if self.square else range(self.half - 1):
            val = val + self.wait_in(slot, c)
        return val

    def finish(self):
        for c in range(self.parts):
            for k, slot, peer in self.ends:
                self.pass_on(k, slot, peer, c).wait_send()

        def sent(k, carry):
            for c in range(self.parts):
                self.to_sib(k, c).wait_send()
            return carry

        lax.fori_loop(0, self.half, sent, 0)


class Line:
    def __init__(self, nz, z, src, out, scratch):
        self.nz, self.z, self.src, self.out = nz, z, src, out
        self.mine, self.above, self.below, self.load_s, self.up_s, self.down_s, self.recv = scratch
        self.parts = src.shape[1]

    @staticmethod
    def scratch(shape):
        dma, lead = pltpu.SemaphoreType.DMA, shape[:2]
        return [pltpu.VMEM(shape, BF)] * 3 + [dma((1,)), dma(lead), dma(lead), dma((2,) + lead)]

    def up(self, src, d, c):
        return send(
            src.at[d, c], self.above.at[d, c], self.up_s.at[d, c], self.recv.at[0, d, c], fsdp=self.z + 1
        )

    def down(self, src, d, c):
        return send(
            src.at[d, c], self.below.at[d, c], self.down_s.at[d, c], self.recv.at[1, d, c], fsdp=self.z - 1
        )

    def start(self):
        top = self.nz - 1

        @pl.when(self.z == 0)
        def _():
            for c in range(self.parts):
                for k in range(top):
                    self.up(self.src, top - k, c).start()

        @pl.when(self.z == top)
        def _():
            for c in range(self.parts):
                for k in range(top):
                    self.down(self.src, k, c).start()

        self.load = pltpu.make_async_copy(self.src, self.mine, self.load_s.at[0])
        self.load.start()

    def loaded(self):
        self.load.wait()

    def pass_up(self, d, c):
        copy = self.up(self.mine, d, c)
        copy.wait_recv()
        self.mine[d, c] = self.mine[d, c] + self.above[d, c]
        copy.start()

    def pass_down(self, d, c):
        copy = self.down(self.mine, d, c)
        copy.wait_recv()
        self.mine[d, c] = self.mine[d, c] + self.below[d, c]
        copy.start()

    def settle(self, place, c):
        z, top = place, self.nz - 1
        total = self.mine[z, c].astype(F32)
        if z > 0:
            self.up(self.mine, z, c).wait_recv()
            total = total + self.above[z, c].astype(F32)
        if z < top:
            self.down(self.mine, z, c).wait_recv()
            total = total + self.below[z, c].astype(F32)
        self.out[c] = total.astype(BF)

    def timed_steps(self, after):
        top = self.nz - 1
        slots = {}

        def put(time, place, fn):
            slots.setdefault(time, {}).setdefault(place, []).append(fn)

        for c in range(self.parts):
            for place in range(self.nz):
                for k in range(top):
                    at = c * top + k
                    if 0 < place < top - k:
                        put(at + place, place, functools.partial(self.pass_up, top - k, c))
                    if k < place < top:
                        put(at + top - place, place, functools.partial(self.pass_down, k, c))
                put((c + 1) * top, place, functools.partial(self.settle, place, c))
                put((c + 1) * top, place, functools.partial(after, c))

        def run(work):
            for place, fns in sorted(work.items()):

                @pl.when(self.z == place)
                def _():
                    for fn in fns:
                        fn()

        return [(0, self.loaded)] + [(t, functools.partial(run, slots[t])) for t in sorted(slots)]

    def finish(self):
        for d in range(self.nz):

            @pl.when(self.z < d)
            def _():
                for c in range(self.parts):
                    self.up(self.mine, d, c).wait_send()

            @pl.when(self.z > d)
            def _():
                for c in range(self.parts):
                    self.down(self.mine, d, c).wait_send()


class Vectors:
    def __init__(self, n, nz, src, out, scratch):
        self.n, self.nz, self.src, self.out = n, nz, src, out
        self.low, self.from_sib, self.chips, self.line = scratch[:4]
        self.ss, self.sr, self.cs, self.cr, self.ls, self.lr = scratch[4:]
        self.me, self.core, self.chip, self.sib, self.others = places(n)
        self.z = lax.axis_index("fsdp")
        self.planes = others_of(self.z, nz)

    @staticmethod
    def scratch(n, nz, shape):
        dma = pltpu.SemaphoreType.DMA
        half = n // 2
        return [
            pltpu.VMEM(shape, BF),
            pltpu.VMEM(shape, BF),
            pltpu.VMEM((half,) + shape, BF),
            pltpu.VMEM((nz,) + shape, BF),
            dma((1,)),
            dma((1,)),
            dma((half - 1,)),
            dma((half - 1,)),
            dma((nz - 1,)),
            dma((nz - 1,)),
        ]

    def to_sib(self):
        return send(self.low, self.from_sib, self.ss.at[0], self.sr.at[0], ctx=self.sib)

    def to_chip(self, d):
        at = self.chips.at[self.chip]
        return send(at, at, self.cs.at[d], self.cr.at[d], ctx=2 * self.others[d] + self.core)

    def to_plane(self, d):
        at = self.line.at[self.z]
        return send(at, at, self.ls.at[d], self.lr.at[d], fsdp=self.planes[d])

    def start(self):
        self.low[...] = self.src[...].astype(BF)
        self.to_sib().start()

    def first(self):
        self.to_sib().wait_recv()
        self.chips[self.chip] = self.low[...] + self.from_sib[...]
        for d in range(self.n // 2 - 1):
            self.to_chip(d).start()

    def second(self):
        for d in range(self.n // 2 - 1):
            self.to_chip(d).wait_recv()
        total = self.chips[0].astype(F32)
        for k in range(1, self.n // 2):
            total = total + self.chips[k].astype(F32)
        self.line[self.z] = total.astype(BF)
        for d in range(self.nz - 1):
            self.to_plane(d).start()

    def third(self):
        for d in range(self.nz - 1):
            self.to_plane(d).wait_recv()
        total = self.line[0].astype(F32)
        for k in range(1, self.nz):
            total = total + self.line[k].astype(F32)
        self.out[...] = total

    def steps(self):
        return [self.first, self.second, self.third]

    def finish(self):
        self.to_sib().wait_send()
        for d in range(self.n // 2 - 1):
            self.to_chip(d).wait_send()
        for d in range(self.nz - 1):
            self.to_plane(d).wait_send()


def beside(n):
    me, core, chip, sib, others = places(n)
    return [sib] + [2 * p + core for p in (others[:2] if n == 8 else others)]


def call(kernel, cid, name, ins, in_specs, outs, out_specs, scratch, mib=60):
    return pl.pallas_call(
        kernel,
        out_shape=[jax.ShapeDtypeStruct(*o) for o in outs],
        in_specs=in_specs,
        out_specs=out_specs,
        scratch_shapes=scratch,
        compiler_params=pltpu.CompilerParams(
            collective_id=cid, has_side_effects=True, vmem_limit_bytes=mib * 1024 * 1024
        ),
        name=name,
    )(*ins)


def middle_kernel(n, o, w, tok, vec, mid, h2_all, h2, *scratch):
    greet(beside(n))
    scatter = Scatter(n, NN, o, w, scratch[:8])
    gather = Gather(n, h2, h2_all, scratch[8:])
    scatter.products()
    for step in scatter.forwards():
        step()
    for c in range(gather.parts):
        win = scatter.win(c)
        val = tok[win, :].astype(F32) + scatter.total(c) + vec[4:5, :]
        mid[win, :] = val
        h2[c] = (norm(val)[0] * vec[5:6, :] + vec[6:7, :]).astype(BF)
        gather.start_part(c)
    for step in gather.steps():
        step()
    gather.finish()
    scatter.finish()


def middle(n, cid, o, w, tok, vec):
    rows, width = tok.shape
    parts = 4 if n == 8 else 1
    piece = (parts, rows // parts, width)
    return call(
        functools.partial(middle_kernel, n),
        cid,
        "middle",
        (o, w, tok, vec),
        [VMEM] * 4,
        [((rows, width), F32), ((n,) + piece, BF)],
        [VMEM, ANY],
        [pltpu.VMEM(piece, BF)] + Scatter.scratch(n, rows, width) + Gather.sems(n, parts),
        MIDDLE if n == 8 else 60,
    )


def spread_kernel(n, src, all_ref, *sems):
    greet(beside(n))
    gather = Gather(n, src, all_ref, sems)
    gather.start()
    for step in gather.steps():
        step()
    gather.finish()


def spread(n, cid, array):
    return call(
        functools.partial(spread_kernel, n),
        cid,
        "spread",
        (array,),
        [VMEM],
        [((n,) + array.shape, BF)],
        [ANY],
        Gather.sems(n, array.shape[0]),
        SPREAD if n == 8 else 60,
    )[0]


def turn_kernel(
    n, du, w_fc, hid_in, w_out_in, mid_in, cot_in, vec, da_all, dmid, layer, sums,
    da, hid, w_out, mid, cot, load_s, *scratch,
):
    loads = [
        pltpu.make_async_copy(src, dst, load_s.at[i])
        for i, (src, dst) in enumerate([(hid_in, hid), (w_out_in, w_out), (mid_in, mid), (cot_in, cot)])
    ]
    for load in loads:
        load.start()
    greet(beside(n))
    back = Scatter(n, NT, du, w_fc, scratch[:8])
    ahead = Scatter(n, NN, hid, w_out, scratch[8:16])
    gather = Gather(n, da, da_all, scratch[16:])
    back.products()
    todo = back.forwards()
    for step in todo[: back.parts]:
        step()
    for load in loads:
        load.wait()
    ahead.products()
    for step in todo[back.parts :]:
        step()
    sums[...] = jnp.zeros_like(sums)
    for c in range(gather.parts):
        win = back.win(c)
        grad = back.total(c)
        unit, rstd = norm(mid[win, :])
        up = cot[win, :].astype(F32)
        val = up + norm_back(grad, unit, rstd, vec[5:6, :])
        dmid[win, :] = val
        low = val.astype(BF)
        da[c] = low
        gather.start_part(c)
        for row, term in ((4, low.astype(F32)), (5, grad * unit), (6, grad), (7, up)):
            sums[row : row + 1, :] += jnp.sum(term, axis=0, keepdims=True)
    merge(gather.steps(), ahead.forwards())
    for c in range(gather.parts):
        win = ahead.win(c)
        layer[win, :] = (mid[win, :] + ahead.total(c) + vec[7:8, :]).astype(BF)
    gather.finish()
    back.finish()
    ahead.finish()


def turn(n, cid, du, w_fc, hidden, w_out, mid, cot, vec):
    rows, width = mid.shape
    parts = 4 if n == 8 else 1
    piece = (parts, rows // parts, width)
    return call(
        functools.partial(turn_kernel, n),
        cid,
        "turn",
        (du, w_fc, hidden, w_out, mid, cot, vec),
        [VMEM] * 2 + [ANY] * 4 + [VMEM],
        [((n,) + piece, BF), ((rows, width), F32), ((rows, width), BF), ((8, width), F32)],
        [ANY, VMEM, VMEM, VMEM],
        [pltpu.VMEM(piece, BF)]
        + [pltpu.VMEM(a.shape, a.dtype) for a in (hidden, w_out, mid, cot)]
        + [pltpu.SemaphoreType.DMA((4,))]
        + Scatter.scratch(n, rows, width)
        + Scatter.scratch(n, rows, width)
        + Gather.sems(n, parts),
        TURN if n == 8 else 60,
    )


def tail_kernel(
    n, nz, fc, part, dqkv, w_qkv, tok, dmid, vec, v_in, fc_all, attn_all, g_tok, v_out,
    v_own, attn, fc_v, dqkv_v, w_v, load_s, *scratch,
):
    z = lax.axis_index("fsdp")
    me, core, chip, sib, others = places(n)
    greet([sib] + [2 * p + core for p in others], others_of(z, nz))
    line = Line(nz, z, part, attn, scratch[:7])
    line.start()
    loads = [
        pltpu.make_async_copy(src, dst, load_s.at[i])
        for i, (src, dst) in enumerate([(dqkv, dqkv_v), (w_qkv, w_v), (fc, fc_v)])
    ]
    for load in loads:
        load.start()
    fc, dqkv, w_qkv = fc_v, dqkv_v, w_v
    scatter = Scatter(n, NT, dqkv, w_qkv, scratch[7:15])
    vectors = Vectors(n, nz, v_own, v_out, scratch[15:25])
    fc_g = Gather(n, fc, fc_all, scratch[25:30])
    attn_g = Gather(n, attn, attn_all, scratch[30:35])
    v_own[...] = v_in[...]
    for load in loads[:2]:
        load.wait()
    scatter.products()
    todo = scatter.forwards()
    for step in todo[: scatter.parts]:
        step()
    loads[2].wait()

    def rest(c):
        win = scatter.win(c)
        grad = scatter.total(c)
        unit, rstd = norm(tok[win, :].astype(F32))
        g_tok[win, :] = (dmid[win, :] + norm_back(grad, unit, rstd, vec[0:1, :])).astype(BF)
        v_own[0:1, :] += jnp.sum(grad * unit, axis=0, keepdims=True)
        v_own[1:2, :] += jnp.sum(grad, axis=0, keepdims=True)

    top = nz - 1
    last = attn_g.parts * top
    part_at = functools.partial
    fc_at = lambda c: 4.0 + 2.0 * c
    timed(
        spaced(todo[scatter.parts :], 1.0, 4.0),
        spaced([part_at(rest, c) for c in range(scatter.parts)], 4.5, 7.0),
        [(7.1, vectors.start), (7.8, vectors.first), (11.0, vectors.second), (last + 3.0, vectors.third)],
        [(fc_at(c), part_at(fc_g.start_part, c)) for c in range(fc_g.parts)],
        fc_g.timed_steps(fc_at, 2.2, 1.6),
        line.timed_steps(attn_g.start_part),
        attn_g.timed_steps(lambda c: (c + 1) * top, 2.2, 1.6),
    )
    for job in (fc_g, attn_g, scatter, line, vectors):
        job.finish()


def tail(n, nz, cid, fc, part, dqkv, w_qkv, tok, dmid, vec, v_in):
    rows, width = tok.shape
    attn = part.shape[1:]
    return call(
        functools.partial(tail_kernel, n, nz),
        cid,
        "tail",
        (fc, part, dqkv, w_qkv, tok, dmid, vec, v_in),
        [HBM] * 4 + [VMEM] * 4,
        [((n,) + fc.shape, BF), ((n,) + attn, BF), (tok.shape, BF), (v_in.shape, F32)],
        [ANY, ANY, VMEM, VMEM],
        [pltpu.VMEM(v_in.shape, F32), pltpu.VMEM(attn, BF)]
        + [pltpu.VMEM(a.shape, BF) for a in (fc, dqkv, w_qkv)]
        + [pltpu.SemaphoreType.DMA((3,))]
        + Line.scratch(part.shape)
        + Scatter.scratch(n, rows, width)
        + Vectors.scratch(n, nz, v_in.shape)
        + Gather.sems(n, fc.shape[0])
        + Gather.sems(n, attn[0]),
        TAIL if n == 8 else 60,
    )


def outer_kernel(x_ref, y_ref, out_ref):
    out_ref[...] = dot(x_ref[...], y_ref[...], TN).astype(BF)


def outer(x, y):
    rows, m = x.shape
    tile = 256
    return pl.pallas_call(
        outer_kernel,
        grid=(pl.cdiv(m, tile),),
        out_shape=jax.ShapeDtypeStruct((m, y.shape[1]), BF),
        in_specs=[pl.BlockSpec((rows, tile), lambda i: (0, i)), fixed(*y.shape)],
        out_specs=tiled(tile, y.shape[1]),
        compiler_params=room(rows, OUTER),
        name="outer",
    )(x, y)


def hidden_kernel(h_ref, w_ref, b_ref, z_ref, s_ref):
    u = dot(h_ref[...], w_ref[...]) + b_ref[...]
    root = 0.7978845608028654
    square = u * u
    inner = jnp.tanh(root * u * (1.0 + 0.044715 * square))
    z_ref[...] = (0.5 * u * (1.0 + inner)).astype(BF)
    slope = 0.5 * (1.0 + inner) + 0.5 * u * (1.0 - inner * inner) * root * (1.0 + 3 * 0.044715 * square)
    s_ref[...] = slope.astype(BF)


def hidden_back_kernel(c_ref, w_ref, s_ref, d_ref, sum_ref):
    du = (dot(c_ref[...], w_ref[...], NT) * s_ref[...].astype(F32)).astype(BF)
    d_ref[...] = du

    @pl.when(pl.program_id(0) == 0)
    def _():
        sum_ref[...] = jnp.zeros_like(sum_ref)

    sum_ref[...] += jnp.sum(du.astype(F32), axis=0, keepdims=True)


def tiled(rows, cols):
    return pl.BlockSpec((rows, cols), lambda i: (i, 0))


def fixed(rows, cols):
    return pl.BlockSpec((rows, cols), lambda i: (0, 0))


def hidden_units(h2, w_fc, bias):
    rows, width = h2.shape
    units = w_fc.shape[1]
    tile = 256
    shape = jax.ShapeDtypeStruct((rows, units), BF)
    return pl.pallas_call(
        hidden_kernel,
        grid=(rows // tile,),
        out_shape=[shape, shape],
        in_specs=[tiled(tile, width), fixed(width, units), fixed(1, units)],
        out_specs=[tiled(tile, units), tiled(tile, units)],
        compiler_params=room(rows, HIDDEN),
        name="hidden",
    )(h2, w_fc, bias)


def hidden_back(cot, w_out, slope):
    rows, width = cot.shape
    units = w_out.shape[0]
    tile = 256
    return pl.pallas_call(
        hidden_back_kernel,
        grid=(rows // tile,),
        out_shape=[
            jax.ShapeDtypeStruct((rows, units), BF),
            jax.ShapeDtypeStruct((1, units), F32),
        ],
        in_specs=[tiled(tile, width), fixed(units, width), tiled(tile, units)],
        out_specs=[tiled(tile, units), fixed(1, units)],
        compiler_params=room(rows, HIDDEN_BACK),
        name="hidden_back",
    )(cot, w_out, slope)


def join_kernel(n, nz, hw, width, fc, qp, out, fc_o, qkv_o, proj_o, out_o):
    uw = fc.shape[-1] // nz
    for c in range(n):
        for b in range(nz):
            at = b * n * uw + c * uw
            fc_o[:, at : at + uw] = fc[c, 0, :, b * uw : (b + 1) * uw].astype(F32)
        size = min(128, width - c * 128)
        if size > 0:
            proj_o[:, c * 128 : c * 128 + size] = qp[c, 0, :, 3 * hw : 3 * hw + size].astype(F32)
        size = min(hw, width - c * hw)
        if size > 0:
            for t in range(3):
                at = t * width + c * hw
                qkv_o[:, at : at + size] = qp[c, 0, :, t * hw : t * hw + size].astype(F32)
    if 128 * n < width:
        proj_o[:, 128 * n :] = qp[n - 1, 0, :, : width - 128 * n].astype(F32)
    out_o[...] = out[...].astype(F32)


def join(n, nz, hw, fc, qp, out):
    tiles = 25
    width = out.shape[1]
    wz = fc.shape[1]
    split = lambda a: a.reshape(n, tiles, wz // tiles, a.shape[-1])
    fc, qp = split(fc), split(qp)
    wide = lambda a: pl.BlockSpec((n, 1, wz // tiles, a.shape[-1]), lambda i: (0, i, 0, 0))
    t, ot = wz // tiles, out.shape[0] // tiles
    cols = (n * fc.shape[-1], 3 * width, width)
    shape = jax.ShapeDtypeStruct
    return pl.pallas_call(
        functools.partial(join_kernel, n, nz, hw, width),
        grid=(tiles,),
        out_shape=[shape((wz, c), F32) for c in cols] + [shape(out.shape, F32)],
        in_specs=[wide(fc), wide(qp), tiled(ot, width)],
        out_specs=[tiled(t, c) for c in cols] + [tiled(ot, width)],
        compiler_params=room(1024, JOIN),
        name="join",
    )(fc, qp, out)


def attend_kernel(blocks, blk, tile, inv_ref, q_ref, k_ref, v_ref, o_ref, p_ref, qn, kn, vn, on, ot):
    length = blocks * blk
    for i in range(blocks):
        src, dst = pl.ds(pl.multiple_of(inv_ref[i] * blk, blk), blk), pl.ds(i * blk, blk)
        qn[dst, :] = q_ref[src, :]
        kn[dst, :] = k_ref[src, :]
        vn[dst, :] = v_ref[src, :]
    v_turned = vn[...].astype(F32).T.astype(BF)
    lane = lax.broadcasted_iota(jnp.int32, (1, 128), 1)
    above = lax.broadcasted_iota(jnp.int32, (tile, tile), 0) > lax.broadcasted_iota(
        jnp.int32, (tile, tile), 1
    )
    for i in range(length // tile):
        cols = pl.ds(i * tile, tile)
        keys = (i + 1) * tile
        for h in range(2):
            here = (lane // 64) == h
            q = jnp.where(here, qn[cols, :].astype(F32) * 0.125, 0.0).astype(BF)
            last = jnp.where(above, -1e30, dot(kn[pl.ds(i * tile, tile), :], q, NT))
            top = jnp.max(last, axis=0, keepdims=True)
            if i:
                early = dot(kn[pl.ds(0, i * tile), :], q, NT)
                top = jnp.maximum(top, jnp.max(early, axis=0, keepdims=True))
            last = jnp.exp(last - top)
            total = jnp.sum(last, axis=0, keepdims=True)
            if i:
                early = jnp.exp(early - top)
                total = total + jnp.sum(early, axis=0, keepdims=True)
            scale = 1.0 / total
            last = (last * scale).astype(BF)
            p_ref[h, pl.ds(i * tile, tile), cols] = last
            half = slice(64 * h, 64 * h + 64)
            o = dot(v_turned[half, i * tile : keys], last)
            if i:
                early = (early * scale).astype(BF)
                p_ref[h, pl.ds(0, i * tile), cols] = early
                o = o + dot(v_turned[half, : i * tile], early)
            ot[half, cols] = o
    on[...] = ot[...].T.astype(BF)
    for i in range(blocks):
        o_ref[pl.ds(pl.multiple_of(inv_ref[i] * blk, blk), blk), :] = on[i * blk : (i + 1) * blk, :]


def attend(qkv, inv, blk):
    length = qkv.shape[0]
    cols = qkv.shape[1] // 3
    pairs = cols // 128
    blocks = inv.shape[0]
    tile = 256
    piece = lambda off: pl.BlockSpec((length, 128), lambda p, s: (0, off * pairs + p))
    return pl.pallas_call(
        functools.partial(attend_kernel, blocks, blk, tile),
        out_shape=[
            jax.ShapeDtypeStruct((length, cols), BF),
            jax.ShapeDtypeStruct((2 * pairs, length, length), BF),
        ]
        + [jax.ShapeDtypeStruct((length, cols), BF)] * 4,
        grid_spec=pltpu.PrefetchScalarGridSpec(
            num_scalar_prefetch=1,
            grid=(pairs,),
            in_specs=[piece(0), piece(1), piece(2)],
            out_specs=[
                pl.BlockSpec((length, 128), lambda p, s: (0, p)),
                pl.BlockSpec((2, length, length), lambda p, s: (p, 0, 0)),
            ]
            + [pl.BlockSpec((length, 128), lambda p, s: (0, p))] * 4,
            scratch_shapes=[pltpu.VMEM((128, length), F32)],
        ),
        compiler_params=room(length, ATTEND),
        name="attend",
    )(inv, qkv, qkv, qkv)


def order_kernel(blocks, blk, table, x, out):
    for i in range(blocks):
        src = pl.ds(pl.multiple_of(table[i] * blk, blk), blk)
        out[i * blk : (i + 1) * blk, :] = x[src, :]


def order(x, table, blk):
    return pl.pallas_call(
        functools.partial(order_kernel, table.shape[0], blk),
        out_shape=jax.ShapeDtypeStruct(x.shape, x.dtype),
        in_specs=[pl.BlockSpec(memory_space=pltpu.SMEM), VMEM],
        out_specs=VMEM,
        compiler_params=room(x.shape[0], ORDER),
        name="order",
    )(table, x)


def heads_kernel(blocks, blk, tile, table, da, w, out, rows):
    step = pl.program_id(0)
    rows[pl.ds(pl.multiple_of(step * tile, tile), tile), :] = dot(da[...], w[...], NT).astype(BF)

    @pl.when(step == pl.num_programs(0) - 1)
    def _():
        for i in range(blocks):
            src = pl.ds(pl.multiple_of(table[i] * blk, blk), blk)
            out[i * blk : (i + 1) * blk, :] = rows[src, :]


def heads_grad(da, w_proj, table, blk):
    length, width = da.shape
    cols = w_proj.shape[0]
    tile = 256
    return pl.pallas_call(
        functools.partial(heads_kernel, table.shape[0], blk, tile),
        out_shape=jax.ShapeDtypeStruct((length, cols), BF),
        grid_spec=pltpu.PrefetchScalarGridSpec(
            num_scalar_prefetch=1,
            grid=(length // tile,),
            in_specs=[
                pl.BlockSpec((tile, width), lambda i, s: (i, 0)),
                pl.BlockSpec((cols, width), lambda i, s: (0, 0)),
            ],
            out_specs=pl.BlockSpec((length, cols), lambda i, s: (0, 0)),
            scratch_shapes=[pltpu.VMEM((length, cols), BF)],
        ),
        compiler_params=room(length, HEADS_GRAD),
        name="heads_grad",
    )(table, da, w_proj)


def back_kernel(
    n, tile, hw, width, ready, q, k, v, o, do, da_hbm, p_hbm, h1_hbm, all_hbm,
    ready_all, dqkv, sums, out,
    da, p, h1, o_all, dqt, dk, dv, load_s, p_s, *sems,
):
    me = lax.axis_index("ctx")
    length, cols = q.shape
    pairs = cols // 128
    slots = p.shape[0]
    greet(beside(n))
    gather = Gather(n, ready, ready_all, sems)
    gather.start()
    loads = [
        pltpu.make_async_copy(src, dst, load_s.at[i])
        for i, (src, dst) in enumerate([(da_hbm, da), (h1_hbm, h1), (all_hbm, o_all)])
    ]

    def load_p(pair):
        at = pair % slots
        return pltpu.make_async_copy(p_hbm.at[pl.ds(2 * pair, 2)], p.at[at], p_s.at[at])

    load_p(0).start()
    for load in loads:
        load.start()
    lane = lax.broadcasted_iota(jnp.int32, (1, 128), 1)
    held = {}

    def begin(pair):
        if pair + 1 < pairs and slots > 1:
            load_p(pair + 1).start()
        at = slice(pair * 128, pair * 128 + 128)
        held["k"] = k[:, at].astype(F32).T.astype(BF)
        prod = (do[:, at].astype(F32) * o[:, at].astype(F32)).T
        held["d"] = [jnp.sum(prod[64 * h : 64 * h + 64, :], axis=0, keepdims=True) for h in range(2)]
        dk[...] = jnp.zeros_like(dk)
        dv[...] = jnp.zeros_like(dv)
        load_p(pair).wait()

    def block(pair, i):
        win = pl.ds(i * tile, tile)
        at = slice(pair * 128, pair * 128 + 128)
        keys = (i + 1) * tile
        for h in range(2):
            here = (lane // 64) == h
            query = jnp.where(here, q[win, at].astype(F32), 0.0).astype(BF)
            grad = jnp.where(here, do[win, at].astype(F32), 0.0).astype(BF)
            prob = p[pair % slots, h, pl.ds(0, keys), win]
            dp = dot(v[pl.ds(0, keys), at], grad, NT)
            ds = (prob.astype(F32) * (dp - held["d"][h][:, i * tile : (i + 1) * tile]) * 0.125).astype(BF)
            half = slice(64 * h, 64 * h + 64)
            dqt[half, win] = dot(held["k"][half, :keys], ds)
            dk[pl.ds(0, keys), :] += dot(ds, query)
            dv[pl.ds(0, keys), :] += dot(prob, grad)

    def end(pair):
        for t, val in enumerate((dqt[...].T, dk[...], dv[...])):
            at = slice((t * pairs + pair) * 128, (t * pairs + pair) * 128 + 128)
            low = val.astype(BF)
            sums[:, at] = jnp.sum(low.astype(F32), axis=0, keepdims=True)
            dqkv[:, at] = low

    spare = max(0, width - 128 * n)
    whole_tiles = width // hw

    def products(rows, x, y):
        out[rows, 3 * cols :] = dot(y, da[:, pl.ds(pl.multiple_of(me * 128, 128), 128)], TN).astype(BF)

        @pl.when(me < n - 1 if spare else me < n)
        def _():
            out[rows, : 3 * cols] = dot(x, dqkv[...], TN).astype(BF)

        if spare:

            @pl.when(me == n - 1)
            def _():
                out[rows, : 3 * cols] = jnp.zeros((x.shape[1], 3 * cols), BF)
                out[rows, :spare] = dot(y, da[:, 128 * n :], TN).astype(BF)

    def weights(lo, hi):
        if lo == 0:
            for load in loads:
                load.wait()

        def body(i, carry):
            at = pl.ds(pl.multiple_of(i * hw, hw), hw)
            products(at, h1[:, at], o_all[i])
            return carry

        lax.fori_loop(lo, hi, body, 0)
        if hi == whole_tiles and width % hw:
            rest = width % hw
            at = pl.ds(hi * hw, rest)
            products(at, h1[:, at], o_all[hi, :, :rest])

    part = functools.partial
    steps = []
    for pair in range(pairs):
        steps.append((1.0, part(begin, pair)))
        steps += [(0.6 + 0.5 * i, part(block, pair, i)) for i in range(length // tile)]
        steps.append((1.0, part(end, pair)))
    cut = whole_tiles // 2
    steps += [(5.5, part(weights, 0, cut)), (5.5, part(weights, cut, whole_tiles))]
    clock, work = 0.0, []
    for size, step in steps:
        work.append((clock, step))
        clock += size
    timed(work, gather.timed_steps(lambda c: 3.5 * c, 6.0, 5.0))
    gather.finish()


def back(n, cid, ready, q, k, v, o, do, da, p, h1, o_all):
    length, hw = q.shape
    width = da.shape[1]
    if 128 * n > width:
        da = jnp.pad(da, ((0, 0), (0, 128 * n - width)))
    assert width <= 128 * n or (n - 1) * hw >= width and width - 128 * n <= 3 * hw
    dma = pltpu.SemaphoreType.DMA
    slots = min(2, hw // 128)
    return call(
        functools.partial(back_kernel, n, 256, hw, width),
        cid,
        "back",
        (ready, q, k, v, o, do, da, p, h1, o_all),
        [VMEM] * 6 + [ANY] * 4,
        [
            ((n,) + ready.shape, BF),
            ((length, 3 * hw), BF),
            ((1, 3 * hw), F32),
            ((width, 3 * hw + 128), BF),
        ],
        [ANY, VMEM, VMEM, VMEM],
        [
            pltpu.VMEM(da.shape, BF),
            pltpu.VMEM((slots, 2, length, length), BF),
            pltpu.VMEM(h1.shape, BF),
            pltpu.VMEM(o_all.shape, BF),
            pltpu.VMEM((128, length), F32),
            pltpu.VMEM((length, 128), F32),
            pltpu.VMEM((length, 128), F32),
            dma((3,)),
            dma((slots,)),
        ]
        + Gather.sems(n, ready.shape[0]),
        BACK if n == 8 else 60,
    )


def norm(values):
    centre = values - jnp.mean(values, axis=-1, keepdims=True)
    rstd = lax.rsqrt(jnp.mean(centre * centre, axis=-1, keepdims=True) + 1e-05)
    return centre * rstd, rstd


def norm_back(grad, unit, rstd, gain):
    inner = grad * gain
    return rstd * (
        inner
        - jnp.mean(inner, axis=-1, keepdims=True)
        - unit * jnp.mean(inner * unit, axis=-1, keepdims=True)
    )


def make_body(n, nz):
    def body(
        tokens, block_table, ln1_gain, ln1_bias, qkv_weight, query_bias, value_bias,
        proj_weight, proj_bias, ln2_gain, ln2_bias, fc_weight, fc_bias, out_weight,
        out_bias, cotangent,
    ):
        ctx = lax.axis_index("ctx")
        z = lax.axis_index("fsdp")
        rows, width = tokens.shape
        blk = rows // 2
        wz = width // nz
        slots = -(-HEADS // n)
        hw = slots * (width // HEADS)
        unit_z = out_weight.shape[0]
        uw = unit_z // n
        units = uw * nz
        table = block_table.reshape(-1)
        inv = jnp.argmax(
            table[None, :] == jnp.arange(table.shape[0], dtype=table.dtype)[:, None], axis=1
        ).astype(jnp.int32)

        take = lambda a, at, size, axis=0: lax.dynamic_slice_in_dim(a, at, size, axis)
        parts = 5
        padded = jnp.pad(qkv_weight, ((0, 0), (0, n * hw - width)))
        wq_own = jnp.concatenate(
            [take(padded, t * width + ctx * hw, hw, 1) for t in range(3)], axis=1
        ).reshape(parts, wz // parts, 3 * hw)
        row = lax.broadcasted_iota(jnp.int32, (16, wz), 0)
        small = jnp.zeros((16, wz), BF)
        for i, v in enumerate(
            [ln1_gain, ln1_bias, query_bias, value_bias, proj_bias, ln2_gain, ln2_bias, out_bias]
            + [jnp.pad(take(fc_bias, ctx * uw, uw), (0, wz - uw))]
        ):
            small = jnp.where(row == i, v[None, :], small)
        tile = math.gcd(wz, hw)
        h1, cot, small, w_qkv, w_proj, tok_own, cot_own, wfc_own, wout_own = entry(
            n,
            nz,
            tokens,
            cotangent,
            small,
            wq_own,
            proj_weight.reshape(wz // tile, tile, width),
            fc_weight.reshape(25, wz // 25, fc_weight.shape[1]),
            out_weight.reshape(n, uw, width),
            hw,
        )
        w_fc = lax.all_gather(wfc_own.reshape(wz, units), "fsdp", axis=0, tiled=True)
        w_out = lax.all_gather(wout_own, "fsdp", axis=0, tiled=True)
        length = n * rows
        flat = lambda a: a.reshape(length, a.shape[-1])
        h1, cot = flat(h1), flat(cot)
        w_qkv, w_proj = w_qkv.reshape(width, 3 * hw), w_proj.reshape(hw, width)
        fb = small[8].reshape(nz, wz)[:, :uw].reshape(1, units)
        pad_cols = lambda v: take(jnp.pad(v, (0, n * hw - width)), ctx * hw, hw)
        qkv_bias = jnp.concatenate([pad_cols(small[2]), jnp.zeros((hw,), F32), pad_cols(small[3])])

        qkv = (dot(h1, w_qkv) + qkv_bias).astype(BF)
        o, p, q_pos, k_pos, v_pos, o_pos = attend(qkv, inv, blk)
        mid, h2 = middle(n, 2, o, w_proj, tok_own, small)
        h2 = flat(h2)
        hidden, slope = hidden_units(h2, w_fc, fb)
        part_out = dot(hidden, cot, TN).astype(BF)
        in_parts = lambda a: a.reshape(nz, parts, a.shape[0] // nz // parts, a.shape[1])
        o, part_out = lax.optimization_barrier((o, part_out))
        o_all = spread(n, 3, o.reshape(4, length // 4, hw))
        h1_pos = order(h1, inv, blk)
        w_out, o_all, h1_pos = lax.optimization_barrier((w_out, o_all, h1_pos))
        to_owner = lambda a: lax.psum_scatter(a, "fsdp", scatter_dimension=0, tiled=True)
        sum_out = to_owner(part_out)
        du, dfb = hidden_back(cot, w_out, slope)
        part_fc = outer(h2, du)
        du, part_fc = lax.optimization_barrier((du, part_fc))
        sum_fc = to_owner(part_fc)
        da, dmid, layer_out, sums = turn(n, 4, du, w_fc, hidden, w_out, mid, cot_own, small)
        da = flat(da)
        all_out, dqkv, bias_cols, part_attn = back(
            n,
            6,
            sum_out.reshape(parts, uw // parts, width),
            q_pos,
            k_pos,
            v_pos,
            o_pos,
            heads_grad(da, w_proj, inv, blk),
            da,
            p,
            h1_pos,
            o_all.reshape(n, length, hw),
        )
        dqkv = order(dqkv, table, blk)

        put = lambda v, size: lax.dynamic_update_slice_in_dim(
            jnp.zeros((1, size), F32), v, ctx * v.shape[1], 1
        )
        biases = jnp.concatenate(
            [put(bias_cols[:, :hw], n * hw), put(bias_cols[:, 2 * hw :], n * hw)]
        )[:, :width]
        wide_fb = lax.dynamic_update_slice_in_dim(
            jnp.zeros((nz, unit_z), F32), dfb.reshape(nz, uw), ctx * uw, 1
        )
        vectors = jnp.concatenate(
            [sums + jnp.pad(biases, ((2, 4), (0, 0))), jnp.pad(wide_fb, ((0, -nz % 8), (0, width - unit_z)))]
        )
        all_fc, all_attn, grad_tokens, vectors = tail(
            n,
            nz,
            5,
            sum_fc.reshape(parts, wz // parts, units),
            in_parts(part_attn),
            dqkv,
            w_qkv,
            tok_own,
            dmid,
            small,
            vectors,
        )
        whole_rows = lambda a: a.reshape(n, a.shape[1] * a.shape[2], a.shape[3])
        grad_fc, grad_qkv, grad_proj, grad_out = join(
            n, nz, hw, whole_rows(all_fc), whole_rows(all_attn), all_out.reshape(unit_z, width)
        )
        vectors, grad_tokens, layer_out, grad_fc = lax.optimization_barrier(
            (vectors, grad_tokens, layer_out, grad_fc)
        )
        mine = take(vectors[:8], z * wz, wz, 1)
        gfb = take(vectors[8 : 8 + nz], z, 1).reshape(-1)[:unit_z]
        return (
            layer_out,
            grad_tokens,
            mine[0],
            mine[1],
            grad_qkv,
            mine[2],
            mine[3],
            grad_proj,
            mine[4],
            mine[5],
            mine[6],
            grad_fc,
            gfb,
            grad_out,
            mine[7],
        )

    return body


def solution(mesh):
    both = P(("fsdp", "ctx"), None)
    vec, mat = P("fsdp"), P("fsdp", None)
    placed = (both, P(), vec, vec, mat, vec, vec, mat, vec, vec, vec, mat, vec, mat, vec, both)
    outs = (both, both, vec, vec, mat, vec, vec, mat, vec, vec, vec, mat, vec, mat, vec)
    return jax.shard_map(
        make_body(mesh.shape["ctx"], mesh.shape["fsdp"]),
        mesh=mesh,
        in_specs=placed,
        out_specs=outs,
        check_vma=False,
    )
```

```python
import functools
import math

import jax
import jax.numpy as jnp
from jax import lax
from jax.experimental import pallas as pl
from jax.experimental.pallas import tpu as pltpu
from jax.sharding import PartitionSpec as P

HEADS = 25
BF = jnp.bfloat16
F32 = jnp.float32
MESH = pl.DeviceIdType.MESH
ENTRY, ATTEND, MIDDLE, SPREAD, TURN, BACK, TAIL = 60, 60, 60, 60, 60, 60, 30
HIDDEN, HIDDEN_BACK, OUTER, ORDER, HEADS_GRAD, JOIN = 60, 60, 60, 9, 60, 8
ANY = pl.BlockSpec(memory_space=pl.ANY)
VMEM = pl.BlockSpec(memory_space=pltpu.VMEM)
HBM = pl.BlockSpec(memory_space=pltpu.HBM)
NN = (((1,), (0,)), ((), ()))
NT = (((1,), (1,)), ((), ()))
TN = (((0,), (0,)), ((), ()))


def room(length, mib):
    return pltpu.CompilerParams(vmem_limit_bytes=(mib if length <= 1024 else 60) * 1024 * 1024)


def dot(a, b, dims=NN):
    return lax.dot_general(a, b, dims, preferred_element_type=F32)


def places(n):
    me = lax.axis_index("ctx")
    core = lax.rem(me, 2)
    chip = me // 2
    sib = me + 1 - 2 * core
    if n == 8:
        across = chip + 1 - 2 * lax.rem(chip, 2)
        along = lax.rem(chip + 2, 4)
        first = across * (1 - core) + along * core
        second = along * (1 - core) + across * core
        others = [first, second, 3 - chip]
    else:
        half = n // 2
        others = [lax.rem(chip + d, half) for d in range(1, half)]
    return me, core, chip, sib, others


def twin(square, k):
    return 1 - k if square and k < 2 else k


def signal(sem, **device):
    pl.semaphore_signal(sem, inc=1, device_id=device, device_id_type=MESH)


def greet(devices, planes=()):
    barrier = pltpu.get_barrier_semaphore()
    for device in devices:
        signal(barrier, ctx=device)
    for plane in planes:
        signal(barrier, fsdp=plane)
    pl.semaphore_wait(barrier, len(devices) + len(planes))


def send(src, dst, ssem, rsem, **device):
    return pltpu.make_async_remote_copy(
        src_ref=src,
        dst_ref=dst,
        send_sem=ssem,
        recv_sem=rsem,
        device_id=device,
        device_id_type=MESH,
    )


def merge(*lists, scales=None):
    keyed = []
    for t, steps in enumerate(lists):
        scale = scales[t] if scales else 1.0
        keyed += [((i + 0.5) * scale / len(steps), t, i, step) for i, step in enumerate(steps)]
    for item in sorted(keyed, key=lambda k: k[:3]):
        item[3]()


def timed(*lists):
    keyed = [(time, t, i, step) for t, steps in enumerate(lists) for i, (time, step) in enumerate(steps)]
    for item in sorted(keyed, key=lambda k: k[:3]):
        item[3]()


def spaced(steps, start, stop):
    return [(start + (stop - start) * (i + 0.5) / len(steps), step) for i, step in enumerate(steps)]


class Gather:
    def __init__(self, n, src, out, sems):
        self.n, self.src, self.out = n, src, out
        self.own_s, self.sib_s, self.sib_r, self.far_s, self.far_r = sems
        self.parts = src.shape[0]
        self.square = n == 8
        self.me, self.core, self.chip, self.sib, self.others = places(n)
        half = n // 2
        if self.square:
            self.froms = self.others
        else:
            self.froms = [lax.rem(self.chip + half - d, half) for d in range(1, half)]
        self.peers = self.others[:2] if self.square else self.others
        self.started = []

    @staticmethod
    def sems(n, parts):
        dma = pltpu.SemaphoreType.DMA
        far = n // 2 - 1
        return [dma((parts,)), dma((far + 1, parts)), dma((far + 1, parts)), dma((far, parts)), dma((far, parts))]

    def own_sends(self, c):
        piece, slot = self.src.at[c], self.out.at[self.me, c]
        copies = [
            send(piece, slot, self.far_s.at[d, c], self.far_r.at[d, c], ctx=2 * p + self.core)
            for d, p in enumerate(self.peers)
        ]
        copies.append(send(piece, slot, self.sib_s.at[0, c], self.sib_r.at[0, c], ctx=self.sib))
        return copies + [pltpu.make_async_copy(piece, slot, self.own_s.at[c])]

    def go(self, copy):
        copy.start()
        self.started.append(copy)

    def start(self):
        for c in range(self.parts):
            self.start_part(c)

    def start_part(self, c):
        for copy in self.own_sends(c):
            copy.start()

    def arrived(self, d, c):
        piece = self.out.at[2 * self.froms[d] + self.core, c]
        send(piece, piece, self.far_s.at[d, c], self.far_r.at[d, c], ctx=self.sib).wait_recv()
        if self.square and d == 0:
            self.go(
                send(
                    piece,
                    piece,
                    self.far_s.at[2, c],
                    self.far_r.at[2, c],
                    ctx=2 * self.others[1] + self.core,
                )
            )
        e = twin(self.square, d) + 1
        self.go(send(piece, piece, self.sib_s.at[e, c], self.sib_r.at[e, c], ctx=self.sib))

    def steps(self):
        todo = []
        for c in range(self.parts):
            for d in range(2 if self.square else len(self.others)):
                todo.append(functools.partial(self.arrived, d, c))
            if self.square and c:
                todo.append(functools.partial(self.arrived, 2, c - 1))
        if self.square:
            todo.append(functools.partial(self.arrived, 2, self.parts - 1))
        return todo

    def timed_steps(self, begin, wait, relay):
        todo = []
        for c in range(self.parts):
            for d in range(len(self.others)):
                late = relay if self.square and d == 2 else 0
                todo.append((begin(c) + wait + late, functools.partial(self.arrived, d, c)))
        return todo

    def finish(self):
        for c in range(self.parts):
            *far, own = self.own_sends(c)
            own.wait()
            for copy in far:
                copy.wait_send()
        for d in range(len(self.others) + 1):
            chip = self.chip if d == 0 else self.froms[d - 1]
            for c in range(self.parts):
                piece = self.out.at[2 * chip + 1 - self.core, c]
                send(
                    piece, piece, self.sib_s.at[d, c], self.sib_r.at[d, c], ctx=self.sib
                ).wait_recv()
        for copy in self.started:
            copy.wait_send()


class Relay:
    def __init__(self, nz, z, lo, hi, count, src, out, sems, lead):
        self.nz, self.z, self.lo, self.hi, self.count = nz, z, lo, hi, count
        self.src, self.out, self.lead = src, out, lead
        self.own_s, self.up_s, self.down_s, self.recv = sems

    @staticmethod
    def sems(blocks):
        return [pltpu.SemaphoreType.DMA((blocks,)) for _ in range(4)]

    def up(self, src, b):
        return send(src, self.out.at[b], self.up_s.at[b], self.recv.at[b], fsdp=self.z + 1)

    def down(self, src, b):
        return send(src, self.out.at[b], self.down_s.at[b], self.recv.at[b], fsdp=self.z - 1)

    def own(self, b):
        return pltpu.make_async_copy(self.src.at[b - self.lead], self.out.at[b], self.own_s.at[b])

    def start(self):
        lo, hi = self.lo, self.hi

        def body(i, carry):
            u, d = hi - 1 - i, lo + i

            @pl.when(self.z < self.nz - 1)
            def _():
                self.up(self.src.at[u - self.lead], u).start()

            @pl.when(self.z > 0)
            def _():
                self.down(self.src.at[d - self.lead], d).start()

            self.own(d).start()
            return carry

        lax.fori_loop(0, hi - lo, body, 0)

    def step(self, i):
        b = self.lo - 1 - i

        @pl.when(b >= 0)
        def _():
            self.up(self.out.at[b], b).wait_recv()

            @pl.when(self.z < self.nz - 1)
            def _():
                self.up(self.out.at[b], b).start()

        e = self.hi + i

        @pl.when(e < self.count)
        def _():
            self.down(self.out.at[e], e).wait_recv()

            @pl.when(self.z > 0)
            def _():
                self.down(self.out.at[e], e).start()

    def steps(self, most):
        return [functools.partial(self.step, i) for i in range(most)]

    def finish(self):
        def sent(b, carry):
            @pl.when((self.z < self.nz - 1) & (b < self.hi))
            def _():
                self.up(self.out.at[b], b).wait_send()

            @pl.when((self.z > 0) & (b >= self.lo))
            def _():
                self.down(self.out.at[b], b).wait_send()

            @pl.when((b >= self.lo) & (b < self.hi))
            def _():
                self.own(b).wait()

            return carry

        lax.fori_loop(0, self.count, sent, 0)


def others_of(z, nz):
    return [lax.rem(z + d, nz) for d in range(1, nz)]


def entry_kernel(
    n, nz, tok_t, cot_t, small, wq, wp, fc_hbm, out_hbm, h1_all, cot_all, vec, wq_all, wp_all, tok, cot_own,
    fc_own, out_own, *scratch
):
    cot, h1, inbox, zeros, fc_all, load_s, small_s, small_r, zero_s = scratch[:9]
    g_h, g_c = scratch[9:14], scratch[14:19]
    r_q, r_p = scratch[19:23], scratch[23:27]
    loads = [
        pltpu.make_async_copy(fc_hbm, fc_all, load_s.at[0]),
        pltpu.make_async_copy(out_hbm.at[lax.axis_index("ctx")], out_own, load_s.at[1]),
    ]
    me, core, chip, sib, others = places(n)
    z = lax.axis_index("fsdp")
    planes = others_of(z, nz)
    greet([sib] + [2 * p + core for p in (others[:2] if n == 8 else others)], planes)
    wz = small.shape[1]
    for d, plane in enumerate(planes):
        send(small, inbox.at[z], small_s.at[d], small_r.at[d], fsdp=plane).start()
    inbox[z] = small[...]
    k = wq.shape[0]
    relay_q = Relay(nz, z, z * k, (z + 1) * k, nz * k, wq, wq_all, r_q, z * k)
    relay_q.start()
    parts, rows = h1.shape[0], h1.shape[1]
    turned = cot_t[...].astype(F32).T.astype(BF)
    cot_own[...] = turned
    for c in range(parts):
        cot[c] = turned[c * rows : (c + 1) * rows, :]
    gather_c = Gather(n, cot, cot_all, g_c)
    gather_c.start()
    tok[...] = tok_t[...].astype(F32).T.astype(BF)
    share, blocks = wp.shape[0], wp_all.shape[0]
    base = me * blocks
    valid = jnp.clip(nz * share - base, 0, blocks)
    lo = jnp.clip(z * share - base, 0, valid)
    hi = jnp.clip((z + 1) * share - base, 0, valid)
    relay_p = Relay(nz, z, lo, hi, valid, wp, wp_all, r_p, z * share - base)
    relay_p.start()
    zeros[...] = jnp.zeros_like(zeros)

    def clear(b, carry):
        pltpu.make_async_copy(zeros, wp_all.at[b], zero_s.at[b]).start()
        return carry

    lax.fori_loop(valid, blocks, clear, 0)
    for d in range(nz - 1):
        came = lax.rem(z + nz - 1 - d, nz)
        send(small, inbox.at[came], small_s.at[d], small_r.at[d], fsdp=planes[d]).wait_recv()
    for p in range(nz):
        vec[:, p * wz : (p + 1) * wz] = inbox[p].astype(F32)
    gain, shift = vec[0:1, :], vec[1:2, :]
    gather_h = Gather(n, h1, h1_all, g_h)
    for c in range(parts):
        unit, _ = norm(tok[c * rows : (c + 1) * rows, :].astype(F32))
        h1[c] = (unit * gain + shift).astype(BF)
        gather_h.start_part(c)
    for load in loads:
        load.start()

    def columns():
        for load in loads:
            load.wait()
        uw = fc_own.shape[-1] // nz
        for place in range(n):

            @pl.when(me == place)
            def _():
                def tile(i, carry):
                    for t in range(nz):
                        at = (t * n + place) * uw
                        fc_own[i, :, t * uw : (t + 1) * uw] = fc_all[i, :, at : at + uw]
                    return carry

                lax.fori_loop(0, fc_own.shape[0], tile, 0)

    steps = gather_c.steps() + gather_h.steps()
    merge(
        steps[:4] + [columns] + steps[4:],
        relay_q.steps(nz * k - k) + relay_p.steps(blocks),
    )
    gather_c.finish()
    gather_h.finish()
    relay_q.finish()
    relay_p.finish()

    def cleared(b, carry):
        pltpu.make_async_copy(zeros, wp_all.at[b], zero_s.at[b]).wait()
        return carry

    lax.fori_loop(valid, blocks, cleared, 0)
    for d, plane in enumerate(planes):
        send(small, inbox.at[z], small_s.at[d], small_r.at[d], fsdp=plane).wait_send()


def entry(n, nz, tokens, cot, small, wq, wp, fc, out, hw):
    rows, width = tokens.shape
    parts = 2 if n == 8 else 1
    dma = pltpu.SemaphoreType.DMA
    k, tile = wq.shape[0], wp.shape[1]
    blocks = hw // tile
    shape = jax.ShapeDtypeStruct
    piece = (parts, rows // parts, width)
    return pl.pallas_call(
        functools.partial(entry_kernel, n, nz),
        out_shape=[
            shape((n,) + piece, BF),
            shape((n,) + piece, BF),
            shape((small.shape[0], width), F32),
            shape((nz * k,) + wq.shape[1:], BF),
            shape((blocks, tile, width), BF),
            shape((rows, width), BF),
            shape((rows, width), BF),
            shape(fc.shape[:2] + (fc.shape[2] // n,), BF),
            shape(out.shape[1:], BF),
        ],
        in_specs=[VMEM] * 5 + [HBM, HBM],
        out_specs=[ANY, ANY, VMEM, ANY, ANY] + [VMEM] * 4,
        scratch_shapes=[
            pltpu.VMEM(piece, BF),
            pltpu.VMEM(piece, BF),
            pltpu.VMEM((nz,) + small.shape, BF),
            pltpu.VMEM((tile, width), BF),
            pltpu.VMEM(fc.shape, BF),
            dma((2,)),
            dma((nz - 1,)),
            dma((nz - 1,)),
            dma((blocks,)),
        ]
        + Gather.sems(n, parts)
        + Gather.sems(n, parts)
        + Relay.sems(nz * k)
        + Relay.sems(blocks),
        compiler_params=pltpu.CompilerParams(
            collective_id=1, has_side_effects=True, vmem_limit_bytes=(ENTRY if n == 8 else 60) * 1024 * 1024
        ),
        name="entry",
    )(tokens.T, cot.T, small, wq, wp, fc, out)


class Scatter:
    def __init__(self, n, dims, a, w, scratch):
        self.n, self.dims, self.a, self.w = n, dims, a, w
        self.part, self.theirs, self.sums, self.inbox = scratch[:4]
        self.sib_s, self.sib_r, self.far_s, self.far_r = scratch[4:]
        self.me, self.core, self.chip, self.sib, self.others = places(n)
        self.square = n == 8
        self.half = n // 2
        self.parts = self.sib_s.shape[1]
        self.full = self.part.shape[2]
        self.rows = self.full // self.parts
        if self.square:
            first, second = [2 * p + self.core for p in self.others[:2]]
            self.ends = [(0, 0, first), (1, 1, first), (2, 2, second)]
        else:
            self.ends = [(k, k, 2 * self.others[k] + self.core) for k in range(self.half - 1)]

    @staticmethod
    def scratch(n, rows, width):
        dma = pltpu.SemaphoreType.DMA
        half, parts = n // 2, 4 if n == 8 else 1
        return [
            pltpu.VMEM((half, 2, rows, width), BF),
            pltpu.VMEM((half, rows, width), BF),
            pltpu.VMEM((half - 1, rows, width), BF),
            pltpu.VMEM((half - 1, rows, width), BF),
            dma((half, parts)),
            dma((half, parts)),
            dma((half - 1, parts)),
            dma((half - 1, parts)),
        ]

    def chip_at(self, k):
        if not self.square:
            return lax.rem(self.chip + 1 + k, self.half)
        x, y = lax.rem(self.chip, 2), self.chip // 2
        first, second = 1 - lax.rem(k, 3) // 2, 1 - lax.rem(k, 2)
        dx = first * (1 - self.core) + second * self.core
        dy = second * (1 - self.core) + first * self.core
        far = (k < 3).astype(jnp.int32)
        dx, dy = dx * far, dy * far
        return (y + dy - 2 * y * dy) * 2 + x + dx - 2 * x * dx

    def twin_at(self, k):
        if not self.square:
            return k
        return k + jnp.where(k == 1, 1, 0) - jnp.where(k == 2, 1, 0)

    def win(self, c):
        return pl.ds(c * self.rows, self.rows)

    def to_sib(self, k, c):
        e = self.twin_at(k)
        return send(
            self.part.at[k, 1 - self.core, self.win(c)],
            self.theirs.at[e, self.win(c)],
            self.sib_s.at[e, c],
            self.sib_r.at[e, c],
            ctx=self.sib,
        )

    def chip_sum(self, k, c):
        win = self.win(c)
        piece = self.theirs.at[k, win]
        send(piece, piece, self.sib_s.at[k, c], self.sib_r.at[k, c], ctx=self.sib).wait_recv()
        return self.part[k, self.core, win, :].astype(F32) + self.theirs[k, win, :].astype(F32)

    def pass_on(self, k, slot, peer, c):
        return send(
            self.sums.at[k, self.win(c)],
            self.inbox.at[slot, self.win(c)],
            self.far_s.at[slot, c],
            self.far_r.at[slot, c],
            ctx=peer,
        )

    def wait_in(self, slot, c):
        piece = self.inbox.at[slot, self.win(c)]
        send(piece, piece, self.far_s.at[slot, c], self.far_r.at[slot, c], ctx=self.sib).wait_recv()
        return self.inbox[slot, self.win(c), :].astype(F32)

    def forward(self, end, c):
        k, slot, peer = self.ends[end]
        total = self.chip_sum(k, c)
        if self.square and end == 2:
            total = total + self.wait_in(0, c)
        self.sums[k, self.win(c), :] = total.astype(BF)
        self.pass_on(k, slot, peer, c).start()

    def products(self):
        def product(k, carry):
            full = self.full
            at = pl.ds(pl.multiple_of(self.chip_at(k) * 2 * full, 2 * full), 2 * full)
            val = dot(self.a[at, :], self.w[...], self.dims).astype(BF)
            self.part[k, 0] = val[:full]
            self.part[k, 1] = val[full:]
            for c in range(self.parts):
                self.to_sib(k, c).start()

            @pl.when(k == 1)
            def _():
                for c in range(self.parts):
                    self.forward(0, c)

            return carry

        lax.fori_loop(0, self.half, product, 0)

    def forwards(self):
        each = range(self.parts)
        return [functools.partial(self.forward, e, c) for e in range(1, self.half - 1) for c in each]

    def total(self, c):
        val = self.chip_sum(self.half - 1, c)
        for slot in (1, 2) if self.square else range(self.half - 1):
            val = val + self.wait_in(slot, c)
        return val

    def finish(self):
        for c in range(self.parts):
            for k, slot, peer in self.ends:
                self.pass_on(k, slot, peer, c).wait_send()

        def sent(k, carry):
            for c in range(self.parts):
                self.to_sib(k, c).wait_send()
            return carry

        lax.fori_loop(0, self.half, sent, 0)


class Line:
    def __init__(self, nz, z, src, out, scratch):
        self.nz, self.z, self.src, self.out = nz, z, src, out
        self.mine, self.above, self.below, self.load_s, self.up_s, self.down_s, self.recv = scratch
        self.parts = src.shape[1]

    @staticmethod
    def scratch(shape):
        dma, lead = pltpu.SemaphoreType.DMA, shape[:2]
        return [pltpu.VMEM(shape, BF)] * 3 + [dma((1,)), dma(lead), dma(lead), dma((2,) + lead)]

    def up(self, src, d, c):
        return send(
            src.at[d, c], self.above.at[d, c], self.up_s.at[d, c], self.recv.at[0, d, c], fsdp=self.z + 1
        )

    def down(self, src, d, c):
        return send(
            src.at[d, c], self.below.at[d, c], self.down_s.at[d, c], self.recv.at[1, d, c], fsdp=self.z - 1
        )

    def start(self):
        top = self.nz - 1

        @pl.when(self.z == 0)
        def _():
            for c in range(self.parts):
                for k in range(top):
                    self.up(self.src, top - k, c).start()

        @pl.when(self.z == top)
        def _():
            for c in range(self.parts):
                for k in range(top):
                    self.down(self.src, k, c).start()

        self.load = pltpu.make_async_copy(self.src, self.mine, self.load_s.at[0])
        self.load.start()

    def loaded(self):
        self.load.wait()

    def pass_up(self, d, c):
        copy = self.up(self.mine, d, c)
        copy.wait_recv()
        self.mine[d, c] = self.mine[d, c] + self.above[d, c]
        copy.start()

    def pass_down(self, d, c):
        copy = self.down(self.mine, d, c)
        copy.wait_recv()
        self.mine[d, c] = self.mine[d, c] + self.below[d, c]
        copy.start()

    def settle(self, place, c):
        z, top = place, self.nz - 1
        total = self.mine[z, c].astype(F32)
        if z > 0:
            self.up(self.mine, z, c).wait_recv()
            total = total + self.above[z, c].astype(F32)
        if z < top:
            self.down(self.mine, z, c).wait_recv()
            total = total + self.below[z, c].astype(F32)
        self.out[c] = total.astype(BF)

    def timed_steps(self, after):
        top = self.nz - 1
        slots = {}

        def put(time, place, fn):
            slots.setdefault(time, {}).setdefault(place, []).append(fn)

        for c in range(self.parts):
            for place in range(self.nz):
                for k in range(top):
                    at = c * top + k
                    if 0 < place < top - k:
                        put(at + place, place, functools.partial(self.pass_up, top - k, c))
                    if k < place < top:
                        put(at + top - place, place, functools.partial(self.pass_down, k, c))
                put((c + 1) * top, place, functools.partial(self.settle, place, c))
                put((c + 1) * top, place, functools.partial(after, c))

        def run(work):
            for place, fns in sorted(work.items()):

                @pl.when(self.z == place)
                def _():
                    for fn in fns:
                        fn()

        return [(0, self.loaded)] + [(t, functools.partial(run, slots[t])) for t in sorted(slots)]

    def finish(self):
        for d in range(self.nz):

            @pl.when(self.z < d)
            def _():
                for c in range(self.parts):
                    self.up(self.mine, d, c).wait_send()

            @pl.when(self.z > d)
            def _():
                for c in range(self.parts):
                    self.down(self.mine, d, c).wait_send()


class Vectors:
    def __init__(self, n, nz, src, out, scratch):
        self.n, self.nz, self.src, self.out = n, nz, src, out
        self.low, self.from_sib, self.chips, self.line = scratch[:4]
        self.ss, self.sr, self.cs, self.cr, self.ls, self.lr = scratch[4:]
        self.me, self.core, self.chip, self.sib, self.others = places(n)
        self.z = lax.axis_index("fsdp")
        self.planes = others_of(self.z, nz)

    @staticmethod
    def scratch(n, nz, shape):
        dma = pltpu.SemaphoreType.DMA
        half = n // 2
        return [
            pltpu.VMEM(shape, BF),
            pltpu.VMEM(shape, BF),
            pltpu.VMEM((half,) + shape, BF),
            pltpu.VMEM((nz,) + shape, BF),
            dma((1,)),
            dma((1,)),
            dma((half - 1,)),
            dma((half - 1,)),
            dma((nz - 1,)),
            dma((nz - 1,)),
        ]

    def to_sib(self):
        return send(self.low, self.from_sib, self.ss.at[0], self.sr.at[0], ctx=self.sib)

    def to_chip(self, d):
        at = self.chips.at[self.chip]
        return send(at, at, self.cs.at[d], self.cr.at[d], ctx=2 * self.others[d] + self.core)

    def to_plane(self, d):
        at = self.line.at[self.z]
        return send(at, at, self.ls.at[d], self.lr.at[d], fsdp=self.planes[d])

    def start(self):
        self.low[...] = self.src[...].astype(BF)
        self.to_sib().start()

    def first(self):
        self.to_sib().wait_recv()
        self.chips[self.chip] = self.low[...] + self.from_sib[...]
        for d in range(self.n // 2 - 1):
            self.to_chip(d).start()

    def second(self):
        for d in range(self.n // 2 - 1):
            self.to_chip(d).wait_recv()
        total = self.chips[0].astype(F32)
        for k in range(1, self.n // 2):
            total = total + self.chips[k].astype(F32)
        self.line[self.z] = total.astype(BF)
        for d in range(self.nz - 1):
            self.to_plane(d).start()

    def third(self):
        for d in range(self.nz - 1):
            self.to_plane(d).wait_recv()
        total = self.line[0].astype(F32)
        for k in range(1, self.nz):
            total = total + self.line[k].astype(F32)
        self.out[...] = total

    def steps(self):
        return [self.first, self.second, self.third]

    def finish(self):
        self.to_sib().wait_send()
        for d in range(self.n // 2 - 1):
            self.to_chip(d).wait_send()
        for d in range(self.nz - 1):
            self.to_plane(d).wait_send()


def beside(n):
    me, core, chip, sib, others = places(n)
    return [sib] + [2 * p + core for p in (others[:2] if n == 8 else others)]


def call(kernel, cid, name, ins, in_specs, outs, out_specs, scratch, mib=60):
    return pl.pallas_call(
        kernel,
        out_shape=[jax.ShapeDtypeStruct(*o) for o in outs],
        in_specs=in_specs,
        out_specs=out_specs,
        scratch_shapes=scratch,
        compiler_params=pltpu.CompilerParams(
            collective_id=cid, has_side_effects=True, vmem_limit_bytes=mib * 1024 * 1024
        ),
        name=name,
    )(*ins)


def middle_kernel(n, o, w, tok, vec, mid, h2_all, h2, *scratch):
    greet(beside(n))
    scatter = Scatter(n, NN, o, w, scratch[:8])
    gather = Gather(n, h2, h2_all, scratch[8:])
    scatter.products()
    for step in scatter.forwards():
        step()
    for c in range(gather.parts):
        win = scatter.win(c)
        val = tok[win, :].astype(F32) + scatter.total(c) + vec[4:5, :]
        mid[win, :] = val
        h2[c] = (norm(val)[0] * vec[5:6, :] + vec[6:7, :]).astype(BF)
        gather.start_part(c)
    for step in gather.steps():
        step()
    gather.finish()
    scatter.finish()


def middle(n, cid, o, w, tok, vec):
    rows, width = tok.shape
    parts = 4 if n == 8 else 1
    piece = (parts, rows // parts, width)
    return call(
        functools.partial(middle_kernel, n),
        cid,
        "middle",
        (o, w, tok, vec),
        [VMEM] * 4,
        [((rows, width), F32), ((n,) + piece, BF)],
        [VMEM, ANY],
        [pltpu.VMEM(piece, BF)] + Scatter.scratch(n, rows, width) + Gather.sems(n, parts),
        MIDDLE if n == 8 else 60,
    )


def spread_kernel(n, src, all_ref, *sems):
    greet(beside(n))
    gather = Gather(n, src, all_ref, sems)
    gather.start()
    for step in gather.steps():
        step()
    gather.finish()


def spread(n, cid, array):
    return call(
        functools.partial(spread_kernel, n),
        cid,
        "spread",
        (array,),
        [VMEM],
        [((n,) + array.shape, BF)],
        [ANY],
        Gather.sems(n, array.shape[0]),
        SPREAD if n == 8 else 60,
    )[0]


def turn_kernel(
    n, du, w_fc, hid_in, w_out_in, mid_in, cot_in, vec, da_all, dmid, layer, sums,
    da, hid, w_out, mid, cot, load_s, *scratch,
):
    loads = [
        pltpu.make_async_copy(src, dst, load_s.at[i])
        for i, (src, dst) in enumerate([(hid_in, hid), (w_out_in, w_out), (mid_in, mid), (cot_in, cot)])
    ]
    for load in loads:
        load.start()
    greet(beside(n))
    back = Scatter(n, NT, du, w_fc, scratch[:8])
    ahead = Scatter(n, NN, hid, w_out, scratch[8:16])
    gather = Gather(n, da, da_all, scratch[16:])
    back.products()
    todo = back.forwards()
    for step in todo[: back.parts]:
        step()
    for load in loads:
        load.wait()
    ahead.products()
    for step in todo[back.parts :]:
        step()
    sums[...] = jnp.zeros_like(sums)
    for c in range(gather.parts):
        win = back.win(c)
        grad = back.total(c)
        unit, rstd = norm(mid[win, :])
        up = cot[win, :].astype(F32)
        val = up + norm_back(grad, unit, rstd, vec[5:6, :])
        dmid[win, :] = val
        low = val.astype(BF)
        da[c] = low
        gather.start_part(c)
        for row, term in ((4, low.astype(F32)), (5, grad * unit), (6, grad), (7, up)):
            sums[row : row + 1, :] += jnp.sum(term, axis=0, keepdims=True)
    merge(gather.steps(), ahead.forwards())
    for c in range(gather.parts):
        win = ahead.win(c)
        layer[win, :] = (mid[win, :] + ahead.total(c) + vec[7:8, :]).astype(BF)
    gather.finish()
    back.finish()
    ahead.finish()


def turn(n, cid, du, w_fc, hidden, w_out, mid, cot, vec):
    rows, width = mid.shape
    parts = 4 if n == 8 else 1
    piece = (parts, rows // parts, width)
    return call(
        functools.partial(turn_kernel, n),
        cid,
        "turn",
        (du, w_fc, hidden, w_out, mid, cot, vec),
        [VMEM] * 2 + [ANY] * 4 + [VMEM],
        [((n,) + piece, BF), ((rows, width), F32), ((rows, width), BF), ((8, width), F32)],
        [ANY, VMEM, VMEM, VMEM],
        [pltpu.VMEM(piece, BF)]
        + [pltpu.VMEM(a.shape, a.dtype) for a in (hidden, w_out, mid, cot)]
        + [pltpu.SemaphoreType.DMA((4,))]
        + Scatter.scratch(n, rows, width)
        + Scatter.scratch(n, rows, width)
        + Gather.sems(n, parts),
        TURN if n == 8 else 60,
    )


def tail_kernel(
    n, nz, fc, part, dqkv, w_qkv, tok, dmid, vec, v_in, fc_all, attn_all, g_tok, v_out,
    v_own, attn, fc_v, dqkv_v, w_v, load_s, *scratch,
):
    z = lax.axis_index("fsdp")
    me, core, chip, sib, others = places(n)
    greet([sib] + [2 * p + core for p in others], others_of(z, nz))
    line = Line(nz, z, part, attn, scratch[:7])
    line.start()
    loads = [
        pltpu.make_async_copy(src, dst, load_s.at[i])
        for i, (src, dst) in enumerate([(dqkv, dqkv_v), (w_qkv, w_v), (fc, fc_v)])
    ]
    for load in loads:
        load.start()
    fc, dqkv, w_qkv = fc_v, dqkv_v, w_v
    scatter = Scatter(n, NT, dqkv, w_qkv, scratch[7:15])
    vectors = Vectors(n, nz, v_own, v_out, scratch[15:25])
    fc_g = Gather(n, fc, fc_all, scratch[25:30])
    attn_g = Gather(n, attn, attn_all, scratch[30:35])
    v_own[...] = v_in[...]
    for load in loads[:2]:
        load.wait()
    scatter.products()
    todo = scatter.forwards()
    for step in todo[: scatter.parts]:
        step()
    loads[2].wait()

    def rest(c):
        win = scatter.win(c)
        grad = scatter.total(c)
        unit, rstd = norm(tok[win, :].astype(F32))
        g_tok[win, :] = (dmid[win, :] + norm_back(grad, unit, rstd, vec[0:1, :])).astype(BF)
        v_own[0:1, :] += jnp.sum(grad * unit, axis=0, keepdims=True)
        v_own[1:2, :] += jnp.sum(grad, axis=0, keepdims=True)

    top = nz - 1
    last = attn_g.parts * top
    part_at = functools.partial
    fc_at = lambda c: 4.0 + 2.0 * c
    timed(
        spaced(todo[scatter.parts :], 1.0, 4.0),
        spaced([part_at(rest, c) for c in range(scatter.parts)], 4.5, 7.0),
        [(7.1, vectors.start), (7.8, vectors.first), (11.0, vectors.second), (last + 3.0, vectors.third)],
        [(fc_at(c), part_at(fc_g.start_part, c)) for c in range(fc_g.parts)],
        fc_g.timed_steps(fc_at, 2.2, 1.6),
        line.timed_steps(attn_g.start_part),
        attn_g.timed_steps(lambda c: (c + 1) * top, 2.2, 1.6),
    )
    for job in (fc_g, attn_g, scatter, line, vectors):
        job.finish()


def tail(n, nz, cid, fc, part, dqkv, w_qkv, tok, dmid, vec, v_in):
    rows, width = tok.shape
    attn = part.shape[1:]
    return call(
        functools.partial(tail_kernel, n, nz),
        cid,
        "tail",
        (fc, part, dqkv, w_qkv, tok, dmid, vec, v_in),
        [HBM] * 4 + [VMEM] * 4,
        [((n,) + fc.shape, BF), ((n,) + attn, BF), (tok.shape, BF), (v_in.shape, F32)],
        [ANY, ANY, VMEM, VMEM],
        [pltpu.VMEM(v_in.shape, F32), pltpu.VMEM(attn, BF)]
        + [pltpu.VMEM(a.shape, BF) for a in (fc, dqkv, w_qkv)]
        + [pltpu.SemaphoreType.DMA((3,))]
        + Line.scratch(part.shape)
        + Scatter.scratch(n, rows, width)
        + Vectors.scratch(n, nz, v_in.shape)
        + Gather.sems(n, fc.shape[0])
        + Gather.sems(n, attn[0]),
        TAIL if n == 8 else 60,
    )


def outer_kernel(x_ref, y_ref, out_ref):
    out_ref[...] = dot(x_ref[...], y_ref[...], TN).astype(BF)


def outer(x, y):
    rows, m = x.shape
    tile = 256
    return pl.pallas_call(
        outer_kernel,
        grid=(pl.cdiv(m, tile),),
        out_shape=jax.ShapeDtypeStruct((m, y.shape[1]), BF),
        in_specs=[pl.BlockSpec((rows, tile), lambda i: (0, i)), fixed(*y.shape)],
        out_specs=tiled(tile, y.shape[1]),
        compiler_params=room(rows, OUTER),
        name="outer",
    )(x, y)


def hidden_kernel(h_ref, w_ref, b_ref, z_ref, s_ref):
    u = dot(h_ref[...], w_ref[...]) + b_ref[...]
    root = 0.7978845608028654
    square = u * u
    inner = jnp.tanh(root * u * (1.0 + 0.044715 * square))
    z_ref[...] = (0.5 * u * (1.0 + inner)).astype(BF)
    slope = 0.5 * (1.0 + inner) + 0.5 * u * (1.0 - inner * inner) * root * (1.0 + 3 * 0.044715 * square)
    s_ref[...] = slope.astype(BF)


def hidden_back_kernel(c_ref, w_ref, s_ref, d_ref, sum_ref):
    du = (dot(c_ref[...], w_ref[...], NT) * s_ref[...].astype(F32)).astype(BF)
    d_ref[...] = du

    @pl.when(pl.program_id(0) == 0)
    def _():
        sum_ref[...] = jnp.zeros_like(sum_ref)

    sum_ref[...] += jnp.sum(du.astype(F32), axis=0, keepdims=True)


def tiled(rows, cols):
    return pl.BlockSpec((rows, cols), lambda i: (i, 0))


def fixed(rows, cols):
    return pl.BlockSpec((rows, cols), lambda i: (0, 0))


def hidden_units(h2, w_fc, bias):
    rows, width = h2.shape
    units = w_fc.shape[1]
    tile = 256
    shape = jax.ShapeDtypeStruct((rows, units), BF)
    return pl.pallas_call(
        hidden_kernel,
        grid=(rows // tile,),
        out_shape=[shape, shape],
        in_specs=[tiled(tile, width), fixed(width, units), fixed(1, units)],
        out_specs=[tiled(tile, units), tiled(tile, units)],
        compiler_params=room(rows, HIDDEN),
        name="hidden",
    )(h2, w_fc, bias)


def hidden_back(cot, w_out, slope):
    rows, width = cot.shape
    units = w_out.shape[0]
    tile = 512
    return pl.pallas_call(
        hidden_back_kernel,
        grid=(rows // tile,),
        out_shape=[
            jax.ShapeDtypeStruct((rows, units), BF),
            jax.ShapeDtypeStruct((1, units), F32),
        ],
        in_specs=[tiled(tile, width), fixed(units, width), tiled(tile, units)],
        out_specs=[tiled(tile, units), fixed(1, units)],
        compiler_params=room(rows, HIDDEN_BACK),
        name="hidden_back",
    )(cot, w_out, slope)


def join_kernel(n, nz, hw, width, fc, qp, out, fc_o, qkv_o, proj_o, out_o):
    uw = fc.shape[-1] // nz
    for c in range(n):
        for b in range(nz):
            at = b * n * uw + c * uw
            fc_o[:, at : at + uw] = fc[c, 0, :, b * uw : (b + 1) * uw].astype(F32)
        size = min(128, width - c * 128)
        if size > 0:
            proj_o[:, c * 128 : c * 128 + size] = qp[c, 0, :, 3 * hw : 3 * hw + size].astype(F32)
        size = min(hw, width - c * hw)
        if size > 0:
            for t in range(3):
                at = t * width + c * hw
                qkv_o[:, at : at + size] = qp[c, 0, :, t * hw : t * hw + size].astype(F32)
    if 128 * n < width:
        proj_o[:, 128 * n :] = qp[n - 1, 0, :, : width - 128 * n].astype(F32)
    out_o[...] = out[...].astype(F32)


def join(n, nz, hw, fc, qp, out):
    tiles = 25
    width = out.shape[1]
    wz = fc.shape[1]
    split = lambda a: a.reshape(n, tiles, wz // tiles, a.shape[-1])
    fc, qp = split(fc), split(qp)
    wide = lambda a: pl.BlockSpec((n, 1, wz // tiles, a.shape[-1]), lambda i: (0, i, 0, 0))
    t, ot = wz // tiles, out.shape[0] // tiles
    cols = (n * fc.shape[-1], 3 * width, width)
    shape = jax.ShapeDtypeStruct
    return pl.pallas_call(
        functools.partial(join_kernel, n, nz, hw, width),
        grid=(tiles,),
        out_shape=[shape((wz, c), F32) for c in cols] + [shape(out.shape, F32)],
        in_specs=[wide(fc), wide(qp), tiled(ot, width)],
        out_specs=[tiled(t, c) for c in cols] + [tiled(ot, width)],
        compiler_params=room(1024, JOIN),
        name="join",
    )(fc, qp, out)


def attend_kernel(blocks, blk, tile, inv_ref, q_ref, k_ref, v_ref, o_ref, p_ref, qn, kn, vn, on, ot):
    length = blocks * blk
    for i in range(blocks):
        src, dst = pl.ds(pl.multiple_of(inv_ref[i] * blk, blk), blk), pl.ds(i * blk, blk)
        qn[dst, :] = q_ref[src, :]
        kn[dst, :] = k_ref[src, :]
        vn[dst, :] = v_ref[src, :]
    v_turned = vn[...].astype(F32).T.astype(BF)
    lane = lax.broadcasted_iota(jnp.int32, (1, 128), 1)
    above = lax.broadcasted_iota(jnp.int32, (tile, tile), 0) > lax.broadcasted_iota(
        jnp.int32, (tile, tile), 1
    )
    for i in range(length // tile):
        cols = pl.ds(i * tile, tile)
        keys = (i + 1) * tile
        for h in range(2):
            here = (lane // 64) == h
            q = jnp.where(here, qn[cols, :].astype(F32) * 0.125, 0.0).astype(BF)
            last = jnp.where(above, -1e30, dot(kn[pl.ds(i * tile, tile), :], q, NT))
            top = jnp.max(last, axis=0, keepdims=True)
            if i:
                early = dot(kn[pl.ds(0, i * tile), :], q, NT)
                top = jnp.maximum(top, jnp.max(early, axis=0, keepdims=True))
            last = jnp.exp(last - top)
            total = jnp.sum(last, axis=0, keepdims=True)
            if i:
                early = jnp.exp(early - top)
                total = total + jnp.sum(early, axis=0, keepdims=True)
            scale = 1.0 / total
            last = (last * scale).astype(BF)
            p_ref[h, pl.ds(i * tile, tile), cols] = last
            half = slice(64 * h, 64 * h + 64)
            o = dot(v_turned[half, i * tile : keys], last)
            if i:
                early = (early * scale).astype(BF)
                p_ref[h, pl.ds(0, i * tile), cols] = early
                o = o + dot(v_turned[half, : i * tile], early)
            ot[half, cols] = o
    on[...] = ot[...].T.astype(BF)
    for i in range(blocks):
        o_ref[pl.ds(pl.multiple_of(inv_ref[i] * blk, blk), blk), :] = on[i * blk : (i + 1) * blk, :]


def attend(qkv, inv, blk):
    length = qkv.shape[0]
    cols = qkv.shape[1] // 3
    pairs = cols // 128
    blocks = inv.shape[0]
    tile = 256
    piece = lambda off: pl.BlockSpec((length, 128), lambda p, s: (0, off * pairs + p))
    return pl.pallas_call(
        functools.partial(attend_kernel, blocks, blk, tile),
        out_shape=[
            jax.ShapeDtypeStruct((length, cols), BF),
            jax.ShapeDtypeStruct((2 * pairs, length, length), BF),
        ]
        + [jax.ShapeDtypeStruct((length, cols), BF)] * 4,
        grid_spec=pltpu.PrefetchScalarGridSpec(
            num_scalar_prefetch=1,
            grid=(pairs,),
            in_specs=[piece(0), piece(1), piece(2)],
            out_specs=[
                pl.BlockSpec((length, 128), lambda p, s: (0, p)),
                pl.BlockSpec((2, length, length), lambda p, s: (p, 0, 0)),
            ]
            + [pl.BlockSpec((length, 128), lambda p, s: (0, p))] * 4,
            scratch_shapes=[pltpu.VMEM((128, length), F32)],
        ),
        compiler_params=room(length, ATTEND),
        name="attend",
    )(inv, qkv, qkv, qkv)


def order_kernel(blocks, blk, table, x, out):
    for i in range(blocks):
        src = pl.ds(pl.multiple_of(table[i] * blk, blk), blk)
        out[i * blk : (i + 1) * blk, :] = x[src, :]


def order(x, table, blk):
    return pl.pallas_call(
        functools.partial(order_kernel, table.shape[0], blk),
        out_shape=jax.ShapeDtypeStruct(x.shape, x.dtype),
        in_specs=[pl.BlockSpec(memory_space=pltpu.SMEM), VMEM],
        out_specs=VMEM,
        compiler_params=room(x.shape[0], ORDER),
        name="order",
    )(table, x)


def heads_kernel(blocks, blk, tile, table, da, w, out, rows):
    step = pl.program_id(0)
    rows[pl.ds(pl.multiple_of(step * tile, tile), tile), :] = dot(da[...], w[...], NT).astype(BF)

    @pl.when(step == pl.num_programs(0) - 1)
    def _():
        for i in range(blocks):
            src = pl.ds(pl.multiple_of(table[i] * blk, blk), blk)
            out[i * blk : (i + 1) * blk, :] = rows[src, :]


def heads_grad(da, w_proj, table, blk):
    length, width = da.shape
    cols = w_proj.shape[0]
    tile = 512
    return pl.pallas_call(
        functools.partial(heads_kernel, table.shape[0], blk, tile),
        out_shape=jax.ShapeDtypeStruct((length, cols), BF),
        grid_spec=pltpu.PrefetchScalarGridSpec(
            num_scalar_prefetch=1,
            grid=(length // tile,),
            in_specs=[
                pl.BlockSpec((tile, width), lambda i, s: (i, 0)),
                pl.BlockSpec((cols, width), lambda i, s: (0, 0)),
            ],
            out_specs=pl.BlockSpec((length, cols), lambda i, s: (0, 0)),
            scratch_shapes=[pltpu.VMEM((length, cols), BF)],
        ),
        compiler_params=room(length, HEADS_GRAD),
        name="heads_grad",
    )(table, da, w_proj)


def back_kernel(
    n, tile, hw, width, ready, q, k, v, o, do, da_hbm, p_hbm, h1_hbm, all_hbm,
    ready_all, dqkv, sums, out,
    da, p, h1, o_all, dqt, dk, dv, load_s, p_s, *sems,
):
    me = lax.axis_index("ctx")
    length, cols = q.shape
    pairs = cols // 128
    slots = p.shape[0]
    greet(beside(n))
    gather = Gather(n, ready, ready_all, sems)
    gather.start()
    loads = [
        pltpu.make_async_copy(src, dst, load_s.at[i])
        for i, (src, dst) in enumerate([(da_hbm, da), (h1_hbm, h1), (all_hbm, o_all)])
    ]

    def load_p(pair):
        at = pair % slots
        return pltpu.make_async_copy(p_hbm.at[pl.ds(2 * pair, 2)], p.at[at], p_s.at[at])

    load_p(0).start()
    for load in loads:
        load.start()
    lane = lax.broadcasted_iota(jnp.int32, (1, 128), 1)
    held = {}

    def begin(pair):
        if pair + 1 < pairs and slots > 1:
            load_p(pair + 1).start()
        at = slice(pair * 128, pair * 128 + 128)
        held["k"] = k[:, at].astype(F32).T.astype(BF)
        prod = (do[:, at].astype(F32) * o[:, at].astype(F32)).T
        held["d"] = [jnp.sum(prod[64 * h : 64 * h + 64, :], axis=0, keepdims=True) for h in range(2)]
        dk[...] = jnp.zeros_like(dk)
        dv[...] = jnp.zeros_like(dv)
        load_p(pair).wait()

    def block(pair, i):
        win = pl.ds(i * tile, tile)
        at = slice(pair * 128, pair * 128 + 128)
        keys = (i + 1) * tile
        for h in range(2):
            here = (lane // 64) == h
            query = jnp.where(here, q[win, at].astype(F32), 0.0).astype(BF)
            grad = jnp.where(here, do[win, at].astype(F32), 0.0).astype(BF)
            prob = p[pair % slots, h, pl.ds(0, keys), win]
            dp = dot(v[pl.ds(0, keys), at], grad, NT)
            ds = (prob.astype(F32) * (dp - held["d"][h][:, i * tile : (i + 1) * tile]) * 0.125).astype(BF)
            half = slice(64 * h, 64 * h + 64)
            dqt[half, win] = dot(held["k"][half, :keys], ds)
            dk[pl.ds(0, keys), :] += dot(ds, query)
            dv[pl.ds(0, keys), :] += dot(prob, grad)

    def end(pair):
        for t, val in enumerate((dqt[...].T, dk[...], dv[...])):
            at = slice((t * pairs + pair) * 128, (t * pairs + pair) * 128 + 128)
            low = val.astype(BF)
            sums[:, at] = jnp.sum(low.astype(F32), axis=0, keepdims=True)
            dqkv[:, at] = low

    spare = max(0, width - 128 * n)
    whole_tiles = width // hw

    def products(rows, x, y):
        out[rows, 3 * cols :] = dot(y, da[:, pl.ds(pl.multiple_of(me * 128, 128), 128)], TN).astype(BF)

        @pl.when(me < n - 1 if spare else me < n)
        def _():
            out[rows, : 3 * cols] = dot(x, dqkv[...], TN).astype(BF)

        if spare:

            @pl.when(me == n - 1)
            def _():
                out[rows, : 3 * cols] = jnp.zeros((x.shape[1], 3 * cols), BF)
                out[rows, :spare] = dot(y, da[:, 128 * n :], TN).astype(BF)

    def weights(lo, hi):
        if lo == 0:
            for load in loads:
                load.wait()

        def body(i, carry):
            at = pl.ds(pl.multiple_of(i * hw, hw), hw)
            products(at, h1[:, at], o_all[i])
            return carry

        lax.fori_loop(lo, hi, body, 0)
        if hi == whole_tiles and width % hw:
            rest = width % hw
            at = pl.ds(hi * hw, rest)
            products(at, h1[:, at], o_all[hi, :, :rest])

    part = functools.partial
    steps = []
    for pair in range(pairs):
        steps.append((1.0, part(begin, pair)))
        steps += [(0.6 + 0.5 * i, part(block, pair, i)) for i in range(length // tile)]
        steps.append((1.0, part(end, pair)))
    cut = whole_tiles // 2
    steps += [(5.5, part(weights, 0, cut)), (5.5, part(weights, cut, whole_tiles))]
    clock, work = 0.0, []
    for size, step in steps:
        work.append((clock, step))
        clock += size
    timed(work, gather.timed_steps(lambda c: 3.5 * c, 6.0, 5.0))
    gather.finish()


def back(n, cid, ready, q, k, v, o, do, da, p, h1, o_all):
    length, hw = q.shape
    width = da.shape[1]
    if 128 * n > width:
        da = jnp.pad(da, ((0, 0), (0, 128 * n - width)))
    assert width <= 128 * n or (n - 1) * hw >= width and width - 128 * n <= 3 * hw
    dma = pltpu.SemaphoreType.DMA
    slots = min(2, hw // 128)
    return call(
        functools.partial(back_kernel, n, 256, hw, width),
        cid,
        "back",
        (ready, q, k, v, o, do, da, p, h1, o_all),
        [VMEM] * 6 + [ANY] * 4,
        [
            ((n,) + ready.shape, BF),
            ((length, 3 * hw), BF),
            ((1, 3 * hw), F32),
            ((width, 3 * hw + 128), BF),
        ],
        [ANY, VMEM, VMEM, VMEM],
        [
            pltpu.VMEM(da.shape, BF),
            pltpu.VMEM((slots, 2, length, length), BF),
            pltpu.VMEM(h1.shape, BF),
            pltpu.VMEM(o_all.shape, BF),
            pltpu.VMEM((128, length), F32),
            pltpu.VMEM((length, 128), F32),
            pltpu.VMEM((length, 128), F32),
            dma((3,)),
            dma((slots,)),
        ]
        + Gather.sems(n, ready.shape[0]),
        BACK if n == 8 else 60,
    )


def norm(values):
    centre = values - jnp.mean(values, axis=-1, keepdims=True)
    rstd = lax.rsqrt(jnp.mean(centre * centre, axis=-1, keepdims=True) + 1e-05)
    return centre * rstd, rstd


def norm_back(grad, unit, rstd, gain):
    inner = grad * gain
    return rstd * (
        inner
        - jnp.mean(inner, axis=-1, keepdims=True)
        - unit * jnp.mean(inner * unit, axis=-1, keepdims=True)
    )


def make_body(n, nz):
    def body(
        tokens, block_table, ln1_gain, ln1_bias, qkv_weight, query_bias, value_bias,
        proj_weight, proj_bias, ln2_gain, ln2_bias, fc_weight, fc_bias, out_weight,
        out_bias, cotangent,
    ):
        ctx = lax.axis_index("ctx")
        z = lax.axis_index("fsdp")
        rows, width = tokens.shape
        blk = rows // 2
        wz = width // nz
        slots = -(-HEADS // n)
        hw = slots * (width // HEADS)
        unit_z = out_weight.shape[0]
        uw = unit_z // n
        units = uw * nz
        table = block_table.reshape(-1)
        inv = jnp.argmax(
            table[None, :] == jnp.arange(table.shape[0], dtype=table.dtype)[:, None], axis=1
        ).astype(jnp.int32)

        take = lambda a, at, size, axis=0: lax.dynamic_slice_in_dim(a, at, size, axis)
        parts = 5
        padded = jnp.pad(qkv_weight, ((0, 0), (0, n * hw - width)))
        wq_own = jnp.concatenate(
            [take(padded, t * width + ctx * hw, hw, 1) for t in range(3)], axis=1
        ).reshape(parts, wz // parts, 3 * hw)
        row = lax.broadcasted_iota(jnp.int32, (16, wz), 0)
        small = jnp.zeros((16, wz), BF)
        for i, v in enumerate(
            [ln1_gain, ln1_bias, query_bias, value_bias, proj_bias, ln2_gain, ln2_bias, out_bias]
            + [jnp.pad(take(fc_bias, ctx * uw, uw), (0, wz - uw))]
        ):
            small = jnp.where(row == i, v[None, :], small)
        tile = math.gcd(wz, hw)
        h1, cot, small, w_qkv, w_proj, tok_own, cot_own, wfc_own, wout_own = entry(
            n,
            nz,
            tokens,
            cotangent,
            small,
            wq_own,
            proj_weight.reshape(wz // tile, tile, width),
            fc_weight.reshape(25, wz // 25, fc_weight.shape[1]),
            out_weight.reshape(n, uw, width),
            hw,
        )
        w_fc = lax.all_gather(wfc_own.reshape(wz, units), "fsdp", axis=0, tiled=True)
        w_out = lax.all_gather(wout_own, "fsdp", axis=0, tiled=True)
        length = n * rows
        flat = lambda a: a.reshape(length, a.shape[-1])
        h1, cot = flat(h1), flat(cot)
        w_qkv, w_proj = w_qkv.reshape(width, 3 * hw), w_proj.reshape(hw, width)
        fb = small[8].reshape(nz, wz)[:, :uw].reshape(1, units)
        pad_cols = lambda v: take(jnp.pad(v, (0, n * hw - width)), ctx * hw, hw)
        qkv_bias = jnp.concatenate([pad_cols(small[2]), jnp.zeros((hw,), F32), pad_cols(small[3])])

        qkv = (dot(h1, w_qkv) + qkv_bias).astype(BF)
        o, p, q_pos, k_pos, v_pos, o_pos = attend(qkv, inv, blk)
        mid, h2 = middle(n, 2, o, w_proj, tok_own, small)
        h2 = flat(h2)
        hidden, slope = hidden_units(h2, w_fc, fb)
        part_out = dot(hidden, cot, TN).astype(BF)
        in_parts = lambda a: a.reshape(nz, parts, a.shape[0] // nz // parts, a.shape[1])
        o, part_out = lax.optimization_barrier((o, part_out))
        o_all = spread(n, 3, o.reshape(4, length // 4, hw))
        h1_pos = order(h1, inv, blk)
        w_out, o_all, h1_pos = lax.optimization_barrier((w_out, o_all, h1_pos))
        to_owner = lambda a: lax.psum_scatter(a, "fsdp", scatter_dimension=0, tiled=True)
        sum_out = to_owner(part_out)
        du, dfb = hidden_back(cot, w_out, slope)
        part_fc = outer(h2, du)
        du, part_fc = lax.optimization_barrier((du, part_fc))
        sum_fc = to_owner(part_fc)
        da, dmid, layer_out, sums = turn(n, 4, du, w_fc, hidden, w_out, mid, cot_own, small)
        da = flat(da)
        all_out, dqkv, bias_cols, part_attn = back(
            n,
            6,
            sum_out.reshape(parts, uw // parts, width),
            q_pos,
            k_pos,
            v_pos,
            o_pos,
            heads_grad(da, w_proj, inv, blk),
            da,
            p,
            h1_pos,
            o_all.reshape(n, length, hw),
        )
        dqkv = order(dqkv, table, blk)

        put = lambda v, size: lax.dynamic_update_slice_in_dim(
            jnp.zeros((1, size), F32), v, ctx * v.shape[1], 1
        )
        biases = jnp.concatenate(
            [put(bias_cols[:, :hw], n * hw), put(bias_cols[:, 2 * hw :], n * hw)]
        )[:, :width]
        wide_fb = lax.dynamic_update_slice_in_dim(
            jnp.zeros((nz, unit_z), F32), dfb.reshape(nz, uw), ctx * uw, 1
        )
        vectors = jnp.concatenate(
            [sums + jnp.pad(biases, ((2, 4), (0, 0))), jnp.pad(wide_fb, ((0, -nz % 8), (0, width - unit_z)))]
        )
        all_fc, all_attn, grad_tokens, vectors = tail(
            n,
            nz,
            5,
            sum_fc.reshape(parts, wz // parts, units),
            in_parts(part_attn),
            dqkv,
            w_qkv,
            tok_own,
            dmid,
            small,
            vectors,
        )
        whole_rows = lambda a: a.reshape(n, a.shape[1] * a.shape[2], a.shape[3])
        grad_fc, grad_qkv, grad_proj, grad_out = join(
            n, nz, hw, whole_rows(all_fc), whole_rows(all_attn), all_out.reshape(unit_z, width)
        )
        vectors, grad_tokens, layer_out, grad_fc = lax.optimization_barrier(
            (vectors, grad_tokens, layer_out, grad_fc)
        )
        mine = take(vectors[:8], z * wz, wz, 1)
        gfb = take(vectors[8 : 8 + nz], z, 1).reshape(-1)[:unit_z]
        return (
            layer_out,
            grad_tokens,
            mine[0],
            mine[1],
            grad_qkv,
            mine[2],
            mine[3],
            grad_proj,
            mine[4],
            mine[5],
            mine[6],
            grad_fc,
            gfb,
            grad_out,
            mine[7],
        )

    return body


def solution(mesh):
    both = P(("fsdp", "ctx"), None)
    vec, mat = P("fsdp"), P("fsdp", None)
    placed = (both, P(), vec, vec, mat, vec, vec, mat, vec, vec, vec, mat, vec, mat, vec, both)
    outs = (both, both, vec, vec, mat, vec, vec, mat, vec, vec, vec, mat, vec, mat, vec)
    return jax.shard_map(
        make_body(mesh.shape["ctx"], mesh.shape["fsdp"]),
        mesh=mesh,
        in_specs=placed,
        out_specs=outs,
        check_vma=False,
    )
```
